32 devices in a mesh: patch: 4 (over x, core), space: 8 (over z, y).
Axes of the slice: x: 2, y: 2, z: 4, core: 2. Of those that a mesh axis runs over, the one named last changes fastest.
Arguments:
- image: bfloat16 [32, 16, 256], P('patch', 'space'), may hold values from -6 to 6
- offsets: int32 [4, 2], replicated, may hold values from 0 to 128, as said below
- conv1_weight: bfloat16 [9, 32, 3], replicated, may hold values from -1.25 to 1.25
- conv2_weight: bfloat16 [9, 32, 96], replicated, may hold values from -0.21875 to 0.21875
- norm1_gain: float32 [32], replicated, may hold values from 0.1 to 1.9
- norm1_bias: float32 [32], replicated, may hold values from -3 to 3
- norm2_gain: float32 [32], replicated, may hold values from 0.1 to 1.9
- norm2_bias: float32 [32], replicated, may hold values from -3 to 3
- head_weight: bfloat16 [3, 32], replicated, may hold values from -1 to 1
- head_bias: float32 [3], replicated, may hold values from -3 to 3
Outputs:
- volume_logits: float32 [32, 3, 16, 256], P('patch', None, 'space')
The draws below stay inside these ranges and needn't reach their ends.
Inputs may be any that keep to these rules, and one draw needn't show every extreme that they name: offsets[p] = (oz, ox) with 0 <= oz <= 16 and 0 <= ox <= 128; some patch starts at oz = 16, some at ox = 128, some at ox = 0.
All inputs are finite; a program needn't handle non-finite values.
Results may differ from the reference program's by a relative error of at most 0.0024.
Values may be sent and summed in bfloat16 or wider, within the bound.
No kernel may reach another device: no remote copies, remote signals or barrier semaphores. Data moves between devices by JAX's collectives and lax.ppermute only.
A program may use at most 64 MiB of HBM per device.

```python
import jax
import jax.numpy as jnp
from jax import lax

CH = 32
CLASSES = 3
PX = 128
PZ = 16
PATCHES = 4
PY = 16
VZ = 32
VX = 256


def draw_offsets(key, part):
    depth_room = VZ - PZ
    width_room = VX - PX
    draw_one = jax.random.randint(jax.random.fold_in(key, 11), (PATCHES,), 0, depth_room + 1)
    draw_two = jax.random.randint(jax.random.fold_in(key, 12), (PATCHES,), 0, depth_room + 1)
    depths = (draw_one + draw_two) // 2
    across = jax.random.randint(jax.random.fold_in(key, 13), (PATCHES,), 0, width_room + 1)
    deep_index = jax.random.randint(jax.random.fold_in(key, 14), (), 0, PATCHES)
    wide_index = jax.random.randint(jax.random.fold_in(key, 15), (), 0, PATCHES)
    step_index = jax.random.randint(jax.random.fold_in(key, 16), (), 0, PATCHES - 1)
    left_index = (wide_index + 1 + step_index) % PATCHES
    depths = depths.at[deep_index].set(depth_room)
    across = across.at[wide_index].set(width_room)
    across = across.at[left_index].set(0)
    return jnp.stack([depths, across], axis=1).astype(jnp.int32)


def shard_levels(key, shape, pieces, smallest, top_value):
    def one(dim, parts):
        heights = jax.random.uniform(jax.random.fold_in(jax.random.fold_in(key, 6), dim), (parts,), jnp.float32, smallest / len(pieces), top_value / len(pieces))
        return jnp.repeat(jnp.exp(heights), shape[dim] // parts).reshape((-1,) + (1,) * (len(shape) - dim - 1))

    loudness = one(*pieces[0])
    for cut in pieces[1:]:
        loudness = loudness * one(*cut)
    return loudness


def centred(rng, dims, scale, bound, pieces=(), kind=jnp.bfloat16):
    array = jax.random.normal(rng, dims, jnp.float32) * scale
    if len(pieces) > 0:
        array = shard_levels(rng, dims, pieces, -0.22, 0.18) * array
    return jnp.clip(array, min=-bound, max=bound).astype(kind)


def setup_inputs(seed: int = 0) -> dict:
    key_of = jax.random.split(jax.random.key(seed), 11)
    return {
        "image": centred(key_of[0], (VZ, PY, VX), 1.0, 6.0, ((0, 4), (1, 8))),
        "offsets": draw_offsets(jax.random.fold_in(key_of[10], 71), 0),
        "conv1_weight": centred(key_of[2], (9, CH, 3), 27 ** -0.5, 1.25),
        "conv2_weight": centred(key_of[3], (9, CH, 3 * CH), (27 * CH) ** -0.5, 0.21875),
        "norm1_gain": jnp.clip(1.0 + 0.18 * jax.random.normal(key_of[4], (CH,), jnp.float32), 0.1, 1.9),
        "norm1_bias": centred(key_of[5], (CH,), 0.5, 3.0, (), jnp.float32),
        "norm2_gain": jnp.clip(1.0 + 0.18 * jax.random.normal(key_of[6], (CH,), jnp.float32), 0.1, 1.9),
        "norm2_bias": centred(key_of[7], (CH,), 0.5, 3.0, (), jnp.float32),
        "head_weight": centred(key_of[8], (CLASSES, CH), CH ** -0.5, 1.0),
        "head_bias": centred(key_of[9], (CLASSES,), 0.5, 3.0, (), jnp.float32),
    }


def gauss_value(positions, length):
    center = (length - 1) / 2.0
    deviation = length / 8.0
    offset = positions - center
    return jnp.exp(-(offset * offset) / (2.0 * deviation * deviation))

def apply_taps(padded, weights):
    depth_cells = padded.shape[2] - 2
    row_cells = padded.shape[3] - 2
    col_cells = padded.shape[4] - 2
    stacked = jnp.concatenate([padded[:, :, :, :, col_shift:col_shift + col_cells] for col_shift in range(3)], axis=1)
    summed = jnp.zeros((padded.shape[0], weights.shape[1], depth_cells, row_cells, col_cells), jnp.float32)
    for depth_tap in range(3):
        for row_tap in range(3):
            window = stacked[:, :, depth_tap:depth_tap + depth_cells, row_tap:row_tap + row_cells, :]
            summed = summed + jnp.einsum('oc,fczyx->fozyx', weights[depth_tap * 3 + row_tap].astype(jnp.float32), window.astype(jnp.float32))
    return summed

def convolve(features, weights):
    padded = jnp.pad(features, ((0, 0), (0, 0), (1, 1), (1, 1), (1, 1)))
    return apply_taps(padded, weights)

def normalize(values, channel_gain, channel_bias):
    average = lax.optimization_barrier(jnp.mean(values, axis=(2, 3, 4)))
    centered = values - average[:, :, None, None, None]
    variance = lax.optimization_barrier(jnp.mean(centered * centered, axis=(2, 3, 4)))
    factor = lax.rsqrt(variance + 1e-05) * channel_gain[None, :]
    shifted = centered * factor[:, :, None, None, None] + channel_bias[None, :, None, None, None]
    return jnp.where(shifted >= 0, shifted, 0.01 * shifted).astype(jnp.bfloat16)

def run_network(patch_cells, conv1_weight, conv2_weight, norm1_gain, norm1_bias, norm2_gain, norm2_bias, head_weight, head_bias):
    flipped = jnp.stack([patch_cells, patch_cells[::-1], patch_cells[:, :, ::-1], patch_cells[::-1, :, ::-1]])[:, None]
    hidden = normalize(convolve(flipped, conv1_weight), norm1_gain, norm1_bias)
    hidden = normalize(convolve(hidden, conv2_weight), norm2_gain, norm2_bias)
    logits = jnp.einsum('kc,fczyx->fzkyx', head_weight.astype(jnp.float32), hidden.astype(jnp.float32))
    logits = logits + head_bias[None, None, :, None, None]
    restored = logits[0] + logits[1][::-1] + logits[2][:, :, :, ::-1] + logits[3][::-1, :, :, ::-1]
    return restored * 0.25

def reference(image, offsets, conv1_weight, conv2_weight, norm1_gain, norm1_bias, norm2_gain, norm2_bias, head_weight, head_bias):
    gauss_depth = gauss_value(jnp.arange(PZ, dtype=jnp.float32), PZ)
    gauss_rows = gauss_value(jnp.arange(PY, dtype=jnp.float32), PY)
    gauss_cols = gauss_value(jnp.arange(PX, dtype=jnp.float32), PX)
    weight_map = gauss_depth[:, None, None] * gauss_rows[None, :, None] * gauss_cols[None, None, :]

    def one_patch(item_index, carried):
        blended, coverage = carried
        corner = lax.dynamic_index_in_dim(offsets, item_index, 0, keepdims=False).astype(jnp.int32)
        start_z = corner[0]
        start_x = corner[1]
        zero_index = jnp.zeros((), jnp.int32)
        patch_cells = lax.dynamic_slice(image, (start_z, zero_index, start_x), (PZ, PY, PX))
        averaged = run_network(patch_cells, conv1_weight, conv2_weight, norm1_gain, norm1_bias, norm2_gain, norm2_bias, head_weight, head_bias)
        contrib = averaged * weight_map[:, None, :, :]
        current = lax.dynamic_slice(blended, (start_z, zero_index, zero_index, start_x), contrib.shape)
        blended = lax.dynamic_update_slice(blended, current + contrib, (start_z, zero_index, zero_index, start_x))
        present = lax.dynamic_slice(coverage, (start_z, zero_index, start_x), weight_map.shape)
        coverage = lax.dynamic_update_slice(coverage, present + weight_map, (start_z, zero_index, start_x))
        return (blended, coverage)
    start_blend = jnp.zeros((VZ, CLASSES, PY, VX), jnp.float32)
    start_cover = jnp.zeros((VZ, PY, VX), jnp.float32)
    blended, coverage = lax.fori_loop(0, PATCHES, one_patch, (start_blend, start_cover))
    return blended / jnp.maximum(coverage, 0.1)[:, None, :, :]
```

```python
import functools

import jax
import jax.numpy as jnp
from jax import lax
from jax.experimental import pallas as pl
from jax.experimental.pallas import tpu as pltpu
from jax.sharding import PartitionSpec as P

PX = 128
PZ = 16
TAPS = 3
ZG = 4
ZI = ZG + TAPS - 1
F32 = jnp.float32
BF16 = jnp.bfloat16
HI = lax.Precision.HIGHEST
CONTRACT_FIRST = (((0,), (0,)), ((), ()))
CONTRACT_LAST = (((1,), (1,)), ((), ()))
VMEM = pl.BlockSpec(memory_space=pltpu.VMEM)
SMEM = pl.BlockSpec(memory_space=pltpu.SMEM)


def iota(shape, dim):
    return lax.broadcasted_iota(jnp.int32, shape, dim)


def repeat_matrix(channels, lanes, dtype):
    shape = (channels, lanes)
    return (iota(shape, 0) == iota(shape, 1) % channels).astype(dtype)


def cut_kernel(offsets_ref, image_ref, out_ref, rows_ref):
    slab_rows, band_rows, width = image_ref.shape
    for z in range(slab_rows):
        rows_ref[z * band_rows : (z + 1) * band_rows, :] = image_ref[z].astype(F32)
    rows = rows_ref[...]
    for item in range(out_ref.shape[0]):
        shift = lax.rem(width - offsets_ref[item, 1], width)
        window = pltpu.roll(rows, shift, 1)[:, :PX].astype(BF16)
        for space in range(out_ref.shape[1]):
            out_ref[item, space] = window


def tap_rows(offsets_ref, gathered_ref, cells_ref, taps_ref, slab_rows, band_rows, spaces):
    block = slab_rows * band_rows
    devices = gathered_ref.shape[0]
    for device in range(devices):
        cells_ref[device * block : (device + 1) * block, :] = gathered_ref[device].astype(F32)
    taps_ref[...] = jnp.zeros_like(taps_ref)
    rows = band_rows * spaces
    for z in range(PZ):
        taps_ref[z, pl.ds(32 + 15, rows, stride=16), :] = jnp.ones((rows, PX), F32)
    item = lax.axis_index("patch")
    start_z = offsets_ref[item, 0]
    lane = iota((spaces, PX), 1)
    for z in range(PZ):
        deep = start_z + z
        slab = lax.div(deep, slab_rows)
        base = slab * (spaces * block) + (deep - slab * slab_rows) * band_rows
        for y in range(band_rows):
            line = cells_ref[pl.ds(base + y, spaces, stride=block), :]
            before = jnp.where(lane == 0, 0.0, pltpu.roll(line, 1, 1))
            after = jnp.where(lane == PX - 1, 0.0, pltpu.roll(line, PX - 1, 1))
            for a in range(TAPS):
                at = z + 1 - a
                if 0 <= at < PZ:
                    for c, value in enumerate((before, line, after)):
                        first = 32 + 16 * y + a * TAPS + c
                        taps_ref[at, pl.ds(first, spaces, stride=16 * band_rows), :] = value


def first_moments(taps_ref, gram_ref, weights, rows):
    cells = [taps_ref[z, 32 : 32 + 16 * rows, :].astype(BF16) for z in range(PZ)]
    cells = jnp.concatenate(cells, axis=1)
    gram_ref[...] = lax.dot_general(cells, cells, CONTRACT_LAST, preferred_element_type=F32)

    def block(y, delta):
        lane = 16 * (y + delta)
        tile = lane // 128 * 128
        value = gram_ref[16 * y : 16 * y + 16, tile : tile + 128]
        return pltpu.roll(value, (tile + 128 - lane) % 128, 1) if lane != tile else value

    def total(values):
        values = list(values)
        while len(values) > 1:
            values = [
                values[i] + values[i + 1] if i + 1 < len(values) else values[i]
                for i in range(0, len(values), 2)
            ]
        return jnp.where(iota((16, 128), 1) < 16, values[0], 0.0)

    head, tail = total([block(0, 0)]), total([block(rows - 1, 0)])
    near = total([block(y, 0) for y in range(rows)])
    next1 = 2.0 * total([block(y, 1) for y in range(rows - 1)])
    next2 = 2.0 * total([block(y, 2) for y in range(rows - 2)])
    diag = (near - tail, near, near - head)
    move = lambda value, k: pltpu.roll(value, 16 * k, 1) if k else value
    form = jnp.concatenate(
        [
            diag[0] + move(next1, 1) + move(next2, 2),
            move(diag[1], 1) + move(next1, 2),
            move(diag[2], 2),
            diag[0] + move(diag[1], 1) + move(diag[2], 2),
        ],
        axis=0,
    )[:, :48]
    product = jnp.dot(form, weights, precision=HI, preferred_element_type=F32)
    squares = jnp.sum(product[:48] * weights, axis=0, keepdims=True)
    return product[63:64], squares


def main_kernel(
    spaces,
    slab_rows,
    band_rows,
    offsets_ref,
    gathered_ref,
    w1_ref,
    w2_ref,
    gain_ref,
    bias_ref,
    conv_ref,
    stats_ref,
    cells_ref,
    taps_ref,
    gram_ref,
    wide_ref,
    w2t_ref,
    sums_ref,
):
    rows = band_rows * spaces
    channels = gain_ref.shape[1]
    hidden_rows = band_rows + TAPS - 1
    in_rows = hidden_rows + TAPS - 1
    width = 4 * hidden_rows * channels
    band = lax.axis_index("space")
    tap_rows(offsets_ref, gathered_ref, cells_ref, taps_ref, slab_rows, band_rows, spaces)

    w1 = w1_ref[...].astype(F32)
    first, second = first_moments(taps_ref, gram_ref, w1.reshape(TAPS * 16, width), rows)
    count = float(PZ * rows * PX)
    repeat = repeat_matrix(channels, width, F32)
    params = jnp.concatenate([gain_ref[...], bias_ref[...], jnp.zeros((6, channels), F32)], axis=0)
    params = jnp.dot(params, repeat, precision=HI, preferred_element_type=F32)
    mean = first / count
    variance = second / count - mean * mean
    lane_row = iota((1, width), 1) // channels % hidden_rows
    y = band * band_rows - 1 + lane_row
    inside = (y >= 0) & (y < rows)
    scale = lax.rsqrt(variance + 1e-05) * params[0:1]
    shift = jnp.where(inside, params[1:2] - mean * scale, 0.0)
    scale = jnp.where(inside, scale, 0.0)

    lane_row = iota((16, width), 1) // channels % hidden_rows
    pieces = []
    for yi in range(in_rows):
        piece = jnp.zeros((16, width), F32)
        for b in range(TAPS):
            if 0 <= yi - b < hidden_rows:
                piece = jnp.where(lane_row == yi - b, w1[b], piece)
        pieces.append(piece)
    w1_full = jnp.concatenate(pieces, axis=0).astype(BF16)

    out_lanes = ZG * band_rows * channels
    spread = repeat_matrix(channels, out_lanes, BF16)
    taps2 = [
        lax.dot_general(w2_ref[t], spread, CONTRACT_FIRST, preferred_element_type=F32)
        for t in range(TAPS * TAPS)
    ]
    group = iota((TAPS * channels, out_lanes), 1) // channels
    for zi in range(ZI):
        for yi in range(hidden_rows):
            piece = jnp.zeros((TAPS * channels, out_lanes), F32)
            for zo in range(ZG):
                for yo in range(band_rows):
                    a, b = zi - zo, yi - yo
                    if 0 <= a < TAPS and 0 <= b < TAPS:
                        piece = jnp.where(group == zo * band_rows + yo, taps2[a * TAPS + b], piece)
            piece = piece.astype(BF16)
            at = (zi * hidden_rows + yi) * channels
            for c in range(TAPS):
                w2t_ref[c, at : at + channels, :] = piece[c * channels : (c + 1) * channels]

    step = hidden_rows * channels
    groups = PZ // ZG
    empty = jnp.zeros((PX, step), BF16)
    for f in range(4):
        for g, j in ((0, 0), (groups - 1, ZI - 1)):
            at = (ZI - 1 - j if f % 2 else j) * step
            wide_ref[f, g * PX : (g + 1) * PX, at : at + step] = empty
    start = pl.multiple_of(band * (16 * band_rows), 16)
    for z in range(PZ):
        cells = taps_ref[z, pl.ds(start, in_rows * 16), :].astype(BF16)
        value = lax.dot_general(cells, w1_full, CONTRACT_FIRST, preferred_element_type=F32)
        value = value * scale + shift
        value = jnp.maximum(value, 0.01 * value).astype(BF16)
        for g in range(groups):
            j = z + 1 - ZG * g
            if 0 <= j < ZI:
                for f in range(4):
                    at = (ZI - 1 - j if f % 2 else j) * step
                    wide_ref[f, g * PX : (g + 1) * PX, at : at + step] = value[
                        :, f * step : (f + 1) * step
                    ]

    x = iota((groups * PX, out_lanes), 0) % PX
    for f in range(4):
        cells = wide_ref[f]
        parts = [
            jnp.dot(cells, w2t_ref[c], preferred_element_type=F32) for c in range(TAPS)
        ]
        before, after = (parts[2], parts[0]) if f >= 2 else (parts[0], parts[2])
        value = (
            parts[1]
            + jnp.where(x == 0, 0.0, pltpu.roll(before, 1, 0))
            + jnp.where(x == PX - 1, 0.0, pltpu.roll(after, groups * PX - 1, 0))
        )
        conv_ref[f] = value
        sums_ref[2 * f : 2 * f + 1, :] = jnp.sum(value, axis=0, keepdims=True)
        sums_ref[2 * f + 1 : 2 * f + 2, :] = jnp.sum(value * value, axis=0, keepdims=True)
    sums = sums_ref[...]
    for space in range(spaces):
        stats_ref[space] = sums


def head_kernel(
    count, band_rows, conv_ref, stats_ref, gain_ref, bias_ref, head_ref, head_bias_ref, out_ref
):
    channels = gain_ref.shape[1]
    lanes = conv_ref.shape[2]
    classes = head_ref.shape[0]
    sums = stats_ref[0]
    for space in range(1, stats_ref.shape[0]):
        sums = sums + stats_ref[space]
    reach = lanes // 2
    while reach >= channels:
        sums = sums + pltpu.roll(sums, reach, 1)
        reach //= 2
    repeat = repeat_matrix(channels, lanes, F32)
    params = jnp.concatenate([gain_ref[...], bias_ref[...], jnp.zeros((6, channels), F32)], axis=0)
    params = jnp.dot(params, repeat, precision=HI, preferred_element_type=F32)
    head = jnp.concatenate([head_ref[...].astype(F32), jnp.zeros((8 - classes, channels), F32)], 0)
    head = jnp.dot(head, repeat, precision=HI, preferred_element_type=F32)
    per_z = classes * band_rows
    shape = (ZG * per_z, lanes)
    row_z, row_k, row_y = (
        iota(shape, 0) // per_z,
        iota(shape, 0) // band_rows % classes,
        iota(shape, 0) % band_rows,
    )
    full = jnp.zeros(shape, F32)
    for k in range(classes):
        full = jnp.where(row_k == k, head[k : k + 1], full)
    lane_z = iota(shape, 1) // (band_rows * channels)
    lane_y = iota(shape, 1) // channels % band_rows
    heads = [
        jnp.where((lane_z == z) & (lane_y == row_y), full, 0.0).astype(BF16)
        for z in (row_z, ZG - 1 - row_z)
    ]
    shape = (ZG * per_z, PX)
    row_k = iota(shape, 0) // band_rows % classes
    bias = jnp.zeros(shape, F32)
    for k in range(classes):
        bias = jnp.where(row_k == k, head_bias_ref[k], bias)
    groups = conv_ref.shape[1] // PX
    totals = [None] * groups
    for f in range(4):
        mean = sums[2 * f : 2 * f + 1] / count
        variance = sums[2 * f + 1 : 2 * f + 2] / count - mean * mean
        scale = lax.rsqrt(variance + 1e-05) * params[0:1]
        shift = params[1:2] - mean * scale
        for g in range(groups):
            value = conv_ref[f, g * PX : (g + 1) * PX, :] * scale + shift
            value = jnp.maximum(value, 0.01 * value).astype(BF16)
            logits = lax.dot_general(
                heads[f % 2], value, CONTRACT_LAST, preferred_element_type=F32
            )
            totals[g] = logits if totals[g] is None else totals[g] + logits
    for g in range(groups):
        at = g * ZG * per_z
        out_ref[at : at + ZG * per_z, :] = totals[g] * 0.25 + bias


def place_kernel(spaces, offsets_ref, parts_ref, out_ref, pad_ref):
    slab_rows, classes, band_rows, width = out_ref.shape
    patch_rows = band_rows * spaces
    per_z = classes * band_rows
    count = slab_rows * per_z
    slab = lax.axis_index("patch") * slab_rows
    band = lax.axis_index("space") * band_rows
    shape = (count, width)
    z = slab + iota(shape, 0) // per_z
    x = iota(shape, 1)
    y = (band + iota(shape, 0) % band_rows).astype(F32) - (patch_rows - 1) / 2.0
    across = y * y * (1.0 / (2.0 * (patch_rows / 8.0) ** 2))
    blended = jnp.zeros(shape, F32)
    coverage = jnp.zeros(shape, F32)
    for item in range(parts_ref.shape[0]):
        pad_ref[item, count : count + PZ * per_z, :] = parts_ref[item].astype(F32)
        start_z, start_x = offsets_ref[item, 0], offsets_ref[item, 1]
        first = jnp.clip(slab - start_z, -slab_rows, PZ) * per_z + count
        part = pad_ref[item, pl.ds(first, count), :]
        part = jnp.concatenate([part, jnp.zeros((count, width - PX), F32)], axis=1)
        part = pltpu.roll(part, start_x, 1)
        rel_z, rel_x = z - start_z, x - start_x
        inside = (rel_z >= 0) & (rel_z < PZ) & (rel_x >= 0) & (rel_x < PX)
        far_z = rel_z.astype(F32) - (PZ - 1) / 2.0
        far_x = rel_x.astype(F32) - (PX - 1) / 2.0
        power = (
            across
            + far_z * far_z * (1.0 / (2.0 * (PZ / 8.0) ** 2))
            + far_x * far_x * (1.0 / (2.0 * (PX / 8.0) ** 2))
        )
        weight = jnp.where(inside, jnp.exp(-power), 0.0)
        blended = blended + jnp.where(inside, part * weight, 0.0)
        coverage = coverage + weight
    value = blended / jnp.maximum(coverage, 0.1)
    for z in range(slab_rows):
        for k in range(classes):
            at = z * per_z + k * band_rows
            out_ref[z, k] = value[at : at + band_rows]


def mirrored(weights, channels):
    taps = weights.reshape(TAPS, TAPS, channels, TAPS)
    sets = jnp.stack([taps, taps[::-1], taps[..., ::-1], taps[::-1, ..., ::-1]])
    return sets.transpose(2, 1, 4, 0, 3).reshape(TAPS, TAPS * TAPS, 4, 1, channels)


def local(
    image,
    offsets,
    conv1_weight,
    conv2_weight,
    norm1_gain,
    norm1_bias,
    norm2_gain,
    norm2_bias,
    head_weight,
    head_bias,
):
    groups = lax.axis_size("patch")
    spaces = lax.axis_size("space")
    slab_rows, band_rows, width = image.shape
    channels = norm1_gain.shape[0]
    classes = head_weight.shape[0]
    rows = band_rows * spaces
    hidden_rows = band_rows + TAPS - 1
    block = slab_rows * band_rows

    windows = pl.pallas_call(
        cut_kernel,
        out_shape=jax.ShapeDtypeStruct((groups, spaces, block, PX), BF16),
        in_specs=[SMEM, VMEM],
        out_specs=VMEM,
        scratch_shapes=[pltpu.VMEM((block, width), F32)],
        name="cut",
    )(offsets, image)
    windows = windows.reshape(groups * spaces, block, PX)
    gathered = lax.all_to_all(windows, ("patch", "space"), 0, 0, tiled=True)

    w1 = mirrored(conv1_weight, channels)
    w1 = jnp.pad(w1, ((0, 0), (0, 16 - TAPS * TAPS), (0, 0), (0, 0), (0, 0)))
    w1 = jnp.broadcast_to(w1, (TAPS, 16, 4, hidden_rows, channels))
    w1 = w1.reshape(TAPS, 16, 4 * hidden_rows * channels)
    out_lanes = ZG * band_rows * channels
    cells = PZ // ZG * PX
    conv, stats = pl.pallas_call(
        functools.partial(main_kernel, spaces, slab_rows, band_rows),
        out_shape=(
            jax.ShapeDtypeStruct((4, cells, out_lanes), F32),
            jax.ShapeDtypeStruct((spaces, 8, out_lanes), F32),
        ),
        in_specs=[SMEM] + [VMEM] * 5,
        out_specs=(VMEM, VMEM),
        scratch_shapes=[
            pltpu.VMEM((groups * spaces * block, PX), F32),
            pltpu.VMEM((PZ, (rows + 4) * 16, PX), F32),
            pltpu.VMEM((rows * 16, rows * 16), F32),
            pltpu.VMEM((4, cells, ZI * hidden_rows * channels), BF16),
            pltpu.VMEM((TAPS, ZI * hidden_rows * channels, out_lanes), BF16),
            pltpu.VMEM((8, out_lanes), F32),
        ],
        name="main",
    )(
        offsets,
        gathered,
        w1,
        conv2_weight,
        norm1_gain.reshape(1, channels),
        norm1_bias.reshape(1, channels),
    )
    stats = lax.all_to_all(stats, "space", 0, 0, tiled=True)
    averaged = pl.pallas_call(
        functools.partial(head_kernel, float(PZ * rows * PX), band_rows),
        out_shape=jax.ShapeDtypeStruct((PZ * classes * band_rows, PX), F32),
        in_specs=[VMEM] * 5 + [SMEM],
        out_specs=VMEM,
        name="head",
    )(
        conv,
        stats,
        norm2_gain.reshape(1, channels),
        norm2_bias.reshape(1, channels),
        head_weight,
        head_bias,
    )
    parts = lax.all_gather(averaged, "patch", axis=0, tiled=False)
    return pl.pallas_call(
        functools.partial(place_kernel, spaces),
        out_shape=jax.ShapeDtypeStruct((slab_rows, classes, band_rows, width), F32),
        in_specs=[SMEM, VMEM],
        out_specs=VMEM,
        scratch_shapes=[
            pltpu.VMEM((groups, (2 * slab_rows + PZ) * classes * band_rows, PX), F32)
        ],
        name="place",
    )(offsets, parts)


def solution(mesh):
    return jax.shard_map(
        local,
        mesh=mesh,
        in_specs=(P("patch", "space", None), P(), P(), P(), P(), P(), P(), P(), P(), P()),
        out_specs=P("patch", None, "space", None),
        check_vma=False,
    )
```

```python
import functools
import math

import jax
import jax.numpy as jnp
from jax import lax
from jax.experimental import pallas as pl
from jax.experimental.pallas import tpu as pltpu
from jax.sharding import PartitionSpec as P

PX = 128
PZ = 16
TAPS = 3
ZG = 4
ZI = ZG + TAPS - 1
F32 = jnp.float32
BF16 = jnp.bfloat16
HI = lax.Precision.HIGHEST
CONTRACT_FIRST = (((0,), (0,)), ((), ()))
CONTRACT_LAST = (((1,), (1,)), ((), ()))
VMEM = pl.BlockSpec(memory_space=pltpu.VMEM)
SMEM = pl.BlockSpec(memory_space=pltpu.SMEM)


def iota(shape, dim):
    return lax.broadcasted_iota(jnp.int32, shape, dim)


def repeat_matrix(channels, lanes, dtype):
    shape = (channels, lanes)
    return (iota(shape, 0) == iota(shape, 1) % channels).astype(dtype)


def cut_kernel(offsets_ref, image_ref, out_ref, rows_ref):
    slab_rows, band_rows, width = image_ref.shape
    for z in range(slab_rows):
        rows_ref[z * band_rows : (z + 1) * band_rows, :] = image_ref[z].astype(F32)
    rows = rows_ref[...]
    for item in range(out_ref.shape[0]):
        shift = lax.rem(width - offsets_ref[1, item], width)
        window = pltpu.roll(rows, shift, 1)[:, :PX].astype(BF16)
        for space in range(out_ref.shape[1]):
            out_ref[item, space] = window


def tap_rows(offsets_ref, gathered_ref, cells_ref, taps_ref, slab_rows, band_rows, spaces):
    block = slab_rows * band_rows
    devices = gathered_ref.shape[0]
    for device in range(devices):
        cells_ref[device * block : (device + 1) * block, :] = gathered_ref[device].astype(F32)
    taps_ref[...] = jnp.zeros_like(taps_ref)
    rows = band_rows * spaces
    for z in range(PZ):
        taps_ref[z, pl.ds(32 + 15, rows, stride=16), :] = jnp.ones((rows, PX), F32)
    item = lax.axis_index("patch")
    start_z = offsets_ref[0, item]
    lane = iota((spaces, PX), 1)
    for z in range(PZ):
        deep = start_z + z
        slab = lax.div(deep, slab_rows)
        base = slab * (spaces * block) + (deep - slab * slab_rows) * band_rows
        for y in range(band_rows):
            line = cells_ref[pl.ds(base + y, spaces, stride=block), :]
            before = jnp.where(lane == 0, 0.0, pltpu.roll(line, 1, 1))
            after = jnp.where(lane == PX - 1, 0.0, pltpu.roll(line, PX - 1, 1))
            for a in range(TAPS):
                at = z + 1 - a
                if 0 <= at < PZ:
                    for c, value in enumerate((before, line, after)):
                        first = 32 + 16 * y + a * TAPS + c
                        taps_ref[at, pl.ds(first, spaces, stride=16 * band_rows), :] = value


def first_moments(taps_ref, gram_ref, weights, rows):
    cells = [taps_ref[z, 32 : 32 + 16 * rows, :].astype(BF16) for z in range(PZ)]
    cells = jnp.concatenate(cells, axis=1)
    gram_ref[...] = lax.dot_general(cells, cells, CONTRACT_LAST, preferred_element_type=F32)

    def block(y, delta):
        lane = 16 * (y + delta)
        tile = lane // 128 * 128
        value = gram_ref[16 * y : 16 * y + 16, tile : tile + 128]
        return pltpu.roll(value, (tile + 128 - lane) % 128, 1) if lane != tile else value

    def total(values):
        values = list(values)
        while len(values) > 1:
            values = [
                values[i] + values[i + 1] if i + 1 < len(values) else values[i]
                for i in range(0, len(values), 2)
            ]
        return jnp.where(iota((16, 128), 1) < 16, values[0], 0.0)

    head, tail = total([block(0, 0)]), total([block(rows - 1, 0)])
    near = total([block(y, 0) for y in range(rows)])
    next1 = 2.0 * total([block(y, 1) for y in range(rows - 1)])
    next2 = 2.0 * total([block(y, 2) for y in range(rows - 2)])
    diag = (near - tail, near, near - head)
    move = lambda value, k: pltpu.roll(value, 16 * k, 1) if k else value
    form = jnp.concatenate(
        [
            diag[0] + move(next1, 1) + move(next2, 2),
            move(diag[1], 1) + move(next1, 2),
            move(diag[2], 2),
            diag[0] + move(diag[1], 1) + move(diag[2], 2),
        ],
        axis=0,
    )[:, :48]
    product = jnp.dot(form, weights, precision=HI, preferred_element_type=F32)
    squares = jnp.sum(product[:48] * weights, axis=0, keepdims=True)
    return product[63:64], squares


def prep_kernel(
    band_rows,
    w1_ref,
    w2_ref,
    gain1_ref,
    bias1_ref,
    gain2_ref,
    bias2_ref,
    head_ref,
    head_bias_ref,
    flat_ref,
    full_ref,
    wide_ref,
    params1_ref,
    params2_ref,
    heads_ref,
    bias_ref,
):
    channels = gain1_ref.shape[1]
    classes = head_ref.shape[0]
    hidden_rows = band_rows + TAPS - 1
    in_rows = hidden_rows + TAPS - 1

    width = flat_ref.shape[1]
    repeat = repeat_matrix(channels, width, BF16)
    taps = [
        jnp.dot(w1_ref[t], repeat, preferred_element_type=F32) for t in range(TAPS * TAPS)
    ]
    mirror = iota((1, width), 1) // (hidden_rows * channels)
    flat_ref[...] = jnp.zeros_like(flat_ref)
    for b in range(TAPS):
        for a in range(TAPS):
            one, two = taps[a * TAPS + b], taps[(TAPS - 1 - a) * TAPS + b]
            for c in range(TAPS):
                d = TAPS - 1 - c
                row = jnp.where(
                    mirror < 2,
                    jnp.where(mirror == 0, one[c : c + 1], two[c : c + 1]),
                    jnp.where(mirror == 2, one[d : d + 1], two[d : d + 1]),
                )
                at = 16 * b + a * TAPS + c
                flat_ref[at : at + 1, :] = row
    lane_row = iota((16, width), 1) // channels % hidden_rows
    for yi in range(in_rows):
        piece = jnp.zeros((16, width), F32)
        for b in range(TAPS):
            if 0 <= yi - b < hidden_rows:
                piece = jnp.where(lane_row == yi - b, flat_ref[16 * b : 16 * b + 16, :], piece)
        full_ref[16 * yi : 16 * yi + 16, :] = piece.astype(BF16)

    lanes = ZG * band_rows * channels
    spread = repeat_matrix(channels, lanes, BF16)
    taps = [
        lax.dot_general(w2_ref[t], spread, CONTRACT_FIRST, preferred_element_type=F32)
        for t in range(TAPS * TAPS)
    ]
    group = iota((TAPS * channels, lanes), 1) // channels
    for zi in range(ZI):
        for yi in range(hidden_rows):
            piece = jnp.zeros((TAPS * channels, lanes), F32)
            for zo in range(ZG):
                for yo in range(band_rows):
                    a, b = zi - zo, yi - yo
                    if 0 <= a < TAPS and 0 <= b < TAPS:
                        piece = jnp.where(group == zo * band_rows + yo, taps[a * TAPS + b], piece)
            piece = piece.astype(BF16)
            at = (zi * hidden_rows + yi) * channels
            for c in range(TAPS):
                wide_ref[c, at : at + channels, :] = piece[c * channels : (c + 1) * channels]

    rest = jnp.zeros((8 - classes - 4, channels), F32)
    rows = jnp.concatenate(
        [
            gain1_ref[...],
            bias1_ref[...],
            gain2_ref[...],
            bias2_ref[...],
            head_ref[...].astype(F32),
            rest,
        ],
        axis=0,
    )
    spread = repeat_matrix(channels, width, F32)
    rows = jnp.dot(rows, spread, precision=HI, preferred_element_type=F32)
    params1_ref[...] = rows
    params2_ref[...] = jnp.concatenate([rows[2:4, :lanes], rows[:6, :lanes]], axis=0)

    per_z = classes * band_rows
    shape = (ZG * per_z, lanes)
    row_z = iota(shape, 0) // per_z
    row_k = iota(shape, 0) // band_rows % classes
    row_y = iota(shape, 0) % band_rows
    full = jnp.zeros(shape, F32)
    for k in range(classes):
        full = jnp.where(row_k == k, rows[4 + k : 5 + k, :lanes], full)
    lane_z = iota(shape, 1) // (band_rows * channels)
    lane_y = iota(shape, 1) // channels % band_rows
    for f, z in enumerate((row_z, ZG - 1 - row_z)):
        heads_ref[f] = jnp.where((lane_z == z) & (lane_y == row_y), full, 0.0).astype(BF16)
    row_k = iota(bias_ref.shape, 0) // band_rows % classes
    bias = jnp.zeros(bias_ref.shape, F32)
    for k in range(classes):
        bias = jnp.where(row_k == k, head_bias_ref[k], bias)
    bias_ref[...] = bias


def main_kernel(
    spaces,
    slab_rows,
    band_rows,
    offsets_ref,
    gathered_ref,
    flat_ref,
    full_ref,
    w2t_ref,
    params_ref,
    conv_ref,
    stats_ref,
    cells_ref,
    taps_ref,
    gram_ref,
    wide_ref,
    sums_ref,
):
    rows = band_rows * spaces
    hidden_rows = band_rows + TAPS - 1
    in_rows = hidden_rows + TAPS - 1
    width = flat_ref.shape[1]
    step = width // 4
    channels = step // hidden_rows
    band = lax.axis_index("space")
    tap_rows(offsets_ref, gathered_ref, cells_ref, taps_ref, slab_rows, band_rows, spaces)

    first, second = first_moments(taps_ref, gram_ref, flat_ref[...], rows)
    count = float(PZ * rows * PX)
    mean = first / count
    variance = second / count - mean * mean
    lane_row = iota((1, width), 1) // channels % hidden_rows
    y = band * band_rows - 1 + lane_row
    inside = (y >= 0) & (y < rows)
    scale = lax.rsqrt(variance + 1e-05) * params_ref[0:1]
    shift = jnp.where(inside, params_ref[1:2] - mean * scale, 0.0)
    scale = jnp.where(inside, scale, 0.0)

    out_lanes = conv_ref.shape[2]
    groups = PZ // ZG
    empty = jnp.zeros((PX, step), BF16)
    for f in range(4):
        for g, j in ((0, 0), (groups - 1, ZI - 1)):
            at = (ZI - 1 - j if f % 2 else j) * step
            wide_ref[f, g * PX : (g + 1) * PX, at : at + step] = empty
    start = pl.multiple_of(band * (16 * band_rows), 16)
    weights = full_ref[...]
    for z in range(PZ):
        cells = taps_ref[z, pl.ds(start, in_rows * 16), :].astype(BF16)
        value = lax.dot_general(cells, weights, CONTRACT_FIRST, preferred_element_type=F32)
        value = value * scale + shift
        value = jnp.maximum(value, 0.01 * value).astype(BF16)
        for g in range(groups):
            j = z + 1 - ZG * g
            if 0 <= j < ZI:
                for f in range(4):
                    at = (ZI - 1 - j if f % 2 else j) * step
                    wide_ref[f, g * PX : (g + 1) * PX, at : at + step] = value[
                        :, f * step : (f + 1) * step
                    ]

    x = iota((groups * PX, out_lanes), 0) % PX
    for f in range(4):
        cells = wide_ref[f]
        parts = [
            jnp.dot(cells, w2t_ref[c], preferred_element_type=F32) for c in range(TAPS)
        ]
        before, after = (parts[2], parts[0]) if f >= 2 else (parts[0], parts[2])
        value = (
            parts[1]
            + jnp.where(x == 0, 0.0, pltpu.roll(before, 1, 0))
            + jnp.where(x == PX - 1, 0.0, pltpu.roll(after, groups * PX - 1, 0))
        )
        conv_ref[f] = value
        sums_ref[2 * f : 2 * f + 1, :] = jnp.sum(value, axis=0, keepdims=True)
        sums_ref[2 * f + 1 : 2 * f + 2, :] = jnp.sum(value * value, axis=0, keepdims=True)
    sums = sums_ref[...]
    for space in range(spaces):
        stats_ref[space] = sums


def head_kernel(count, channels, conv_ref, stats_ref, params_ref, heads_ref, bias_ref, out_ref):
    lanes = conv_ref.shape[2]
    per_group = heads_ref.shape[1]
    sums = stats_ref[0]
    for space in range(1, stats_ref.shape[0]):
        sums = sums + stats_ref[space]
    reach = lanes // 2
    while reach >= channels:
        sums = sums + pltpu.roll(sums, reach, 1)
        reach //= 2
    groups = conv_ref.shape[1] // PX
    totals = [None] * groups
    for f in range(4):
        mean = sums[2 * f : 2 * f + 1] / count
        variance = sums[2 * f + 1 : 2 * f + 2] / count - mean * mean
        scale = lax.rsqrt(variance + 1e-05) * params_ref[0:1]
        shift = params_ref[1:2] - mean * scale
        for g in range(groups):
            value = conv_ref[f, g * PX : (g + 1) * PX, :] * scale + shift
            value = jnp.maximum(value, 0.01 * value).astype(BF16)
            logits = lax.dot_general(
                heads_ref[f % 2], value, CONTRACT_LAST, preferred_element_type=F32
            )
            totals[g] = logits if totals[g] is None else totals[g] + logits
    for g in range(groups):
        out_ref[g * per_group : (g + 1) * per_group, :] = totals[g] * 0.25 + bias_ref[...]


def place_kernel(spaces, offsets_ref, parts_ref, out_ref, pad_ref):
    slab_rows, classes, band_rows, width = out_ref.shape
    patch_rows = band_rows * spaces
    per_z = classes * band_rows
    count = slab_rows * per_z
    slab = lax.axis_index("patch") * slab_rows
    band = lax.axis_index("space") * band_rows
    shape = (count, width)
    z = slab + iota(shape, 0) // per_z
    x = iota(shape, 1)
    y = (band + iota(shape, 0) % band_rows).astype(F32) - (patch_rows - 1) / 2.0
    across = y * y * (1.0 / (2.0 * (patch_rows / 8.0) ** 2))
    blended = jnp.zeros(shape, F32)
    coverage = jnp.zeros(shape, F32)
    for item in range(parts_ref.shape[0]):
        pad_ref[item, count : count + PZ * per_z, :] = parts_ref[item].astype(F32)
        start_z, start_x = offsets_ref[0, item], offsets_ref[1, item]
        first = jnp.clip(slab - start_z, -slab_rows, PZ) * per_z + count
        part = pad_ref[item, pl.ds(first, count), :]
        part = jnp.concatenate([part, jnp.zeros((count, width - PX), F32)], axis=1)
        part = pltpu.roll(part, start_x, 1)
        rel_z, rel_x = z - start_z, x - start_x
        inside = (rel_z >= 0) & (rel_z < PZ) & (rel_x >= 0) & (rel_x < PX)
        far_z = rel_z.astype(F32) - (PZ - 1) / 2.0
        far_x = rel_x.astype(F32) - (PX - 1) / 2.0
        power = (
            across
            + far_z * far_z * (1.0 / (2.0 * (PZ / 8.0) ** 2))
            + far_x * far_x * (1.0 / (2.0 * (PX / 8.0) ** 2))
        )
        weight = jnp.where(inside, jnp.exp(-power), 0.0)
        blended = blended + jnp.where(inside, part * weight, 0.0)
        coverage = coverage + weight
    value = blended / jnp.maximum(coverage, 0.1)
    for z in range(slab_rows):
        for k in range(classes):
            at = z * per_z + k * band_rows
            out_ref[z, k] = value[at : at + band_rows]


def in_vmem(value):
    return pltpu.with_memory_space_constraint(value, pltpu.VMEM)


def in_hbm(value):
    return pltpu.with_memory_space_constraint(value, pltpu.HBM)


def local(
    image,
    offsets,
    conv1_weight,
    conv2_weight,
    norm1_gain,
    norm1_bias,
    norm2_gain,
    norm2_bias,
    head_weight,
    head_bias,
):
    groups = lax.axis_size("patch")
    spaces = lax.axis_size("space")
    slab_rows, band_rows, width = image.shape
    channels = norm1_gain.shape[0]
    classes = head_weight.shape[0]
    rows = band_rows * spaces
    hidden_rows = band_rows + TAPS - 1
    in_rows = hidden_rows + TAPS - 1
    block = slab_rows * band_rows
    lanes1 = 4 * hidden_rows * channels
    lanes2 = ZG * band_rows * channels
    depth2 = ZI * hidden_rows * channels
    cells = PZ // ZG * PX
    per_z = classes * band_rows
    corners = in_hbm(offsets.T)

    windows = pl.pallas_call(
        cut_kernel,
        out_shape=jax.ShapeDtypeStruct((groups, spaces, block, PX), BF16),
        in_specs=[SMEM, VMEM],
        out_specs=VMEM,
        scratch_shapes=[pltpu.VMEM((block, width), F32)],
        name="cut",
    )(corners, image)
    windows = windows.reshape(groups * spaces, block, PX)
    gathered = lax.all_to_all(windows, ("patch", "space"), 0, 0, tiled=True)

    flat, full, w2t, params1, params2, heads, bias = pl.pallas_call(
        functools.partial(prep_kernel, band_rows),
        out_shape=(
            pltpu.VMEM((TAPS * 16, lanes1), F32),
            pltpu.VMEM((in_rows * 16, lanes1), BF16),
            pltpu.VMEM((TAPS, depth2, lanes2), BF16),
            pltpu.VMEM((8, lanes1), F32),
            pltpu.VMEM((8, lanes2), F32),
            pltpu.VMEM((2, ZG * per_z, lanes2), BF16),
            pltpu.VMEM((ZG * per_z, PX), F32),
        ),
        in_specs=[VMEM] * 7 + [SMEM],
        out_specs=(VMEM,) * 7,
        name="prep",
    )(
        in_hbm(conv1_weight.transpose(0, 2, 1)),
        in_hbm(conv2_weight),
        in_hbm(norm1_gain.reshape(1, channels)),
        in_hbm(norm1_bias.reshape(1, channels)),
        in_hbm(norm2_gain.reshape(1, channels)),
        in_hbm(norm2_bias.reshape(1, channels)),
        in_hbm(head_weight),
        in_hbm(head_bias),
    )
    scratch = (
        ((groups * spaces * block, PX), F32),
        ((PZ, (rows + 4) * 16, PX), F32),
        ((rows * 16, rows * 16), F32),
        ((4, cells, depth2), BF16),
        ((8, lanes2), F32),
    )
    size = sum(math.prod(shape) * jnp.dtype(kind).itemsize for shape, kind in scratch)
    conv, stats = pl.pallas_call(
        functools.partial(main_kernel, spaces, slab_rows, band_rows),
        out_shape=(
            pltpu.VMEM((4, cells, lanes2), F32),
            pltpu.VMEM((spaces, 8, lanes2), F32),
        ),
        in_specs=[SMEM] + [VMEM] * 5,
        out_specs=(VMEM, VMEM),
        scratch_shapes=[pltpu.VMEM(shape, kind) for shape, kind in scratch],
        compiler_params=pltpu.CompilerParams(vmem_limit_bytes=min(2 * size + (16 << 20), 52 << 20)),
        name="main",
    )(
        corners,
        in_vmem(gathered),
        in_vmem(flat),
        in_vmem(full),
        in_vmem(w2t),
        in_vmem(params1),
    )
    stats = lax.all_to_all(stats, "space", 0, 0, tiled=True)
    averaged = pl.pallas_call(
        functools.partial(head_kernel, float(PZ * rows * PX), channels),
        out_shape=pltpu.VMEM((PZ * per_z, PX), F32),
        in_specs=[VMEM] * 5,
        out_specs=VMEM,
        compiler_params=pltpu.CompilerParams(vmem_limit_bytes=8 << 20),
        name="head",
    )(in_vmem(conv), in_vmem(stats), in_vmem(params2), in_vmem(heads), in_vmem(bias))
    parts = lax.all_gather(averaged, "patch", axis=0, tiled=False)
    return pl.pallas_call(
        functools.partial(place_kernel, spaces),
        out_shape=jax.ShapeDtypeStruct((slab_rows, classes, band_rows, width), F32),
        in_specs=[SMEM, VMEM],
        out_specs=VMEM,
        scratch_shapes=[pltpu.VMEM((groups, (2 * slab_rows + PZ) * per_z, PX), F32)],
        compiler_params=pltpu.CompilerParams(vmem_limit_bytes=8 << 20),
        name="place",
    )(corners, in_vmem(parts))


def solution(mesh):
    return jax.shard_map(
        local,
        mesh=mesh,
        in_specs=(P("patch", "space", None), P(), P(), P(), P(), P(), P(), P(), P(), P()),
        out_specs=P("patch", None, "space", None),
        check_vma=False,
    )
```

```python
import functools
import math

import jax
import jax.numpy as jnp
from jax import lax
from jax.experimental import pallas as pl
from jax.experimental.pallas import tpu as pltpu
from jax.sharding import PartitionSpec as P

PX = 128
PZ = 16
TAPS = 3
ZG = 4
ZI = ZG + TAPS - 1
F32 = jnp.float32
BF16 = jnp.bfloat16
HI = lax.Precision.HIGHEST
CONTRACT_FIRST = (((0,), (0,)), ((), ()))
CONTRACT_LAST = (((1,), (1,)), ((), ()))
VMEM = pl.BlockSpec(memory_space=pltpu.VMEM)
SMEM = pl.BlockSpec(memory_space=pltpu.SMEM)


def iota(shape, dim):
    return lax.broadcasted_iota(jnp.int32, shape, dim)


def repeat_matrix(channels, lanes, dtype):
    shape = (channels, lanes)
    return (iota(shape, 0) == iota(shape, 1) % channels).astype(dtype)


def cut_kernel(offsets_ref, image_ref, out_ref, rows_ref):
    slab_rows, band_rows, width = image_ref.shape
    for z in range(slab_rows):
        rows_ref[z * band_rows : (z + 1) * band_rows, :] = image_ref[z].astype(F32)
    rows = rows_ref[...]
    items = offsets_ref.shape[1]
    spaces = out_ref.shape[0] // items
    for item in range(items):
        shift = lax.rem(width - offsets_ref[1, item], width)
        window = pltpu.roll(rows, shift, 1)[:, :PX].astype(BF16)
        for space in range(spaces):
            out_ref[item * spaces + space] = window


def prep_kernel(
    spaces,
    slab_rows,
    band_rows,
    offsets_ref,
    w1_ref,
    w2_ref,
    gain1_ref,
    bias1_ref,
    gain2_ref,
    bias2_ref,
    head_ref,
    head_bias_ref,
    every_ref,
    own_ref,
    wide_ref,
    params_ref,
    heads_ref,
    bias_ref,
    weights_ref,
    corner_ref,
    flat_ref,
):
    channels = gain1_ref.shape[1]
    classes = head_ref.shape[0]
    rows = band_rows * spaces
    hidden_rows = band_rows + TAPS - 1
    step = 4 * channels
    band = lax.axis_index("space")
    patch = lax.axis_index("patch")

    repeat = repeat_matrix(channels, step, BF16)
    taps = [
        jnp.dot(w1_ref[t], repeat, preferred_element_type=F32) for t in range(TAPS * TAPS)
    ]
    mirror = iota((1, step), 1) // channels
    flat_ref[...] = jnp.zeros_like(flat_ref)
    for b in range(TAPS):
        for a in range(TAPS):
            one, two = taps[a * TAPS + b], taps[(TAPS - 1 - a) * TAPS + b]
            for c in range(TAPS):
                d = TAPS - 1 - c
                row = jnp.where(
                    mirror < 2,
                    jnp.where(mirror == 0, one[c : c + 1], two[c : c + 1]),
                    jnp.where(mirror == 2, one[d : d + 1], two[d : d + 1]),
                )
                at = 16 * b + a * TAPS + c
                flat_ref[at : at + 1, :] = row
    flat = flat_ref[...]

    def row_of(shape):
        r = iota(shape, 0)
        return r % spaces * band_rows + r // spaces

    zeros = jnp.zeros((16, step), BF16)
    for y in range(rows):
        delta = row_of((rows, step)) - (y - 1)
        masks = [delta == b for b in range(TAPS)]
        for slot in range(TAPS * TAPS):
            piece = jnp.zeros((rows, step), F32)
            for b in range(TAPS):
                piece = jnp.where(masks[b], flat[16 * b + slot : 16 * b + slot + 1], piece)
            every_ref[slot * rows : (slot + 1) * rows, y * step : (y + 1) * step] = piece.astype(
                BF16
            )
        every_ref[TAPS * TAPS * rows :, y * step : (y + 1) * step] = zeros
    lanes = own_ref.shape[1]
    shape = (step, lanes)
    lane = iota(shape, 1)
    spread = iota(shape, 0) == lane // (hidden_rows * channels) * channels + lane % channels
    spread = jnp.dot(flat.astype(BF16), spread.astype(BF16), preferred_element_type=F32)
    shape = (rows, lanes)
    delta = row_of(shape) - iota(shape, 1) // channels % hidden_rows - (band * band_rows - 2)
    masks = [delta == b for b in range(TAPS)]
    for slot in range(TAPS * TAPS):
        piece = jnp.zeros(shape, F32)
        for b in range(TAPS):
            piece = jnp.where(masks[b], spread[16 * b + slot : 16 * b + slot + 1], piece)
        own_ref[slot * rows : (slot + 1) * rows, :] = piece.astype(BF16)
    own_ref[TAPS * TAPS * rows :, :] = jnp.zeros((16, lanes), BF16)

    lanes = ZG * band_rows * channels
    spread = repeat_matrix(channels, lanes, BF16)
    taps = [
        lax.dot_general(w2_ref[t], spread, CONTRACT_FIRST, preferred_element_type=F32)
        for t in range(TAPS * TAPS)
    ]
    group = iota((TAPS * channels, lanes), 1) // channels
    for zi in range(ZI):
        for yi in range(hidden_rows):
            piece = jnp.zeros((TAPS * channels, lanes), F32)
            for zo in range(ZG):
                for yo in range(band_rows):
                    a, b = zi - zo, yi - yo
                    if 0 <= a < TAPS and 0 <= b < TAPS:
                        piece = jnp.where(group == zo * band_rows + yo, taps[a * TAPS + b], piece)
            piece = piece.astype(BF16)
            at = (zi * hidden_rows + yi) * channels
            for c in range(TAPS):
                wide_ref[c, at : at + channels, :] = piece[c * channels : (c + 1) * channels]

    table = jnp.concatenate(
        [
            gain1_ref[...],
            bias1_ref[...],
            gain2_ref[...],
            bias2_ref[...],
            head_ref[...].astype(F32),
            jnp.zeros((8 - classes - 4, channels), F32),
        ],
        axis=0,
    )
    spread = repeat_matrix(channels, lanes, F32)
    table = jnp.dot(table, spread, precision=HI, preferred_element_type=F32)
    params_ref[...] = table[:, :step]

    per_z = classes * band_rows
    shape = (ZG * per_z, lanes)
    row_z = iota(shape, 0) // per_z
    row_k = iota(shape, 0) // band_rows % classes
    row_y = iota(shape, 0) % band_rows
    full = jnp.zeros(shape, F32)
    for k in range(classes):
        full = jnp.where(row_k == k, table[4 + k : 5 + k], full)
    lane_z = iota(shape, 1) // (band_rows * channels)
    lane_y = iota(shape, 1) // channels % band_rows
    for f, z in enumerate((row_z, ZG - 1 - row_z)):
        heads_ref[f] = jnp.where((lane_z == z) & (lane_y == row_y), full, 0.0).astype(BF16)
    row_k = iota(bias_ref.shape, 0) // band_rows % classes
    bias = jnp.zeros(bias_ref.shape, F32)
    for k in range(classes):
        bias = jnp.where(row_k == k, head_bias_ref[k], bias)
    bias_ref[...] = bias

    items, count, width = weights_ref.shape
    shape = (count, width)
    slab = patch * slab_rows
    z = slab + iota(shape, 0) // per_z
    x = iota(shape, 1)
    y = (band * band_rows + iota(shape, 0) % band_rows).astype(F32) - (rows - 1) / 2.0
    across = y * y * (1.0 / (2.0 * (rows / 8.0) ** 2))
    shape = corner_ref.shape
    corner_row, corner_lane = iota(shape, 0), iota(shape, 1)
    own_z = jnp.where(corner_lane == 0, offsets_ref[0, patch], 0)
    corners = jnp.where(corner_row == items, own_z, 0)
    coverage = jnp.zeros((count, width), F32)
    weights = []
    for k in range(items):
        item = jnp.bitwise_xor(patch, k)
        start_z, start_x = offsets_ref[0, item], offsets_ref[1, item]
        first = jnp.clip(slab - start_z, -slab_rows, PZ) * per_z + count
        values = jnp.where(corner_lane == 0, first, start_x)
        corners = jnp.where((corner_row == k) & (corner_lane < 2), values, corners)
        rel_z, rel_x = z - start_z, x - start_x
        inside = (rel_z >= 0) & (rel_z < PZ) & (rel_x >= 0) & (rel_x < PX)
        far_z = rel_z.astype(F32) - (PZ - 1) / 2.0
        far_x = rel_x.astype(F32) - (PX - 1) / 2.0
        power = (
            across
            + far_z * far_z * (1.0 / (2.0 * (PZ / 8.0) ** 2))
            + far_x * far_x * (1.0 / (2.0 * (PX / 8.0) ** 2))
        )
        weight = jnp.where(inside, jnp.exp(-power), 0.0)
        weights.append(weight)
        coverage = coverage + weight
    share = 1.0 / jnp.maximum(coverage, 0.1)
    for k in range(items):
        weights_ref[k] = weights[k] * share
    corner_ref[...] = corners


def tap_rows(start_z, gathered_ref, cells_ref, taps_ref, slab_rows, band_rows, spaces):
    block = slab_rows * band_rows
    for device in range(gathered_ref.shape[0]):
        cells_ref[device * block : (device + 1) * block, :] = gathered_ref[device].astype(F32)
    rows = band_rows * spaces
    lane = iota((spaces, PX), 1)
    empty = jnp.zeros((rows, PX), F32)
    for c in range(TAPS):
        taps_ref[0, c * rows : (c + 1) * rows, :] = empty
        at = (TAPS * (TAPS - 1) + c) * rows
        taps_ref[PZ - 1, at : at + rows, :] = empty
    ones = jnp.ones((16, PX), F32)
    for z in range(PZ):
        taps_ref[z, TAPS * TAPS * rows :, :] = ones
        deep = start_z + z
        slab = lax.div(deep, slab_rows)
        base = slab * (spaces * block) + (deep - slab * slab_rows) * band_rows
        for y in range(band_rows):
            line = cells_ref[pl.ds(base + y, spaces, stride=block), :]
            before = jnp.where(lane == 0, 0.0, pltpu.roll(line, 1, 1))
            after = jnp.where(lane == PX - 1, 0.0, pltpu.roll(line, PX - 1, 1))
            for a in range(TAPS):
                at = z + 1 - a
                if 0 <= at < PZ:
                    for c, value in enumerate((before, line, after)):
                        first = (a * TAPS + c) * rows + y * spaces
                        taps_ref[at, first : first + spaces, :] = value


def first_moments(taps_ref, every_ref, rows, step):
    cells = [taps_ref[z].astype(BF16) for z in range(PZ)]
    cells = jnp.concatenate(cells, axis=1)
    gram = lax.dot_general(cells, cells, CONTRACT_LAST, preferred_element_type=F32)
    high = gram.astype(BF16)
    left = gram - high.astype(F32)
    middle = left.astype(BF16)
    low = (left - middle.astype(F32)).astype(BF16)
    first = jnp.zeros((1, step), F32)
    second = jnp.zeros((1, step), F32)
    wide = 4 * step
    for at in range(0, rows * step, wide):
        weights = every_ref[:, at : at + wide]
        product = (
            jnp.dot(high, weights, preferred_element_type=F32)
            + jnp.dot(middle, weights, preferred_element_type=F32)
            + jnp.dot(low, weights, preferred_element_type=F32)
        )
        squares = jnp.sum(product * weights.astype(F32), axis=0, keepdims=True)
        ones = TAPS * TAPS * rows
        for lane in range(0, wide, step):
            first = first + product[ones : ones + 1, lane : lane + step]
            second = second + squares[:, lane : lane + step]
    return first, second


def spread_mirror(value, f, channels):
    value = jnp.where(iota(value.shape, 1) // channels == f, value, 0.0)
    reach = channels
    while reach < value.shape[1]:
        value = value + pltpu.roll(value, reach, 1)
        reach *= 2
    return value


def main_kernel(
    spaces,
    slab_rows,
    band_rows,
    channels,
    gathered_ref,
    corner_ref,
    every_ref,
    own_ref,
    w2t_ref,
    params_ref,
    conv_ref,
    stats_ref,
    cells_ref,
    taps_ref,
    wide_ref,
    sums_ref,
):
    rows = band_rows * spaces
    hidden_rows = band_rows + TAPS - 1
    step = hidden_rows * channels
    band = lax.axis_index("space")
    start_z = corner_ref[lax.axis_size("patch"), 0]
    tap_rows(start_z, gathered_ref, cells_ref, taps_ref, slab_rows, band_rows, spaces)

    first, second = first_moments(taps_ref, every_ref, rows, step)
    count = float(PZ * rows * PX)
    mean = first / count
    variance = second / count - mean * mean
    scale = lax.rsqrt(variance + 1e-05) * params_ref[0:1]
    shift = params_ref[1:2] - mean * scale
    table = jnp.concatenate([scale, shift, jnp.zeros((6, step), F32)], axis=0)
    y = band * band_rows - 1 + iota((8, step), 1) // channels
    inside = (y >= 0) & (y < rows)
    table = jnp.concatenate(
        [jnp.where(inside, spread_mirror(table, f, channels), 0.0) for f in range(4)], axis=1
    )
    scale, shift = table[0:1], table[1:2]

    out_lanes = conv_ref.shape[2]
    groups = PZ // ZG
    empty = jnp.zeros((PX, step), BF16)
    for f in range(4):
        for g, j in ((0, 0), (groups - 1, ZI - 1)):
            at = (ZI - 1 - j if f % 2 else j) * step
            wide_ref[f, g * PX : (g + 1) * PX, at : at + step] = empty
    weights = own_ref[...]
    for z in range(PZ):
        cells = taps_ref[z].astype(BF16)
        value = lax.dot_general(cells, weights, CONTRACT_FIRST, preferred_element_type=F32)
        value = value * scale + shift
        value = jnp.maximum(value, 0.01 * value).astype(BF16)
        for g in range(groups):
            j = z + 1 - ZG * g
            if 0 <= j < ZI:
                for f in range(4):
                    at = (ZI - 1 - j if f % 2 else j) * step
                    wide_ref[f, g * PX : (g + 1) * PX, at : at + step] = value[
                        :, f * step : (f + 1) * step
                    ]

    x = iota((groups * PX, out_lanes), 0) % PX
    for f in range(4):
        cells = wide_ref[f]
        parts = [
            jnp.dot(cells, w2t_ref[c], preferred_element_type=F32) for c in range(TAPS)
        ]
        before, after = (parts[2], parts[0]) if f >= 2 else (parts[0], parts[2])
        value = (
            parts[1]
            + jnp.where(x == 0, 0.0, pltpu.roll(before, 1, 0))
            + jnp.where(x == PX - 1, 0.0, pltpu.roll(after, groups * PX - 1, 0))
        )
        conv_ref[f] = value
        sums_ref[f : f + 1, :] = jnp.sum(value, axis=0, keepdims=True)
        sums_ref[f + 4 : f + 5, :] = jnp.sum(value * value, axis=0, keepdims=True)
    sums = sums_ref[...]
    lanes = 4 * channels
    sums = sum(sums[:, at : at + lanes] for at in range(0, out_lanes, lanes))
    reach = lanes // 2
    while reach >= channels:
        sums = sums + pltpu.roll(sums, reach, 1)
        reach //= 2
    mirror = iota((1, lanes), 1) // channels
    for kind in range(2):
        row = sums[4 * kind : 4 * kind + 1]
        for f in range(1, 4):
            row = jnp.where(mirror == f, sums[4 * kind + f : 4 * kind + f + 1], row)
        for space in range(spaces):
            stats_ref[space, kind : kind + 1, :] = row


def head_kernel(count, channels, conv_ref, stats_ref, params_ref, heads_ref, bias_ref, out_ref):
    lanes = conv_ref.shape[2]
    per_group = heads_ref.shape[1]
    sums = stats_ref[0]
    for space in range(1, stats_ref.shape[0]):
        sums = sums + stats_ref[space]
    mean = sums[0:1] / count
    variance = sums[1:2] / count - mean * mean
    scale = lax.rsqrt(variance + 1e-05) * params_ref[2:3]
    shift = params_ref[3:4] - mean * scale
    table = jnp.concatenate([scale, shift, jnp.zeros((6, 4 * channels), F32)], axis=0)
    groups = conv_ref.shape[1] // PX
    totals = [None] * groups
    for f in range(4):
        own = spread_mirror(table, f, channels)
        own = jnp.concatenate([own] * (lanes // own.shape[1]), axis=1)
        for g in range(groups):
            value = conv_ref[f, g * PX : (g + 1) * PX, :] * own[0:1] + own[1:2]
            value = jnp.maximum(value, 0.01 * value).astype(BF16)
            logits = lax.dot_general(
                heads_ref[f % 2], value, CONTRACT_LAST, preferred_element_type=F32
            )
            totals[g] = logits if totals[g] is None else totals[g] + logits
    for g in range(groups):
        out_ref[g * per_group : (g + 1) * per_group, :] = (
            totals[g] * 0.25 + bias_ref[...]
        ).astype(out_ref.dtype)


def place_kernel(items, corner_ref, weights_ref, *refs):
    parts, (out_ref, pad_ref) = refs[:items], refs[items:]
    slab_rows, classes, band_rows, width = out_ref.shape
    per_z = classes * band_rows
    count = slab_rows * per_z
    blended = jnp.zeros((count, width), F32)
    for k in range(items):
        pad_ref[k, count : count + PZ * per_z, :] = parts[k][...].astype(F32)
        part = pad_ref[k, pl.ds(corner_ref[k, 0], count), :]
        part = jnp.concatenate([part, jnp.zeros((count, width - PX), F32)], axis=1)
        part = pltpu.roll(part, corner_ref[k, 1], 1)
        weight = weights_ref[k]
        blended = blended + jnp.where(weight > 0, part * weight, 0.0)
    for z in range(slab_rows):
        for k in range(classes):
            at = z * per_z + k * band_rows
            out_ref[z, k] = blended[at : at + band_rows]


def in_vmem(value):
    return pltpu.with_memory_space_constraint(value, pltpu.VMEM)


def in_hbm(value):
    return pltpu.with_memory_space_constraint(value, pltpu.HBM)


def local(
    image,
    offsets,
    conv1_weight,
    conv2_weight,
    norm1_gain,
    norm1_bias,
    norm2_gain,
    norm2_bias,
    head_weight,
    head_bias,
):
    groups = lax.axis_size("patch")
    spaces = lax.axis_size("space")
    slab_rows, band_rows, width = image.shape
    channels = norm1_gain.shape[0]
    classes = head_weight.shape[0]
    rows = band_rows * spaces
    hidden_rows = band_rows + TAPS - 1
    block = slab_rows * band_rows
    step = 4 * channels
    lanes1 = 4 * hidden_rows * channels
    lanes2 = ZG * band_rows * channels
    depth1 = TAPS * TAPS * rows + 16
    depth2 = ZI * hidden_rows * channels
    cells = PZ // ZG * PX
    per_z = classes * band_rows
    corners = in_hbm(offsets.T)

    windows = pl.pallas_call(
        cut_kernel,
        out_shape=pltpu.VMEM((groups * spaces, block, PX), BF16),
        in_specs=[SMEM, VMEM],
        out_specs=VMEM,
        scratch_shapes=[pltpu.VMEM((block, width), F32)],
        name="cut",
    )(corners, image)
    gathered = lax.all_to_all(in_vmem(windows), ("patch", "space"), 0, 0, tiled=True)

    every, own, w2t, params, heads, bias, weights, corner = pl.pallas_call(
        functools.partial(prep_kernel, spaces, slab_rows, band_rows),
        out_shape=(
            pltpu.VMEM((depth1, rows * step), BF16),
            pltpu.VMEM((depth1, lanes1), BF16),
            pltpu.VMEM((TAPS, depth2, lanes2), BF16),
            pltpu.VMEM((8, step), F32),
            pltpu.VMEM((2, ZG * per_z, lanes2), BF16),
            pltpu.VMEM((ZG * per_z, PX), F32),
            pltpu.VMEM((groups, slab_rows * per_z, width), F32),
            pltpu.VMEM(((groups + 8) // 8 * 8, 128), jnp.int32),
        ),
        in_specs=[SMEM] + [VMEM] * 7 + [SMEM],
        out_specs=(VMEM,) * 8,
        scratch_shapes=[pltpu.VMEM((TAPS * 16, step), F32)],
        compiler_params=pltpu.CompilerParams(vmem_limit_bytes=16 << 20),
        name="prep",
    )(
        corners,
        in_hbm(conv1_weight.transpose(0, 2, 1)),
        in_hbm(conv2_weight),
        in_hbm(norm1_gain.reshape(1, channels)),
        in_hbm(norm1_bias.reshape(1, channels)),
        in_hbm(norm2_gain.reshape(1, channels)),
        in_hbm(norm2_bias.reshape(1, channels)),
        in_hbm(head_weight),
        in_hbm(head_bias),
    )
    scratch = (
        ((groups * spaces * block, PX), F32),
        ((PZ, depth1, PX), F32),
        ((4, cells, depth2), BF16),
        ((8, lanes2), F32),
    )
    size = sum(math.prod(shape) * jnp.dtype(kind).itemsize for shape, kind in scratch)
    conv, stats = pl.pallas_call(
        functools.partial(main_kernel, spaces, slab_rows, band_rows, channels),
        out_shape=(
            pltpu.VMEM((4, cells, lanes2), F32),
            pltpu.VMEM((spaces, 2, step), F32),
        ),
        in_specs=[VMEM] * 6,
        out_specs=(VMEM, VMEM),
        scratch_shapes=[pltpu.VMEM(shape, kind) for shape, kind in scratch],
        compiler_params=pltpu.CompilerParams(vmem_limit_bytes=min(2 * size + (16 << 20), 40 << 20)),
        name="main",
    )(
        in_vmem(gathered),
        in_vmem(corner),
        in_vmem(every),
        in_vmem(own),
        in_vmem(w2t),
        in_vmem(params),
    )
    stats = lax.all_to_all(stats, "space", 0, 0, tiled=True)
    averaged = pl.pallas_call(
        functools.partial(head_kernel, float(PZ * rows * PX), channels),
        out_shape=pltpu.VMEM((PZ * per_z, PX), BF16),
        in_specs=[VMEM] * 5,
        out_specs=VMEM,
        compiler_params=pltpu.CompilerParams(vmem_limit_bytes=8 << 20),
        name="head",
    )(in_vmem(conv), in_vmem(stats), in_vmem(params), in_vmem(heads), in_vmem(bias))
    parts = [averaged] + [
        lax.ppermute(averaged, "patch", [(i, i ^ k) for i in range(groups)])
        for k in range(1, groups)
    ]
    return pl.pallas_call(
        functools.partial(place_kernel, groups),
        out_shape=jax.ShapeDtypeStruct((slab_rows, classes, band_rows, width), F32),
        in_specs=[VMEM] * (2 + groups),
        out_specs=VMEM,
        scratch_shapes=[pltpu.VMEM((groups, (2 * slab_rows + PZ) * per_z, PX), F32)],
        compiler_params=pltpu.CompilerParams(vmem_limit_bytes=8 << 20),
        name="place",
    )(in_vmem(corner), in_vmem(weights), *[in_vmem(part) for part in parts])


def solution(mesh):
    return jax.shard_map(
        local,
        mesh=mesh,
        in_specs=(P("patch", "space", None), P(), P(), P(), P(), P(), P(), P(), P(), P()),
        out_specs=P("patch", None, "space", None),
        check_vma=False,
    )
```

```python
import functools
import math

import jax
import jax.numpy as jnp
from jax import lax
from jax.experimental import pallas as pl
from jax.experimental.pallas import tpu as pltpu
from jax.sharding import PartitionSpec as P

PX = 128
PZ = 16
TAPS = 3
ZG = 4
ZI = ZG + TAPS - 1
SLOTS = 16
LINE = TAPS * (PZ + 2) + 1
F32 = jnp.float32
BF16 = jnp.bfloat16
HI = lax.Precision.HIGHEST
CONTRACT_FIRST = (((0,), (0,)), ((), ()))
CONTRACT_LAST = (((1,), (1,)), ((), ()))
VMEM = pl.BlockSpec(memory_space=pltpu.VMEM)
SMEM = pl.BlockSpec(memory_space=pltpu.SMEM)


def iota(shape, dim):
    return lax.broadcasted_iota(jnp.int32, shape, dim)


def repeat_matrix(channels, lanes, dtype):
    shape = (channels, lanes)
    return (iota(shape, 0) == iota(shape, 1) % channels).astype(dtype)


def cut_kernel(offsets_ref, image_ref, out_ref, rows_ref):
    slab_rows, band_rows, width = image_ref.shape
    for z in range(slab_rows):
        rows_ref[z * band_rows : (z + 1) * band_rows, :] = image_ref[z].astype(F32)
    rows = rows_ref[...]
    items = offsets_ref.shape[1]
    spaces = out_ref.shape[0] // items
    for item in range(items):
        shift = lax.rem(width - offsets_ref[1, item], width)
        window = pltpu.roll(rows, shift, 1)[:, :PX].astype(BF16)
        for space in range(spaces):
            out_ref[item * spaces + space] = window


def prep_kernel(
    spaces,
    slab_rows,
    band_rows,
    offsets_ref,
    w1_ref,
    w2_ref,
    gain1_ref,
    bias1_ref,
    gain2_ref,
    bias2_ref,
    head_ref,
    head_bias_ref,
    flat_ref,
    full_ref,
    wide_ref,
    params_ref,
    heads_ref,
    bias_ref,
    weights_ref,
    corner_ref,
    narrow_ref,
):
    channels = gain1_ref.shape[1]
    classes = head_ref.shape[0]
    rows = band_rows * spaces
    hidden_rows = band_rows + TAPS - 1
    step = 4 * channels
    band = lax.axis_index("space")
    patch = lax.axis_index("patch")

    repeat = repeat_matrix(channels, step, BF16)
    taps = [
        jnp.dot(w1_ref[t], repeat, preferred_element_type=F32) for t in range(TAPS * TAPS)
    ]
    mirror = iota((1, step), 1) // channels
    narrow_ref[...] = jnp.zeros_like(narrow_ref)
    for b in range(TAPS):
        for a in range(TAPS):
            one, two = taps[a * TAPS + b], taps[(TAPS - 1 - a) * TAPS + b]
            for c in range(TAPS):
                d = TAPS - 1 - c
                row = jnp.where(
                    mirror < 2,
                    jnp.where(mirror == 0, one[c : c + 1], two[c : c + 1]),
                    jnp.where(mirror == 2, one[d : d + 1], two[d : d + 1]),
                )
                at = SLOTS * b + a * TAPS + c
                narrow_ref[at : at + 1, :] = row
    lanes = flat_ref.shape[1]
    shape = (step, lanes)
    lane = iota(shape, 1)
    spread = iota(shape, 0) == lane // (hidden_rows * channels) * channels + lane % channels
    flat = jnp.dot(
        narrow_ref[...].astype(BF16), spread.astype(BF16), preferred_element_type=F32
    )
    flat_ref[...] = flat
    lane_row = iota((SLOTS, lanes), 1) // channels % hidden_rows
    for yi in range(hidden_rows + TAPS - 1):
        piece = jnp.zeros((SLOTS, lanes), F32)
        for b in range(TAPS):
            if 0 <= yi - b < hidden_rows:
                piece = jnp.where(lane_row == yi - b, flat[SLOTS * b : SLOTS * b + SLOTS], piece)
        full_ref[SLOTS * yi : SLOTS * yi + SLOTS, :] = piece.astype(BF16)

    lanes = ZG * band_rows * channels
    spread = repeat_matrix(channels, lanes, BF16)
    taps = [
        lax.dot_general(w2_ref[t], spread, CONTRACT_FIRST, preferred_element_type=F32)
        for t in range(TAPS * TAPS)
    ]
    group = iota((TAPS * channels, lanes), 1) // channels
    for zi in range(ZI):
        for yi in range(hidden_rows):
            piece = jnp.zeros((TAPS * channels, lanes), F32)
            for zo in range(ZG):
                for yo in range(band_rows):
                    a, b = zi - zo, yi - yo
                    if 0 <= a < TAPS and 0 <= b < TAPS:
                        piece = jnp.where(group == zo * band_rows + yo, taps[a * TAPS + b], piece)
            piece = piece.astype(BF16)
            at = (zi * hidden_rows + yi) * channels
            for c in range(TAPS):
                wide_ref[c, at : at + channels, :] = piece[c * channels : (c + 1) * channels]

    table = jnp.concatenate(
        [
            gain1_ref[...],
            bias1_ref[...],
            gain2_ref[...],
            bias2_ref[...],
            head_ref[...].astype(F32),
            jnp.zeros((8 - classes - 4, channels), F32),
        ],
        axis=0,
    )
    spread = repeat_matrix(channels, params_ref.shape[1], F32)
    table = jnp.dot(table, spread, precision=HI, preferred_element_type=F32)
    params_ref[...] = table
    table = table[:, :lanes]

    per_z = classes * band_rows
    shape = (ZG * per_z, lanes)
    row_z = iota(shape, 0) // per_z
    row_k = iota(shape, 0) // band_rows % classes
    row_y = iota(shape, 0) % band_rows
    full = jnp.zeros(shape, F32)
    for k in range(classes):
        full = jnp.where(row_k == k, table[4 + k : 5 + k], full)
    lane_z = iota(shape, 1) // (band_rows * channels)
    lane_y = iota(shape, 1) // channels % band_rows
    for f, z in enumerate((row_z, ZG - 1 - row_z)):
        heads_ref[f] = jnp.where((lane_z == z) & (lane_y == row_y), full, 0.0).astype(BF16)
    row_k = iota(bias_ref.shape, 0) // band_rows % classes
    bias = jnp.zeros(bias_ref.shape, F32)
    for k in range(classes):
        bias = jnp.where(row_k == k, head_bias_ref[k], bias)
    bias_ref[...] = bias

    items, count, width = weights_ref.shape
    shape = (count, width)
    slab = patch * slab_rows
    z = slab + iota(shape, 0) // per_z
    x = iota(shape, 1)
    y = (band * band_rows + iota(shape, 0) % band_rows).astype(F32) - (rows - 1) / 2.0
    across = y * y * (1.0 / (2.0 * (rows / 8.0) ** 2))
    shape = corner_ref.shape
    corner_row, corner_lane = iota(shape, 0), iota(shape, 1)
    own_z = jnp.where(corner_lane == 0, offsets_ref[0, patch], 0)
    corners = jnp.where(corner_row == items, own_z, 0)
    coverage = jnp.zeros((count, width), F32)
    weights = []
    for k in range(items):
        item = jnp.bitwise_xor(patch, k)
        start_z, start_x = offsets_ref[0, item], offsets_ref[1, item]
        first = jnp.clip(slab - start_z, -slab_rows, PZ) * per_z + count
        values = jnp.where(corner_lane == 0, first, start_x)
        corners = jnp.where((corner_row == k) & (corner_lane < 2), values, corners)
        rel_z, rel_x = z - start_z, x - start_x
        inside = (rel_z >= 0) & (rel_z < PZ) & (rel_x >= 0) & (rel_x < PX)
        far_z = rel_z.astype(F32) - (PZ - 1) / 2.0
        far_x = rel_x.astype(F32) - (PX - 1) / 2.0
        power = (
            across
            + far_z * far_z * (1.0 / (2.0 * (PZ / 8.0) ** 2))
            + far_x * far_x * (1.0 / (2.0 * (PX / 8.0) ** 2))
        )
        weight = jnp.where(inside, jnp.exp(-power), 0.0)
        weights.append(weight)
        coverage = coverage + weight
    share = 1.0 / jnp.maximum(coverage, 0.1)
    for k in range(items):
        weights_ref[k] = weights[k] * share
    corner_ref[...] = corners


def line_rows(start_z, gathered_ref, cells_ref, lines_ref, slab_rows, band_rows, spaces):
    block = slab_rows * band_rows
    pitch = block + 1
    for device in range(gathered_ref.shape[0]):
        cells_ref[device * pitch : device * pitch + block, :] = gathered_ref[device].astype(F32)
    lane = iota((spaces, PX), 1)
    empty = jnp.zeros((spaces, PX), F32)
    edge = jnp.zeros((LINE, PX), F32)
    last = band_rows * (spaces + 2) * LINE
    lines_ref[last : last + SLOTS, :] = edge[:SLOTS]
    for y in range(band_rows):
        base = y * (spaces + 2) * LINE
        lines_ref[base : base + LINE, :] = edge
        lines_ref[base + (spaces + 1) * LINE : base + (spaces + 2) * LINE, :] = edge
        base = base + LINE
        for k in (0, 1, 2, LINE - 4, LINE - 3, LINE - 2, LINE - 1):
            lines_ref[pl.ds(base + k, spaces, stride=LINE), :] = empty
    for z in range(PZ):
        deep = start_z + z
        slab = lax.div(deep, slab_rows)
        first = slab * (spaces * pitch) + (deep - slab * slab_rows) * band_rows
        for y in range(band_rows):
            line = cells_ref[pl.ds(first + y, spaces, stride=pitch), :]
            before = jnp.where(lane == 0, 0.0, pltpu.roll(line, 1, 1))
            after = jnp.where(lane == PX - 1, 0.0, pltpu.roll(line, PX - 1, 1))
            base = (y * (spaces + 2) + 1) * LINE + TAPS * (z + 1)
            for c, value in enumerate((before, line, after)):
                lines_ref[pl.ds(base + c, spaces, stride=LINE), :] = value


def tree_sum(values):
    values = list(values)
    while len(values) > 1:
        values = [
            values[i] + values[i + 1] if i + 1 < len(values) else values[i]
            for i in range(0, len(values), 2)
        ]
    return values[0]


def first_moments(lines_ref, gram_ref, weights, band_rows, spaces):
    rows = band_rows * spaces
    cells = []
    sums = [None] * rows
    for z in range(PZ):
        column = []
        for y in range(rows):
            at = (y % band_rows * (spaces + 2) + y // band_rows + 1) * LINE + TAPS * z
            value = lines_ref[at : at + SLOTS, :]
            sums[y] = value if sums[y] is None else sums[y] + value
            column.append(value.astype(BF16))
        cells.append(jnp.concatenate(column, axis=0))
    cells = jnp.concatenate(cells, axis=1)
    gram_ref[...] = lax.dot_general(cells, cells, CONTRACT_LAST, preferred_element_type=F32)

    def block(y, delta):
        lane = SLOTS * (y + delta)
        tile = lane // 128 * 128
        value = gram_ref[SLOTS * y : SLOTS * y + SLOTS, tile : tile + 128]
        return pltpu.roll(value, (tile + 128 - lane) % 128, 1) if lane != tile else value

    def total(values):
        return jnp.where(iota((SLOTS, 128), 1) < SLOTS, tree_sum(values), 0.0)

    head, tail = total([block(0, 0)]), total([block(rows - 1, 0)])
    near = total([block(y, 0) for y in range(rows)])
    next1 = 2.0 * total([block(y, 1) for y in range(rows - 1)])
    next2 = 2.0 * total([block(y, 2) for y in range(rows - 2)])
    move = lambda value, k: pltpu.roll(value, SLOTS * k, 1)
    form = jnp.concatenate(
        [
            near - tail + move(next1, 1) + move(next2, 2),
            move(near, 1) + move(next1, 2),
            move(near - head, 2),
        ],
        axis=0,
    )[:, : TAPS * SLOTS]
    product = jnp.dot(form, weights, precision=HI, preferred_element_type=F32)
    squares = jnp.sum(product * weights, axis=0, keepdims=True)
    every = tree_sum(sums)
    column = jnp.concatenate([every - sums[rows - 1], every, every - sums[0]], axis=0)
    column = jnp.sum(column, axis=1, keepdims=True)
    return jnp.sum(column * weights, axis=0, keepdims=True), squares


def spread_mirror(value, f, channels):
    value = jnp.where(iota(value.shape, 1) // channels == f, value, 0.0)
    reach = channels
    while reach < value.shape[1]:
        value = value + pltpu.roll(value, reach, 1)
        reach *= 2
    return value


def main_kernel(
    spaces,
    slab_rows,
    band_rows,
    channels,
    gathered_ref,
    corner_ref,
    flat_ref,
    full_ref,
    w2t_ref,
    params_ref,
    conv_ref,
    stats_ref,
    cells_ref,
    lines_ref,
    gram_ref,
    wide_ref,
    sums_ref,
):
    rows = band_rows * spaces
    hidden_rows = band_rows + TAPS - 1
    step = hidden_rows * channels
    band = lax.axis_index("space")
    start_z = corner_ref[lax.axis_size("patch"), 0]
    line_rows(start_z, gathered_ref, cells_ref, lines_ref, slab_rows, band_rows, spaces)

    first, second = first_moments(lines_ref, gram_ref, flat_ref[...], band_rows, spaces)
    count = float(PZ * rows * PX)
    mean = first / count
    variance = second / count - mean * mean
    lane_row = iota(mean.shape, 1) // channels % hidden_rows
    y = band * band_rows - 1 + lane_row
    inside = (y >= 0) & (y < rows)
    scale = lax.rsqrt(variance + 1e-05) * params_ref[0:1]
    shift = jnp.where(inside, params_ref[1:2] - mean * scale, 0.0)
    scale = jnp.where(inside, scale, 0.0)

    out_lanes = conv_ref.shape[2]
    groups = PZ // ZG
    empty = jnp.zeros((PX, step), BF16)
    for f in range(4):
        for g, j in ((0, 0), (groups - 1, ZI - 1)):
            at = (ZI - 1 - j if f % 2 else j) * step
            wide_ref[f, g * PX : (g + 1) * PX, at : at + step] = empty
    weights = full_ref[...]
    for z in range(PZ):
        cells = []
        for yi in range(hidden_rows + TAPS - 1):
            at = (yi % band_rows * (spaces + 2) + yi // band_rows + band) * LINE + TAPS * z
            cells.append(lines_ref[pl.ds(at, SLOTS), :].astype(BF16))
        cells = jnp.concatenate(cells, axis=0)
        value = lax.dot_general(cells, weights, CONTRACT_FIRST, preferred_element_type=F32)
        value = value * scale + shift
        value = jnp.maximum(value, 0.01 * value).astype(BF16)
        for g in range(groups):
            j = z + 1 - ZG * g
            if 0 <= j < ZI:
                for f in range(4):
                    at = (ZI - 1 - j if f % 2 else j) * step
                    wide_ref[f, g * PX : (g + 1) * PX, at : at + step] = value[
                        :, f * step : (f + 1) * step
                    ]

    x = iota((groups * PX, out_lanes), 0) % PX
    for f in range(4):
        cells = wide_ref[f]
        parts = [
            jnp.dot(cells, w2t_ref[c], preferred_element_type=F32) for c in range(TAPS)
        ]
        before, after = (parts[2], parts[0]) if f >= 2 else (parts[0], parts[2])
        value = (
            parts[1]
            + jnp.where(x == 0, 0.0, pltpu.roll(before, 1, 0))
            + jnp.where(x == PX - 1, 0.0, pltpu.roll(after, groups * PX - 1, 0))
        )
        conv_ref[f] = value
        sums_ref[f : f + 1, :] = jnp.sum(value, axis=0, keepdims=True)
        sums_ref[f + 4 : f + 5, :] = jnp.sum(value * value, axis=0, keepdims=True)
    sums = sums_ref[...]
    lanes = 4 * channels
    sums = sum(sums[:, at : at + lanes] for at in range(0, out_lanes, lanes))
    reach = lanes // 2
    while reach >= channels:
        sums = sums + pltpu.roll(sums, reach, 1)
        reach //= 2
    mirror = iota((1, lanes), 1) // channels
    for kind in range(2):
        row = sums[4 * kind : 4 * kind + 1]
        for f in range(1, 4):
            row = jnp.where(mirror == f, sums[4 * kind + f : 4 * kind + f + 1], row)
        for space in range(spaces):
            stats_ref[space, kind : kind + 1, :] = row


def head_kernel(count, channels, conv_ref, stats_ref, params_ref, heads_ref, bias_ref, out_ref):
    lanes = conv_ref.shape[2]
    per_group = heads_ref.shape[1]
    sums = stats_ref[0]
    for space in range(1, stats_ref.shape[0]):
        sums = sums + stats_ref[space]
    mean = sums[0:1] / count
    variance = sums[1:2] / count - mean * mean
    scale = lax.rsqrt(variance + 1e-05) * params_ref[2:3, : 4 * channels]
    shift = params_ref[3:4, : 4 * channels] - mean * scale
    table = jnp.concatenate([scale, shift, jnp.zeros((6, 4 * channels), F32)], axis=0)
    groups = conv_ref.shape[1] // PX
    totals = [None] * groups
    for f in range(4):
        own = spread_mirror(table, f, channels)
        own = jnp.concatenate([own] * (lanes // own.shape[1]), axis=1)
        for g in range(groups):
            value = conv_ref[f, g * PX : (g + 1) * PX, :] * own[0:1] + own[1:2]
            value = jnp.maximum(value, 0.01 * value).astype(BF16)
            logits = lax.dot_general(
                heads_ref[f % 2], value, CONTRACT_LAST, preferred_element_type=F32
            )
            totals[g] = logits if totals[g] is None else totals[g] + logits
    for g in range(groups):
        out_ref[g * per_group : (g + 1) * per_group, :] = (
            totals[g] * 0.25 + bias_ref[...]
        ).astype(out_ref.dtype)


def place_kernel(items, corner_ref, weights_ref, *refs):
    parts, (out_ref, pad_ref) = refs[:items], refs[items:]
    slab_rows, classes, band_rows, width = out_ref.shape
    per_z = classes * band_rows
    count = slab_rows * per_z
    blended = jnp.zeros((count, width), F32)
    for k in range(items):
        pad_ref[k, count : count + PZ * per_z, :] = parts[k][...].astype(F32)
        part = pad_ref[k, pl.ds(corner_ref[k, 0], count), :]
        part = jnp.concatenate([part, jnp.zeros((count, width - PX), F32)], axis=1)
        part = pltpu.roll(part, corner_ref[k, 1], 1)
        weight = weights_ref[k]
        blended = blended + jnp.where(weight > 0, part * weight, 0.0)
    for z in range(slab_rows):
        for k in range(classes):
            at = z * per_z + k * band_rows
            out_ref[z, k] = blended[at : at + band_rows]


def in_vmem(value):
    return pltpu.with_memory_space_constraint(value, pltpu.VMEM)


def in_hbm(value):
    return pltpu.with_memory_space_constraint(value, pltpu.HBM)


def local(
    image,
    offsets,
    conv1_weight,
    conv2_weight,
    norm1_gain,
    norm1_bias,
    norm2_gain,
    norm2_bias,
    head_weight,
    head_bias,
):
    groups = lax.axis_size("patch")
    spaces = lax.axis_size("space")
    slab_rows, band_rows, width = image.shape
    channels = norm1_gain.shape[0]
    classes = head_weight.shape[0]
    rows = band_rows * spaces
    hidden_rows = band_rows + TAPS - 1
    block = slab_rows * band_rows
    step = 4 * channels
    lanes1 = 4 * hidden_rows * channels
    lanes2 = ZG * band_rows * channels
    depth2 = ZI * hidden_rows * channels
    cells = PZ // ZG * PX
    per_z = classes * band_rows
    corners = in_hbm(offsets.T)

    windows = pl.pallas_call(
        cut_kernel,
        out_shape=pltpu.VMEM((groups * spaces, block, PX), BF16),
        in_specs=[SMEM, VMEM],
        out_specs=VMEM,
        scratch_shapes=[pltpu.VMEM((block, width), F32)],
        name="cut",
    )(corners, image)
    gathered = lax.all_to_all(in_vmem(windows), ("patch", "space"), 0, 0, tiled=True)

    flat, full, w2t, params, heads, bias, weights, corner = pl.pallas_call(
        functools.partial(prep_kernel, spaces, slab_rows, band_rows),
        out_shape=(
            pltpu.VMEM((TAPS * SLOTS, lanes1), F32),
            pltpu.VMEM(((hidden_rows + TAPS - 1) * SLOTS, lanes1), BF16),
            pltpu.VMEM((TAPS, depth2, lanes2), BF16),
            pltpu.VMEM((8, lanes1), F32),
            pltpu.VMEM((2, ZG * per_z, lanes2), BF16),
            pltpu.VMEM((ZG * per_z, PX), F32),
            pltpu.VMEM((groups, slab_rows * per_z, width), F32),
            pltpu.VMEM(((groups + 8) // 8 * 8, 128), jnp.int32),
        ),
        in_specs=[SMEM] + [VMEM] * 7 + [SMEM],
        out_specs=(VMEM,) * 8,
        scratch_shapes=[pltpu.VMEM((TAPS * SLOTS, step), F32)],
        compiler_params=pltpu.CompilerParams(vmem_limit_bytes=16 << 20),
        name="prep",
    )(
        corners,
        in_hbm(conv1_weight.transpose(0, 2, 1)),
        in_hbm(conv2_weight),
        in_hbm(norm1_gain.reshape(1, channels)),
        in_hbm(norm1_bias.reshape(1, channels)),
        in_hbm(norm2_gain.reshape(1, channels)),
        in_hbm(norm2_bias.reshape(1, channels)),
        in_hbm(head_weight),
        in_hbm(head_bias),
    )
    scratch = (
        ((groups * spaces * (block + 1), PX), F32),
        ((band_rows * (spaces + 2) * LINE + SLOTS, PX), F32),
        ((rows * SLOTS, rows * SLOTS), F32),
        ((4, cells, depth2), BF16),
        ((8, lanes2), F32),
    )
    size = sum(math.prod(shape) * jnp.dtype(kind).itemsize for shape, kind in scratch)
    conv, stats = pl.pallas_call(
        functools.partial(main_kernel, spaces, slab_rows, band_rows, channels),
        out_shape=(
            pltpu.VMEM((4, cells, lanes2), F32),
            pltpu.VMEM((spaces, 2, step), F32),
        ),
        in_specs=[VMEM] * 6,
        out_specs=(VMEM, VMEM),
        scratch_shapes=[pltpu.VMEM(shape, kind) for shape, kind in scratch],
        compiler_params=pltpu.CompilerParams(vmem_limit_bytes=min(2 * size + (16 << 20), 40 << 20)),
        name="main",
    )(
        in_vmem(gathered),
        in_vmem(corner),
        in_vmem(flat),
        in_vmem(full),
        in_vmem(w2t),
        in_vmem(params),
    )
    stats = lax.all_to_all(stats, "space", 0, 0, tiled=True)
    averaged = pl.pallas_call(
        functools.partial(head_kernel, float(PZ * rows * PX), channels),
        out_shape=pltpu.VMEM((PZ * per_z, PX), BF16),
        in_specs=[VMEM] * 5,
        out_specs=VMEM,
        compiler_params=pltpu.CompilerParams(vmem_limit_bytes=8 << 20),
        name="head",
    )(in_vmem(conv), in_vmem(stats), in_vmem(params), in_vmem(heads), in_vmem(bias))
    parts = [averaged] + [
        lax.ppermute(averaged, "patch", [(i, i ^ k) for i in range(groups)])
        for k in range(1, groups)
    ]
    return pl.pallas_call(
        functools.partial(place_kernel, groups),
        out_shape=jax.ShapeDtypeStruct((slab_rows, classes, band_rows, width), F32),
        in_specs=[VMEM] * (2 + groups),
        out_specs=VMEM,
        scratch_shapes=[pltpu.VMEM((groups, (2 * slab_rows + PZ) * per_z, PX), F32)],
        compiler_params=pltpu.CompilerParams(vmem_limit_bytes=8 << 20),
        name="place",
    )(in_vmem(corner), in_vmem(weights), *[in_vmem(part) for part in parts])


def solution(mesh):
    return jax.shard_map(
        local,
        mesh=mesh,
        in_specs=(P("patch", "space", None), P(), P(), P(), P(), P(), P(), P(), P(), P()),
        out_specs=P("patch", None, "space", None),
        check_vma=False,
    )
```

```python
import functools
import math

import jax
import jax.numpy as jnp
from jax import lax
from jax.experimental import pallas as pl
from jax.experimental.pallas import tpu as pltpu
from jax.sharding import PartitionSpec as P

PX = 128
PZ = 16
TAPS = 3
ZG = 4
ZI = ZG + TAPS - 1
SLOTS = 16
LINE = TAPS * (PZ + 2) + 1
F32 = jnp.float32
BF16 = jnp.bfloat16
HI = lax.Precision.HIGHEST
CONTRACT_FIRST = (((0,), (0,)), ((), ()))
CONTRACT_LAST = (((1,), (1,)), ((), ()))
VMEM = pl.BlockSpec(memory_space=pltpu.VMEM)
SMEM = pl.BlockSpec(memory_space=pltpu.SMEM)


def iota(shape, dim):
    return lax.broadcasted_iota(jnp.int32, shape, dim)


def repeat_matrix(channels, lanes, dtype):
    shape = (channels, lanes)
    return (iota(shape, 0) == iota(shape, 1) % channels).astype(dtype)


def cut_kernel(offsets_ref, image_ref, out_ref, rows_ref):
    slab_rows, band_rows, width = image_ref.shape
    for z in range(slab_rows):
        rows_ref[z * band_rows : (z + 1) * band_rows, :] = image_ref[z].astype(F32)
    rows = rows_ref[...]
    items = offsets_ref.shape[1]
    spaces = out_ref.shape[0] // items
    for item in range(items):
        shift = lax.rem(width - offsets_ref[1, item], width)
        window = pltpu.roll(rows, shift, 1)[:, :PX].astype(BF16)
        for space in range(spaces):
            out_ref[item * spaces + space] = window


def prep_kernel(
    spaces,
    slab_rows,
    band_rows,
    offsets_ref,
    w1_ref,
    w2_ref,
    gain1_ref,
    bias1_ref,
    gain2_ref,
    bias2_ref,
    head_ref,
    head_bias_ref,
    flat_ref,
    full_ref,
    wide_ref,
    pair_ref,
    params_ref,
    heads_ref,
    bias_ref,
    weights_ref,
    corner_ref,
    narrow_ref,
):
    channels = gain1_ref.shape[1]
    classes = head_ref.shape[0]
    rows = band_rows * spaces
    hidden_rows = band_rows + TAPS - 1
    step = 4 * channels
    band = lax.axis_index("space")
    patch = lax.axis_index("patch")

    repeat = repeat_matrix(channels, step, BF16)
    taps = [
        jnp.dot(w1_ref[t], repeat, preferred_element_type=F32) for t in range(TAPS * TAPS)
    ]
    mirror = iota((1, step), 1) // channels
    narrow_ref[...] = jnp.zeros_like(narrow_ref)
    for b in range(TAPS):
        for a in range(TAPS):
            one, two = taps[a * TAPS + b], taps[(TAPS - 1 - a) * TAPS + b]
            for c in range(TAPS):
                d = TAPS - 1 - c
                row = jnp.where(
                    mirror < 2,
                    jnp.where(mirror == 0, one[c : c + 1], two[c : c + 1]),
                    jnp.where(mirror == 2, one[d : d + 1], two[d : d + 1]),
                )
                at = SLOTS * b + a * TAPS + c
                narrow_ref[at : at + 1, :] = row
    lanes = flat_ref.shape[1]
    shape = (step, lanes)
    lane = iota(shape, 1)
    spread = iota(shape, 0) == lane // (hidden_rows * channels) * channels + lane % channels
    flat = jnp.dot(
        narrow_ref[...].astype(BF16), spread.astype(BF16), preferred_element_type=F32
    )
    flat_ref[...] = flat
    lane_row = iota((SLOTS, lanes), 1) // channels % hidden_rows
    for yi in range(hidden_rows + TAPS - 1):
        piece = jnp.zeros((SLOTS, lanes), F32)
        for b in range(TAPS):
            if 0 <= yi - b < hidden_rows:
                piece = jnp.where(lane_row == yi - b, flat[SLOTS * b : SLOTS * b + SLOTS], piece)
        full_ref[SLOTS * yi : SLOTS * yi + SLOTS, :] = piece.astype(BF16)

    lanes = ZG * band_rows * channels
    spread = repeat_matrix(channels, lanes, BF16)
    taps = [
        lax.dot_general(w2_ref[t], spread, CONTRACT_FIRST, preferred_element_type=F32)
        for t in range(TAPS * TAPS)
    ]
    half = lanes // 2
    group = iota((channels, lanes), 1) // channels
    outer = TAPS - 1
    for zi in range(ZI):
        for yi in range(hidden_rows):
            at = (zi * hidden_rows + yi) * channels
            piece = jnp.zeros((channels, lanes), F32)
            pair = jnp.zeros((channels, lanes), F32)
            for zo in range(ZG):
                for yo in range(band_rows):
                    a, b = zi - zo, yi - yo
                    if 0 <= a < TAPS and 0 <= b < TAPS:
                        to = zo * band_rows + yo
                        tap = taps[a * TAPS + b]
                        piece = jnp.where(group == to, tap[outer * channels :], piece)
                        if zo < ZG // 2:
                            pair = jnp.where(group == to, tap[:channels], pair)
                            to = to + half // channels
                            pair = jnp.where(
                                group == to, tap[channels : 2 * channels], pair
                            )
            wide_ref[at : at + channels, :] = piece.astype(BF16)
            if zi < ZI - ZG // 2:
                pair_ref[at : at + channels, :] = pair.astype(BF16)

    table = jnp.concatenate(
        [
            gain1_ref[...],
            bias1_ref[...],
            gain2_ref[...],
            bias2_ref[...],
            head_ref[...].astype(F32),
            jnp.zeros((8 - classes - 4, channels), F32),
        ],
        axis=0,
    )
    spread = repeat_matrix(channels, params_ref.shape[1], F32)
    table = jnp.dot(table, spread, precision=HI, preferred_element_type=F32)
    params_ref[...] = table
    table = table[:, :lanes]

    per_z = classes * band_rows
    shape = (ZG * per_z, lanes)
    row_z = iota(shape, 0) // per_z
    row_k = iota(shape, 0) // band_rows % classes
    row_y = iota(shape, 0) % band_rows
    full = jnp.zeros(shape, F32)
    for k in range(classes):
        full = jnp.where(row_k == k, table[4 + k : 5 + k], full)
    lane_z = iota(shape, 1) // (band_rows * channels)
    lane_y = iota(shape, 1) // channels % band_rows
    for f, z in enumerate((row_z, ZG - 1 - row_z)):
        heads_ref[f] = jnp.where((lane_z == z) & (lane_y == row_y), full, 0.0).astype(BF16)
    row_k = iota(bias_ref.shape, 0) // band_rows % classes
    bias = jnp.zeros(bias_ref.shape, F32)
    for k in range(classes):
        bias = jnp.where(row_k == k, head_bias_ref[k], bias)
    bias_ref[...] = bias

    items, count, width = weights_ref.shape
    shape = (count, width)
    slab = patch * slab_rows
    z = slab + iota(shape, 0) // per_z
    x = iota(shape, 1)
    y = (band * band_rows + iota(shape, 0) % band_rows).astype(F32) - (rows - 1) / 2.0
    across = y * y * (1.0 / (2.0 * (rows / 8.0) ** 2))
    shape = corner_ref.shape
    corner_row, corner_lane = iota(shape, 0), iota(shape, 1)
    own_z = jnp.where(corner_lane == 0, offsets_ref[0, patch], 0)
    corners = jnp.where(corner_row == items, own_z, 0)
    coverage = jnp.zeros((count, width), F32)
    weights = []
    for k in range(items):
        item = jnp.bitwise_xor(patch, k)
        start_z, start_x = offsets_ref[0, item], offsets_ref[1, item]
        first = jnp.clip(slab - start_z, -slab_rows, PZ) * per_z + count
        values = jnp.where(corner_lane == 0, first, start_x)
        corners = jnp.where((corner_row == k) & (corner_lane < 2), values, corners)
        rel_z, rel_x = z - start_z, x - start_x
        inside = (rel_z >= 0) & (rel_z < PZ) & (rel_x >= 0) & (rel_x < PX)
        far_z = rel_z.astype(F32) - (PZ - 1) / 2.0
        far_x = rel_x.astype(F32) - (PX - 1) / 2.0
        power = (
            across
            + far_z * far_z * (1.0 / (2.0 * (PZ / 8.0) ** 2))
            + far_x * far_x * (1.0 / (2.0 * (PX / 8.0) ** 2))
        )
        weight = jnp.where(inside, jnp.exp(-power), 0.0)
        weights.append(weight)
        coverage = coverage + weight
    share = 1.0 / jnp.maximum(coverage, 0.1)
    for k in range(items):
        weights_ref[k] = weights[k] * share
    corner_ref[...] = corners


def line_rows(start_z, gathered_ref, cells_ref, lines_ref, slab_rows, band_rows, spaces):
    block = slab_rows * band_rows
    pitch = block + 1
    for device in range(gathered_ref.shape[0]):
        cells_ref[device * pitch : device * pitch + block, :] = gathered_ref[device].astype(F32)
    lane = iota((spaces, PX), 1)
    empty = jnp.zeros((spaces, PX), F32)
    edge = jnp.zeros((LINE, PX), F32)
    last = band_rows * (spaces + 2) * LINE
    lines_ref[last : last + SLOTS, :] = edge[:SLOTS]
    for y in range(band_rows):
        base = y * (spaces + 2) * LINE
        lines_ref[base : base + LINE, :] = edge
        lines_ref[base + (spaces + 1) * LINE : base + (spaces + 2) * LINE, :] = edge
        base = base + LINE
        for k in (0, 1, 2, LINE - 4, LINE - 3, LINE - 2, LINE - 1):
            lines_ref[pl.ds(base + k, spaces, stride=LINE), :] = empty
    for z in range(PZ):
        deep = start_z + z
        slab = lax.div(deep, slab_rows)
        first = slab * (spaces * pitch) + (deep - slab * slab_rows) * band_rows
        for y in range(band_rows):
            line = cells_ref[pl.ds(first + y, spaces, stride=pitch), :]
            before = jnp.where(lane == 0, 0.0, pltpu.roll(line, 1, 1))
            after = jnp.where(lane == PX - 1, 0.0, pltpu.roll(line, PX - 1, 1))
            base = (y * (spaces + 2) + 1) * LINE + TAPS * (z + 1)
            for c, value in enumerate((before, line, after)):
                lines_ref[pl.ds(base + c, spaces, stride=LINE), :] = value


def tree_sum(values):
    values = list(values)
    while len(values) > 1:
        values = [
            values[i] + values[i + 1] if i + 1 < len(values) else values[i]
            for i in range(0, len(values), 2)
        ]
    return values[0]


def first_moments(lines_ref, gram_ref, weights, band_rows, spaces):
    rows = band_rows * spaces
    chunks = gram_ref.shape[0]
    size = rows // chunks
    ahead = TAPS - 1
    cells = []
    sums = [None] * rows
    for y in range(rows + ahead):
        line = []
        for z in range(PZ):
            at = (y % band_rows * (spaces + 2) + y // band_rows + 1) * LINE + TAPS * z
            value = lines_ref[at : at + SLOTS, :]
            line.append(value.astype(BF16))
            if y < rows:
                sums[y] = value if sums[y] is None else sums[y] + value
        cells.append(jnp.concatenate(line, axis=1))
    for chunk in range(chunks):
        left = jnp.concatenate(cells[chunk * size : (chunk + 1) * size], axis=0)
        right = jnp.concatenate(cells[chunk * size : (chunk + 1) * size + ahead], axis=0)
        gram_ref[chunk] = lax.dot_general(
            left, right, CONTRACT_LAST, preferred_element_type=F32
        )

    def block(y, delta, chosen):
        lane = SLOTS * (y + delta)
        tile = lane // 128 * 128
        end = min(tile + 128, gram_ref.shape[2])
        value = tree_sum(
            [gram_ref[chunk, SLOTS * y : SLOTS * (y + 1), tile:end] for chunk in chosen]
        )
        if end < tile + 128:
            value = jnp.concatenate(
                [value, jnp.zeros((SLOTS, tile + 128 - end), F32)], axis=1
            )
        return pltpu.roll(value, (tile + 128 - lane) % 128, 1) if lane != tile else value

    def total(values):
        return jnp.where(iota((SLOTS, 128), 1) < SLOTS, tree_sum(values), 0.0)

    every = range(chunks)
    head, tail = total([block(0, 0, [0])]), total([block(size - 1, 0, [chunks - 1])])
    near = total([block(y, 0, every) for y in range(size)])
    next1 = 2.0 * total([block(y, 1, every) for y in range(size)])
    next2 = 2.0 * total([block(y, 2, every) for y in range(size)])
    move = lambda value, k: pltpu.roll(value, SLOTS * k, 1)
    form = jnp.concatenate(
        [
            near - tail + move(next1, 1) + move(next2, 2),
            move(near, 1) + move(next1, 2),
            move(near - head, 2),
        ],
        axis=0,
    )[:, : TAPS * SLOTS]
    high = form.astype(BF16)
    left = form - high.astype(F32)
    middle = left.astype(BF16)
    low = (left - middle.astype(F32)).astype(BF16)
    product = jnp.dot(
        jnp.concatenate([high, middle, low], axis=0),
        weights.astype(BF16),
        preferred_element_type=F32,
    )
    size = TAPS * SLOTS
    product = product[:size] + (product[size : 2 * size] + product[2 * size :])
    squares = jnp.sum(product * weights, axis=0, keepdims=True)
    every = tree_sum(sums)
    column = jnp.concatenate([every - sums[rows - 1], every, every - sums[0]], axis=0)
    column = jnp.sum(column, axis=1, keepdims=True)
    return jnp.sum(column * weights, axis=0, keepdims=True), squares


def spread_mirror(value, f, channels):
    value = jnp.where(iota(value.shape, 1) // channels == f, value, 0.0)
    reach = channels
    while reach < value.shape[1]:
        value = value + pltpu.roll(value, reach, 1)
        reach *= 2
    return value


def main_kernel(
    spaces,
    slab_rows,
    band_rows,
    channels,
    gathered_ref,
    corner_ref,
    flat_ref,
    full_ref,
    w2t_ref,
    w2p_ref,
    params_ref,
    conv_ref,
    stats_ref,
    cells_ref,
    lines_ref,
    gram_ref,
    wide_ref,
):
    rows = band_rows * spaces
    hidden_rows = band_rows + TAPS - 1
    step = hidden_rows * channels
    band = lax.axis_index("space")
    start_z = corner_ref[lax.axis_size("patch"), 0]
    line_rows(start_z, gathered_ref, cells_ref, lines_ref, slab_rows, band_rows, spaces)

    first, second = first_moments(lines_ref, gram_ref, flat_ref[...], band_rows, spaces)
    count = float(PZ * rows * PX)
    mean = first / count
    variance = second / count - mean * mean
    lane_row = iota(mean.shape, 1) // channels % hidden_rows
    y = band * band_rows - 1 + lane_row
    inside = (y >= 0) & (y < rows)
    scale = lax.rsqrt(variance + 1e-05) * params_ref[0:1]
    shift = jnp.where(inside, params_ref[1:2] - mean * scale, 0.0)
    scale = jnp.where(inside, scale, 0.0)

    out_lanes = conv_ref.shape[2]
    half = out_lanes // 2
    groups = PZ // ZG
    empty = jnp.zeros((PX, step), BF16)
    for f in range(4):
        for g, j in ((0, 0), (groups - 1, ZI - 1)):
            at = (ZI - 1 - j if f % 2 else j) * step
            wide_ref[g, f * PX : (f + 1) * PX, at : at + step] = empty
    weights = full_ref[...]

    def hidden(cells_z):
        cells = []
        for yi in range(hidden_rows + TAPS - 1):
            base = (yi % band_rows * (spaces + 2) + yi // band_rows + band) * LINE
            line = [
                lines_ref[pl.ds(base + TAPS * z, SLOTS), :].astype(BF16) for z in cells_z
            ]
            cells.append(jnp.concatenate(line, axis=1))
        cells = jnp.concatenate(cells, axis=0)
        values = lax.dot_general(cells, weights, CONTRACT_FIRST, preferred_element_type=F32)
        for k, z in enumerate(cells_z):
            value = values[k * PX : (k + 1) * PX] * scale + shift
            value = jnp.maximum(value, 0.01 * value).astype(BF16)
            for g in range(groups):
                j = z + 1 - ZG * g
                if 0 <= j < ZI:
                    for f in range(4):
                        at = (ZI - 1 - j if f % 2 else j) * step
                        wide_ref[g, f * PX : (f + 1) * PX, at : at + step] = value[
                            :, f * step : (f + 1) * step
                        ]

    x = iota((2 * PX, out_lanes), 0) % PX
    totals = [[None] * 4, [None] * 4]
    done = 0
    for g in range(groups):
        upto = min(ZG * g + ZG + 1, PZ)
        hidden(range(done, upto))
        done = upto
        cells = wide_ref[g]
        last = jnp.dot(cells, w2t_ref[...], preferred_element_type=F32)
        pairs = [
            jnp.dot(
                cells[:, at : at + w2p_ref.shape[0]], w2p_ref[...], preferred_element_type=F32
            )
            for at in (0, ZG // 2 * step)
        ]
        first, middle = (
            jnp.concatenate([pair[:, at : at + half] for pair in pairs], axis=1)
            for at in (0, half)
        )
        for flip in range(2):
            at = flip * 2 * PX
            before, after = (last, first) if flip else (first, last)
            value = (
                middle[at : at + 2 * PX]
                + jnp.where(x == 0, 0.0, pltpu.roll(before[at : at + 2 * PX], 1, 0))
                + jnp.where(
                    x == PX - 1, 0.0, pltpu.roll(after[at : at + 2 * PX], 2 * PX - 1, 0)
                )
            )
            conv_ref[g, at : at + 2 * PX, :] = value
            for f in (2 * flip, 2 * flip + 1):
                part = value[f * PX - at : (f + 1) * PX - at]
                for kind, item in enumerate((part, part * part)):
                    item = jnp.sum(item, axis=0, keepdims=True)
                    old = totals[kind][f]
                    totals[kind][f] = item if old is None else old + item
    sums = jnp.concatenate(totals[0] + totals[1], axis=0)
    lanes = 4 * channels
    sums = sum(sums[:, at : at + lanes] for at in range(0, out_lanes, lanes))
    reach = lanes // 2
    while reach >= channels:
        sums = sums + pltpu.roll(sums, reach, 1)
        reach //= 2
    mirror = iota((1, lanes), 1) // channels
    for kind in range(2):
        row = sums[4 * kind : 4 * kind + 1]
        for f in range(1, 4):
            row = jnp.where(mirror == f, sums[4 * kind + f : 4 * kind + f + 1], row)
        for space in range(spaces):
            stats_ref[space, kind : kind + 1, :] = row


def head_kernel(count, channels, conv_ref, stats_ref, params_ref, heads_ref, bias_ref, out_ref):
    lanes = conv_ref.shape[2]
    per_group = heads_ref.shape[1]
    sums = stats_ref[0]
    for space in range(1, stats_ref.shape[0]):
        sums = sums + stats_ref[space]
    mean = sums[0:1] / count
    variance = sums[1:2] / count - mean * mean
    scale = lax.rsqrt(variance + 1e-05) * params_ref[2:3, : 4 * channels]
    shift = params_ref[3:4, : 4 * channels] - mean * scale
    table = jnp.concatenate([scale, shift, jnp.zeros((6, 4 * channels), F32)], axis=0)
    groups = conv_ref.shape[0]
    totals = [None] * groups
    for f in range(4):
        own = spread_mirror(table, f, channels)
        own = jnp.concatenate([own] * (lanes // own.shape[1]), axis=1)
        for g in range(groups):
            value = conv_ref[g, f * PX : (f + 1) * PX, :] * own[0:1] + own[1:2]
            value = jnp.maximum(value, 0.01 * value).astype(BF16)
            logits = lax.dot_general(
                heads_ref[f % 2], value, CONTRACT_LAST, preferred_element_type=F32
            )
            totals[g] = logits if totals[g] is None else totals[g] + logits
    for g in range(groups):
        out_ref[g * per_group : (g + 1) * per_group, :] = (
            totals[g] * 0.25 + bias_ref[...]
        ).astype(out_ref.dtype)


def place_kernel(items, corner_ref, weights_ref, *refs):
    parts, (out_ref, pad_ref) = refs[:items], refs[items:]
    slab_rows, classes, band_rows, width = out_ref.shape
    per_z = classes * band_rows
    count = slab_rows * per_z
    blended = jnp.zeros((count, width), F32)
    for k in range(items):
        pad_ref[k, count : count + PZ * per_z, :] = parts[k][...].astype(F32)
        part = pad_ref[k, pl.ds(corner_ref[k, 0], count), :]
        part = jnp.concatenate([part, jnp.zeros((count, width - PX), F32)], axis=1)
        part = pltpu.roll(part, corner_ref[k, 1], 1)
        weight = weights_ref[k]
        blended = blended + jnp.where(weight > 0, part * weight, 0.0)
    for z in range(slab_rows):
        for k in range(classes):
            at = z * per_z + k * band_rows
            out_ref[z, k] = blended[at : at + band_rows]


def in_vmem(value):
    return pltpu.with_memory_space_constraint(value, pltpu.VMEM)


def in_hbm(value):
    return pltpu.with_memory_space_constraint(value, pltpu.HBM)


def local(
    image,
    offsets,
    conv1_weight,
    conv2_weight,
    norm1_gain,
    norm1_bias,
    norm2_gain,
    norm2_bias,
    head_weight,
    head_bias,
):
    groups = lax.axis_size("patch")
    spaces = lax.axis_size("space")
    slab_rows, band_rows, width = image.shape
    channels = norm1_gain.shape[0]
    classes = head_weight.shape[0]
    rows = band_rows * spaces
    hidden_rows = band_rows + TAPS - 1
    block = slab_rows * band_rows
    step = 4 * channels
    lanes1 = 4 * hidden_rows * channels
    lanes2 = ZG * band_rows * channels
    depth2 = ZI * hidden_rows * channels
    depth3 = (ZI - ZG // 2) * hidden_rows * channels
    per_z = classes * band_rows
    corners = in_hbm(offsets.T)

    windows = pl.pallas_call(
        cut_kernel,
        out_shape=pltpu.VMEM((groups * spaces, block, PX), BF16),
        in_specs=[SMEM, VMEM],
        out_specs=VMEM,
        scratch_shapes=[pltpu.VMEM((block, width), F32)],
        name="cut",
    )(corners, image)
    gathered = lax.all_to_all(in_vmem(windows), ("patch", "space"), 0, 0, tiled=True)

    flat, full, w2t, w2p, params, heads, bias, weights, corner = pl.pallas_call(
        functools.partial(prep_kernel, spaces, slab_rows, band_rows),
        out_shape=(
            pltpu.VMEM((TAPS * SLOTS, lanes1), F32),
            pltpu.VMEM(((hidden_rows + TAPS - 1) * SLOTS, lanes1), BF16),
            pltpu.VMEM((depth2, lanes2), BF16),
            pltpu.VMEM((depth3, lanes2), BF16),
            pltpu.VMEM((8, lanes1), F32),
            pltpu.VMEM((2, ZG * per_z, lanes2), BF16),
            pltpu.VMEM((ZG * per_z, PX), F32),
            pltpu.VMEM((groups, slab_rows * per_z, width), F32),
            pltpu.VMEM(((groups + 8) // 8 * 8, 128), jnp.int32),
        ),
        in_specs=[SMEM] + [VMEM] * 7 + [SMEM],
        out_specs=(VMEM,) * 9,
        scratch_shapes=[pltpu.VMEM((TAPS * SLOTS, step), F32)],
        compiler_params=pltpu.CompilerParams(vmem_limit_bytes=16 << 20),
        name="prep",
    )(
        corners,
        in_hbm(conv1_weight.transpose(0, 2, 1)),
        in_hbm(conv2_weight),
        in_hbm(norm1_gain.reshape(1, channels)),
        in_hbm(norm1_bias.reshape(1, channels)),
        in_hbm(norm2_gain.reshape(1, channels)),
        in_hbm(norm2_bias.reshape(1, channels)),
        in_hbm(head_weight),
        in_hbm(head_bias),
    )
    chunks = max(rows // 8, 1)
    scratch = (
        ((groups * spaces * (block + 1), PX), F32),
        ((band_rows * (spaces + 2) * LINE + SLOTS, PX), F32),
        ((chunks, rows // chunks * SLOTS, (rows // chunks + TAPS - 1) * SLOTS), F32),
        ((PZ // ZG, 4 * PX, depth2), BF16),
    )
    size = sum(math.prod(shape) * jnp.dtype(kind).itemsize for shape, kind in scratch)
    conv, stats = pl.pallas_call(
        functools.partial(main_kernel, spaces, slab_rows, band_rows, channels),
        out_shape=(
            pltpu.VMEM((PZ // ZG, 4 * PX, lanes2), F32),
            pltpu.VMEM((spaces, 2, step), F32),
        ),
        in_specs=[VMEM] * 7,
        out_specs=(VMEM, VMEM),
        scratch_shapes=[pltpu.VMEM(shape, kind) for shape, kind in scratch],
        compiler_params=pltpu.CompilerParams(vmem_limit_bytes=min(2 * size + (16 << 20), 40 << 20)),
        name="main",
    )(
        in_vmem(gathered),
        in_vmem(corner),
        in_vmem(flat),
        in_vmem(full),
        in_vmem(w2t),
        in_vmem(w2p),
        in_vmem(params),
    )
    stats = lax.all_to_all(stats, "space", 0, 0, tiled=True)
    averaged = pl.pallas_call(
        functools.partial(head_kernel, float(PZ * rows * PX), channels),
        out_shape=pltpu.VMEM((PZ * per_z, PX), BF16),
        in_specs=[VMEM] * 5,
        out_specs=VMEM,
        compiler_params=pltpu.CompilerParams(vmem_limit_bytes=8 << 20),
        name="head",
    )(in_vmem(conv), in_vmem(stats), in_vmem(params), in_vmem(heads), in_vmem(bias))
    parts = [averaged] + [
        lax.ppermute(averaged, "patch", [(i, i ^ k) for i in range(groups)])
        for k in range(1, groups)
    ]
    return pl.pallas_call(
        functools.partial(place_kernel, groups),
        out_shape=jax.ShapeDtypeStruct((slab_rows, classes, band_rows, width), F32),
        in_specs=[VMEM] * (2 + groups),
        out_specs=VMEM,
        scratch_shapes=[pltpu.VMEM((groups, (2 * slab_rows + PZ) * per_z, PX), F32)],
        compiler_params=pltpu.CompilerParams(vmem_limit_bytes=8 << 20),
        name="place",
    )(in_vmem(corner), in_vmem(weights), *[in_vmem(part) for part in parts])


def solution(mesh):
    return jax.shard_map(
        local,
        mesh=mesh,
        in_specs=(P("patch", "space", None), P(), P(), P(), P(), P(), P(), P(), P(), P()),
        out_specs=P("patch", None, "space", None),
        check_vma=False,
    )
```

```python
import functools
import math

import jax
import jax.numpy as jnp
from jax import lax
from jax.experimental import pallas as pl
from jax.experimental.pallas import tpu as pltpu
from jax.sharding import PartitionSpec as P

PX = 128
PZ = 16
TAPS = 3
ZG = 4
ZI = ZG + TAPS - 1
SLOTS = 16
LINE = TAPS * (PZ + 2) + 1
F32 = jnp.float32
BF16 = jnp.bfloat16
HI = lax.Precision.HIGHEST
CONTRACT_FIRST = (((0,), (0,)), ((), ()))
CONTRACT_LAST = (((1,), (1,)), ((), ()))
VMEM = pl.BlockSpec(memory_space=pltpu.VMEM)
SMEM = pl.BlockSpec(memory_space=pltpu.SMEM)


def iota(shape, dim):
    return lax.broadcasted_iota(jnp.int32, shape, dim)


def repeat_matrix(channels, lanes, dtype):
    shape = (channels, lanes)
    return (iota(shape, 0) == iota(shape, 1) % channels).astype(dtype)


def cut_kernel(offsets_ref, image_ref, out_ref, rows_ref):
    slab_rows, band_rows, width = image_ref.shape
    for z in range(slab_rows):
        rows_ref[z * band_rows : (z + 1) * band_rows, :] = image_ref[z].astype(F32)
    rows = rows_ref[...]
    items = offsets_ref.shape[1]
    spaces = out_ref.shape[0] // items
    for item in range(items):
        shift = lax.rem(width - offsets_ref[1, item], width)
        window = pltpu.roll(rows, shift, 1)[:, :PX].astype(BF16)
        for space in range(spaces):
            out_ref[item * spaces + space] = window


def prep_kernel(
    spaces,
    slab_rows,
    band_rows,
    offsets_ref,
    w1_ref,
    w2_ref,
    gain1_ref,
    bias1_ref,
    gain2_ref,
    bias2_ref,
    head_ref,
    head_bias_ref,
    flat_ref,
    full_ref,
    wide_ref,
    pair_ref,
    params_ref,
    heads_ref,
    bias_ref,
    weights_ref,
    corner_ref,
    narrow_ref,
):
    channels = gain1_ref.shape[1]
    classes = head_ref.shape[0]
    rows = band_rows * spaces
    hidden_rows = band_rows + TAPS - 1
    step = 4 * channels
    band = lax.axis_index("space")
    patch = lax.axis_index("patch")

    repeat = repeat_matrix(channels, step, BF16)
    taps = [
        jnp.dot(w1_ref[t], repeat, preferred_element_type=F32) for t in range(TAPS * TAPS)
    ]
    mirror = iota((1, step), 1) // channels
    narrow_ref[...] = jnp.zeros_like(narrow_ref)
    for b in range(TAPS):
        for a in range(TAPS):
            one, two = taps[a * TAPS + b], taps[(TAPS - 1 - a) * TAPS + b]
            for c in range(TAPS):
                d = TAPS - 1 - c
                row = jnp.where(
                    mirror < 2,
                    jnp.where(mirror == 0, one[c : c + 1], two[c : c + 1]),
                    jnp.where(mirror == 2, one[d : d + 1], two[d : d + 1]),
                )
                at = SLOTS * b + a * TAPS + c
                narrow_ref[at : at + 1, :] = row
    lanes = flat_ref.shape[1]
    shape = (step, lanes)
    lane = iota(shape, 1)
    spread = iota(shape, 0) == lane // (hidden_rows * channels) * channels + lane % channels
    flat = jnp.dot(
        narrow_ref[...].astype(BF16), spread.astype(BF16), preferred_element_type=F32
    )
    flat_ref[...] = flat
    lane_row = iota((SLOTS, lanes), 1) // channels % hidden_rows
    for yi in range(hidden_rows + TAPS - 1):
        piece = jnp.zeros((SLOTS, lanes), F32)
        for b in range(TAPS):
            if 0 <= yi - b < hidden_rows:
                piece = jnp.where(lane_row == yi - b, flat[SLOTS * b : SLOTS * b + SLOTS], piece)
        full_ref[SLOTS * yi : SLOTS * yi + SLOTS, :] = piece.astype(BF16)

    lanes = ZG * band_rows * channels
    spread = repeat_matrix(channels, lanes, BF16)
    taps = [
        lax.dot_general(w2_ref[t], spread, CONTRACT_FIRST, preferred_element_type=F32)
        for t in range(TAPS * TAPS)
    ]
    half = lanes // 2
    group = iota((channels, lanes), 1) // channels
    outer = TAPS - 1
    for zi in range(ZI):
        for yi in range(hidden_rows):
            at = (zi * hidden_rows + yi) * channels
            piece = jnp.zeros((channels, lanes), F32)
            pair = jnp.zeros((channels, lanes), F32)
            for zo in range(ZG):
                for yo in range(band_rows):
                    a, b = zi - zo, yi - yo
                    if 0 <= a < TAPS and 0 <= b < TAPS:
                        to = zo * band_rows + yo
                        tap = taps[a * TAPS + b]
                        piece = jnp.where(group == to, tap[outer * channels :], piece)
                        if zo < ZG // 2:
                            pair = jnp.where(group == to, tap[:channels], pair)
                            to = to + half // channels
                            pair = jnp.where(
                                group == to, tap[channels : 2 * channels], pair
                            )
            wide_ref[at : at + channels, :] = piece.astype(BF16)
            if zi < ZI - ZG // 2:
                pair_ref[at : at + channels, :] = pair.astype(BF16)

    table = jnp.concatenate(
        [
            gain1_ref[...],
            bias1_ref[...],
            gain2_ref[...],
            bias2_ref[...],
            head_ref[...].astype(F32),
            jnp.zeros((8 - classes - 4, channels), F32),
        ],
        axis=0,
    )
    spread = repeat_matrix(channels, params_ref.shape[1], F32)
    table = jnp.dot(table, spread, precision=HI, preferred_element_type=F32)
    params_ref[...] = table
    table = table[:, :lanes]

    per_z = classes * band_rows
    shape = (ZG * per_z, lanes)
    row_z = iota(shape, 0) // per_z
    row_k = iota(shape, 0) // band_rows % classes
    row_y = iota(shape, 0) % band_rows
    full = jnp.zeros(shape, F32)
    for k in range(classes):
        full = jnp.where(row_k == k, table[4 + k : 5 + k], full)
    lane_z = iota(shape, 1) // (band_rows * channels)
    lane_y = iota(shape, 1) // channels % band_rows
    for f, z in enumerate((row_z, ZG - 1 - row_z)):
        heads_ref[f] = jnp.where((lane_z == z) & (lane_y == row_y), full, 0.0).astype(BF16)
    row_k = iota(bias_ref.shape, 0) // band_rows % classes
    bias = jnp.zeros(bias_ref.shape, F32)
    for k in range(classes):
        bias = jnp.where(row_k == k, head_bias_ref[k], bias)
    bias_ref[...] = bias

    items, count, width = weights_ref.shape
    shape = (count, width)
    slab = patch * slab_rows
    z = slab + iota(shape, 0) // per_z
    x = iota(shape, 1)
    y = (band * band_rows + iota(shape, 0) % band_rows).astype(F32) - (rows - 1) / 2.0
    across = y * y * (1.0 / (2.0 * (rows / 8.0) ** 2))
    shape = corner_ref.shape
    corner_row, corner_lane = iota(shape, 0), iota(shape, 1)
    own_z = jnp.where(corner_lane == 0, offsets_ref[0, patch], 0)
    corners = jnp.where(corner_row == items, own_z, 0)
    coverage = jnp.zeros((count, width), F32)
    weights = []
    for k in range(items):
        item = jnp.bitwise_xor(patch, k)
        start_z, start_x = offsets_ref[0, item], offsets_ref[1, item]
        first = jnp.clip(slab - start_z, -slab_rows, PZ) * per_z + count
        values = jnp.where(corner_lane == 0, first, start_x)
        corners = jnp.where((corner_row == k) & (corner_lane < 2), values, corners)
        rel_z, rel_x = z - start_z, x - start_x
        inside = (rel_z >= 0) & (rel_z < PZ) & (rel_x >= 0) & (rel_x < PX)
        far_z = rel_z.astype(F32) - (PZ - 1) / 2.0
        far_x = rel_x.astype(F32) - (PX - 1) / 2.0
        power = (
            across
            + far_z * far_z * (1.0 / (2.0 * (PZ / 8.0) ** 2))
            + far_x * far_x * (1.0 / (2.0 * (PX / 8.0) ** 2))
        )
        weight = jnp.where(inside, jnp.exp(-power), 0.0)
        weights.append(weight)
        coverage = coverage + weight
    share = 1.0 / jnp.maximum(coverage, 0.1)
    for k in range(items):
        weights_ref[k] = weights[k] * share
    corner_ref[...] = corners


def line_rows(start_z, gathered_ref, cells_ref, lines_ref, slab_rows, band_rows, spaces):
    block = slab_rows * band_rows
    pitch = block + 1
    for device in range(gathered_ref.shape[0]):
        cells_ref[device * pitch : device * pitch + block, :] = gathered_ref[device].astype(F32)
    lane = iota((spaces, PX), 1)
    empty = jnp.zeros((spaces, PX), F32)
    edge = jnp.zeros((LINE, PX), F32)
    last = band_rows * (spaces + 2) * LINE
    lines_ref[last : last + SLOTS, :] = edge[:SLOTS]
    for y in range(band_rows):
        base = y * (spaces + 2) * LINE
        lines_ref[base : base + LINE, :] = edge
        lines_ref[base + (spaces + 1) * LINE : base + (spaces + 2) * LINE, :] = edge
        base = base + LINE
        for k in (0, 1, 2, LINE - 4, LINE - 3, LINE - 2, LINE - 1):
            lines_ref[pl.ds(base + k, spaces, stride=LINE), :] = empty
    for z in range(PZ):
        deep = start_z + z
        slab = lax.div(deep, slab_rows)
        first = slab * (spaces * pitch) + (deep - slab * slab_rows) * band_rows
        for y in range(band_rows):
            line = cells_ref[pl.ds(first + y, spaces, stride=pitch), :]
            before = jnp.where(lane == 0, 0.0, pltpu.roll(line, 1, 1))
            after = jnp.where(lane == PX - 1, 0.0, pltpu.roll(line, PX - 1, 1))
            base = (y * (spaces + 2) + 1) * LINE + TAPS * (z + 1)
            for c, value in enumerate((before, line, after)):
                lines_ref[pl.ds(base + c, spaces, stride=LINE), :] = value


def tree_sum(values):
    values = list(values)
    while len(values) > 1:
        values = [
            values[i] + values[i + 1] if i + 1 < len(values) else values[i]
            for i in range(0, len(values), 2)
        ]
    return values[0]


def first_moments(lines_ref, gram_ref, weights, band_rows, spaces):
    rows = band_rows * spaces
    chunks = gram_ref.shape[0]
    size = rows // chunks
    ahead = TAPS - 1
    cells = []
    sums = [None] * rows
    for y in range(rows + ahead):
        line = []
        for z in range(PZ):
            at = (y % band_rows * (spaces + 2) + y // band_rows + 1) * LINE + TAPS * z
            value = lines_ref[at : at + SLOTS, :]
            line.append(value.astype(BF16))
            if y < rows:
                sums[y] = value if sums[y] is None else sums[y] + value
        cells.append(jnp.concatenate(line, axis=1))
    for chunk in range(chunks):
        left = jnp.concatenate(cells[chunk * size : (chunk + 1) * size], axis=0)
        right = jnp.concatenate(cells[chunk * size : (chunk + 1) * size + ahead], axis=0)
        gram_ref[chunk] = lax.dot_general(
            left, right, CONTRACT_LAST, preferred_element_type=F32
        )

    def block(y, delta, chosen):
        lane = SLOTS * (y + delta)
        tile = lane // 128 * 128
        end = min(tile + 128, gram_ref.shape[2])
        value = tree_sum(
            [gram_ref[chunk, SLOTS * y : SLOTS * (y + 1), tile:end] for chunk in chosen]
        )
        if end < tile + 128:
            value = jnp.concatenate(
                [value, jnp.zeros((SLOTS, tile + 128 - end), F32)], axis=1
            )
        return pltpu.roll(value, (tile + 128 - lane) % 128, 1) if lane != tile else value

    def total(values):
        return jnp.where(iota((SLOTS, 128), 1) < SLOTS, tree_sum(values), 0.0)

    every = range(chunks)
    head, tail = total([block(0, 0, [0])]), total([block(size - 1, 0, [chunks - 1])])
    near = total([block(y, 0, every) for y in range(size)])
    next1 = 2.0 * total([block(y, 1, every) for y in range(size)])
    next2 = 2.0 * total([block(y, 2, every) for y in range(size)])
    move = lambda value, k: pltpu.roll(value, SLOTS * k, 1)
    form = jnp.concatenate(
        [
            near - tail + move(next1, 1) + move(next2, 2),
            move(near, 1) + move(next1, 2),
            move(near - head, 2),
        ],
        axis=0,
    )[:, : TAPS * SLOTS]
    high = form.astype(BF16)
    left = form - high.astype(F32)
    middle = left.astype(BF16)
    low = (left - middle.astype(F32)).astype(BF16)
    product = jnp.dot(
        jnp.concatenate([high, middle, low], axis=0),
        weights.astype(BF16),
        preferred_element_type=F32,
    )
    size = TAPS * SLOTS
    product = product[:size] + (product[size : 2 * size] + product[2 * size :])
    squares = jnp.sum(product * weights, axis=0, keepdims=True)
    every = tree_sum(sums)
    column = jnp.concatenate([every - sums[rows - 1], every, every - sums[0]], axis=0)
    column = jnp.sum(column, axis=1, keepdims=True)
    return jnp.sum(column * weights, axis=0, keepdims=True), squares


def spread_mirror(value, f, channels):
    value = jnp.where(iota(value.shape, 1) // channels == f, value, 0.0)
    reach = channels
    while reach < value.shape[1]:
        value = value + pltpu.roll(value, reach, 1)
        reach *= 2
    return value


def main_kernel(
    spaces,
    slab_rows,
    band_rows,
    channels,
    gathered_ref,
    corner_ref,
    flat_ref,
    full_ref,
    w2t_ref,
    w2p_ref,
    params_ref,
    conv_ref,
    stats_ref,
    cells_ref,
    lines_ref,
    gram_ref,
    wide_ref,
):
    rows = band_rows * spaces
    hidden_rows = band_rows + TAPS - 1
    step = hidden_rows * channels
    band = lax.axis_index("space")
    start_z = corner_ref[lax.axis_size("patch"), 0]
    line_rows(start_z, gathered_ref, cells_ref, lines_ref, slab_rows, band_rows, spaces)

    first, second = first_moments(lines_ref, gram_ref, flat_ref[...], band_rows, spaces)
    count = float(PZ * rows * PX)
    mean = first / count
    variance = second / count - mean * mean
    lane_row = iota(mean.shape, 1) // channels % hidden_rows
    y = band * band_rows - 1 + lane_row
    inside = (y >= 0) & (y < rows)
    scale = lax.rsqrt(variance + 1e-05) * params_ref[0:1]
    shift = jnp.where(inside, params_ref[1:2] - mean * scale, 0.0)
    scale = jnp.where(inside, scale, 0.0)

    out_lanes = conv_ref.shape[2]
    half = out_lanes // 2
    groups = PZ // ZG
    empty = jnp.zeros((PX, step), BF16)
    for f in range(4):
        for g, j in ((0, 0), (groups - 1, ZI - 1)):
            at = (ZI - 1 - j if f % 2 else j) * step
            wide_ref[g, f * PX : (f + 1) * PX, at : at + step] = empty
    weights = full_ref[...]

    def hidden(cells_z):
        cells = []
        for yi in range(hidden_rows + TAPS - 1):
            base = (yi % band_rows * (spaces + 2) + yi // band_rows + band) * LINE
            line = [
                lines_ref[pl.ds(base + TAPS * z, SLOTS), :].astype(BF16) for z in cells_z
            ]
            cells.append(jnp.concatenate(line, axis=1))
        cells = jnp.concatenate(cells, axis=0)
        values = lax.dot_general(cells, weights, CONTRACT_FIRST, preferred_element_type=F32)
        for k, z in enumerate(cells_z):
            value = values[k * PX : (k + 1) * PX] * scale + shift
            value = jnp.maximum(value, 0.01 * value).astype(BF16)
            for g in range(groups):
                j = z + 1 - ZG * g
                if 0 <= j < ZI:
                    for f in range(4):
                        at = (ZI - 1 - j if f % 2 else j) * step
                        wide_ref[g, f * PX : (f + 1) * PX, at : at + step] = value[
                            :, f * step : (f + 1) * step
                        ]

    x = iota((2 * PX, out_lanes), 0) % PX
    totals = [[None] * 4, [None] * 4]
    ends = [0] + [min(ZG * g + ZG + 1, PZ) for g in range(groups)]
    hidden(range(ends[0], ends[1]))
    for g in range(groups):
        if g + 1 < groups:
            hidden(range(ends[g + 1], ends[g + 2]))
        cells = wide_ref[g]
        last = jnp.dot(cells, w2t_ref[...], preferred_element_type=F32)
        pairs = [
            jnp.dot(
                cells[:, at : at + w2p_ref.shape[0]], w2p_ref[...], preferred_element_type=F32
            )
            for at in (0, ZG // 2 * step)
        ]
        first, middle = (
            jnp.concatenate([pair[:, at : at + half] for pair in pairs], axis=1)
            for at in (0, half)
        )
        for flip in range(2):
            at = flip * 2 * PX
            before, after = (last, first) if flip else (first, last)
            value = (
                middle[at : at + 2 * PX]
                + jnp.where(x == 0, 0.0, pltpu.roll(before[at : at + 2 * PX], 1, 0))
                + jnp.where(
                    x == PX - 1, 0.0, pltpu.roll(after[at : at + 2 * PX], 2 * PX - 1, 0)
                )
            )
            conv_ref[g, at : at + 2 * PX, :] = value
            for f in (2 * flip, 2 * flip + 1):
                part = value[f * PX - at : (f + 1) * PX - at]
                for kind, item in enumerate((part, part * part)):
                    item = jnp.sum(item, axis=0, keepdims=True)
                    old = totals[kind][f]
                    totals[kind][f] = item if old is None else old + item
    sums = jnp.concatenate(totals[0] + totals[1], axis=0)
    lanes = 4 * channels
    sums = sum(sums[:, at : at + lanes] for at in range(0, out_lanes, lanes))
    reach = lanes // 2
    while reach >= channels:
        sums = sums + pltpu.roll(sums, reach, 1)
        reach //= 2
    mirror = iota((1, lanes), 1) // channels
    for kind in range(2):
        row = sums[4 * kind : 4 * kind + 1]
        for f in range(1, 4):
            row = jnp.where(mirror == f, sums[4 * kind + f : 4 * kind + f + 1], row)
        for space in range(spaces):
            stats_ref[space, kind : kind + 1, :] = row


def head_kernel(count, channels, conv_ref, stats_ref, params_ref, heads_ref, bias_ref, out_ref):
    lanes = conv_ref.shape[2]
    per_group = heads_ref.shape[1]
    sums = stats_ref[0]
    for space in range(1, stats_ref.shape[0]):
        sums = sums + stats_ref[space]
    mean = sums[0:1] / count
    variance = sums[1:2] / count - mean * mean
    scale = lax.rsqrt(variance + 1e-05) * params_ref[2:3, : 4 * channels]
    shift = params_ref[3:4, : 4 * channels] - mean * scale
    table = jnp.concatenate([scale, shift, jnp.zeros((6, 4 * channels), F32)], axis=0)
    groups = conv_ref.shape[0]
    totals = [None] * groups
    for f in range(4):
        own = spread_mirror(table, f, channels)
        own = jnp.concatenate([own] * (lanes // own.shape[1]), axis=1)
        for g in range(groups):
            value = conv_ref[g, f * PX : (f + 1) * PX, :] * own[0:1] + own[1:2]
            value = jnp.maximum(value, 0.01 * value).astype(BF16)
            logits = lax.dot_general(
                heads_ref[f % 2], value, CONTRACT_LAST, preferred_element_type=F32
            )
            totals[g] = logits if totals[g] is None else totals[g] + logits
    for g in range(groups):
        out_ref[g * per_group : (g + 1) * per_group, :] = (
            totals[g] * 0.25 + bias_ref[...]
        ).astype(out_ref.dtype)


def place_kernel(items, corner_ref, weights_ref, *refs):
    parts, (out_ref, pad_ref) = refs[:items], refs[items:]
    slab_rows, classes, band_rows, width = out_ref.shape
    per_z = classes * band_rows
    count = slab_rows * per_z
    blended = jnp.zeros((count, width), F32)
    for k in range(items):
        pad_ref[k, count : count + PZ * per_z, :] = parts[k][...].astype(F32)
        part = pad_ref[k, pl.ds(corner_ref[k, 0], count), :]
        part = jnp.concatenate([part, jnp.zeros((count, width - PX), F32)], axis=1)
        part = pltpu.roll(part, corner_ref[k, 1], 1)
        weight = weights_ref[k]
        blended = blended + jnp.where(weight > 0, part * weight, 0.0)
    for z in range(slab_rows):
        for k in range(classes):
            at = z * per_z + k * band_rows
            out_ref[z, k] = blended[at : at + band_rows]


def in_vmem(value):
    return pltpu.with_memory_space_constraint(value, pltpu.VMEM)


def in_hbm(value):
    return pltpu.with_memory_space_constraint(value, pltpu.HBM)


def local(
    image,
    offsets,
    conv1_weight,
    conv2_weight,
    norm1_gain,
    norm1_bias,
    norm2_gain,
    norm2_bias,
    head_weight,
    head_bias,
):
    groups = lax.axis_size("patch")
    spaces = lax.axis_size("space")
    slab_rows, band_rows, width = image.shape
    channels = norm1_gain.shape[0]
    classes = head_weight.shape[0]
    rows = band_rows * spaces
    hidden_rows = band_rows + TAPS - 1
    block = slab_rows * band_rows
    step = 4 * channels
    lanes1 = 4 * hidden_rows * channels
    lanes2 = ZG * band_rows * channels
    depth2 = ZI * hidden_rows * channels
    depth3 = (ZI - ZG // 2) * hidden_rows * channels
    per_z = classes * band_rows
    corners = in_hbm(offsets.T)

    windows = pl.pallas_call(
        cut_kernel,
        out_shape=pltpu.VMEM((groups * spaces, block, PX), BF16),
        in_specs=[SMEM, VMEM],
        out_specs=VMEM,
        scratch_shapes=[pltpu.VMEM((block, width), F32)],
        name="cut",
    )(corners, image)
    gathered = lax.all_to_all(in_vmem(windows), ("patch", "space"), 0, 0, tiled=True)

    flat, full, w2t, w2p, params, heads, bias, weights, corner = pl.pallas_call(
        functools.partial(prep_kernel, spaces, slab_rows, band_rows),
        out_shape=(
            pltpu.VMEM((TAPS * SLOTS, lanes1), F32),
            pltpu.VMEM(((hidden_rows + TAPS - 1) * SLOTS, lanes1), BF16),
            pltpu.VMEM((depth2, lanes2), BF16),
            pltpu.VMEM((depth3, lanes2), BF16),
            pltpu.VMEM((8, lanes1), F32),
            pltpu.VMEM((2, ZG * per_z, lanes2), BF16),
            pltpu.VMEM((ZG * per_z, PX), F32),
            pltpu.VMEM((groups, slab_rows * per_z, width), F32),
            pltpu.VMEM(((groups + 8) // 8 * 8, 128), jnp.int32),
        ),
        in_specs=[SMEM] + [VMEM] * 7 + [SMEM],
        out_specs=(VMEM,) * 9,
        scratch_shapes=[pltpu.VMEM((TAPS * SLOTS, step), F32)],
        compiler_params=pltpu.CompilerParams(vmem_limit_bytes=16 << 20),
        name="prep",
    )(
        corners,
        in_hbm(conv1_weight.transpose(0, 2, 1)),
        in_hbm(conv2_weight),
        in_hbm(norm1_gain.reshape(1, channels)),
        in_hbm(norm1_bias.reshape(1, channels)),
        in_hbm(norm2_gain.reshape(1, channels)),
        in_hbm(norm2_bias.reshape(1, channels)),
        in_hbm(head_weight),
        in_hbm(head_bias),
    )
    chunks = max(rows // 8, 1)
    scratch = (
        ((groups * spaces * (block + 1), PX), F32),
        ((band_rows * (spaces + 2) * LINE + SLOTS, PX), F32),
        ((chunks, rows // chunks * SLOTS, (rows // chunks + TAPS - 1) * SLOTS), F32),
        ((PZ // ZG, 4 * PX, depth2), BF16),
    )
    size = sum(math.prod(shape) * jnp.dtype(kind).itemsize for shape, kind in scratch)
    conv, stats = pl.pallas_call(
        functools.partial(main_kernel, spaces, slab_rows, band_rows, channels),
        out_shape=(
            pltpu.VMEM((PZ // ZG, 4 * PX, lanes2), F32),
            pltpu.VMEM((spaces, 2, step), F32),
        ),
        in_specs=[VMEM] * 7,
        out_specs=(VMEM, VMEM),
        scratch_shapes=[pltpu.VMEM(shape, kind) for shape, kind in scratch],
        compiler_params=pltpu.CompilerParams(vmem_limit_bytes=min(2 * size + (16 << 20), 40 << 20)),
        name="main",
    )(
        in_vmem(gathered),
        in_vmem(corner),
        in_vmem(flat),
        in_vmem(full),
        in_vmem(w2t),
        in_vmem(w2p),
        in_vmem(params),
    )
    stats = lax.all_to_all(stats, "space", 0, 0, tiled=True)
    averaged = pl.pallas_call(
        functools.partial(head_kernel, float(PZ * rows * PX), channels),
        out_shape=pltpu.VMEM((PZ * per_z, PX), BF16),
        in_specs=[VMEM] * 5,
        out_specs=VMEM,
        compiler_params=pltpu.CompilerParams(vmem_limit_bytes=8 << 20),
        name="head",
    )(in_vmem(conv), in_vmem(stats), in_vmem(params), in_vmem(heads), in_vmem(bias))
    parts = [averaged] + [
        lax.ppermute(averaged, "patch", [(i, i ^ k) for i in range(groups)])
        for k in range(1, groups)
    ]
    return pl.pallas_call(
        functools.partial(place_kernel, groups),
        out_shape=jax.ShapeDtypeStruct((slab_rows, classes, band_rows, width), F32),
        in_specs=[VMEM] * (2 + groups),
        out_specs=VMEM,
        scratch_shapes=[pltpu.VMEM((groups, (2 * slab_rows + PZ) * per_z, PX), F32)],
        compiler_params=pltpu.CompilerParams(vmem_limit_bytes=8 << 20),
        name="place",
    )(in_vmem(corner), in_vmem(weights), *[in_vmem(part) for part in parts])


def solution(mesh):
    return jax.shard_map(
        local,
        mesh=mesh,
        in_specs=(P("patch", "space", None), P(), P(), P(), P(), P(), P(), P(), P(), P()),
        out_specs=P("patch", None, "space", None),
        check_vma=False,
    )
```

```python
import functools
import math

import jax
import jax.numpy as jnp
from jax import lax
from jax.experimental import pallas as pl
from jax.experimental.pallas import tpu as pltpu
from jax.sharding import PartitionSpec as P

PX = 128
PZ = 16
TAPS = 3
ZG = 4
ZI = ZG + TAPS - 1
SLOTS = 16
LINE = TAPS * (PZ + 2) + 1
F32 = jnp.float32
BF16 = jnp.bfloat16
HI = lax.Precision.HIGHEST
CONTRACT_FIRST = (((0,), (0,)), ((), ()))
CONTRACT_LAST = (((1,), (1,)), ((), ()))
VMEM = pl.BlockSpec(memory_space=pltpu.VMEM)
SMEM = pl.BlockSpec(memory_space=pltpu.SMEM)


def iota(shape, dim):
    return lax.broadcasted_iota(jnp.int32, shape, dim)


def repeat_matrix(channels, lanes, dtype):
    shape = (channels, lanes)
    return (iota(shape, 0) == iota(shape, 1) % channels).astype(dtype)


def cut_kernel(offsets_ref, image_ref, out_ref, rows_ref):
    slab_rows, band_rows, width = image_ref.shape
    for z in range(slab_rows):
        rows_ref[z * band_rows : (z + 1) * band_rows, :] = image_ref[z].astype(F32)
    rows = rows_ref[...]
    items = offsets_ref.shape[1]
    spaces = out_ref.shape[0] // items
    for item in range(items):
        shift = lax.rem(width - offsets_ref[1, item], width)
        window = pltpu.roll(rows, shift, 1)[:, :PX].astype(BF16)
        for space in range(spaces):
            out_ref[space * items + item] = window


def prep_kernel(
    spaces,
    slab_rows,
    band_rows,
    offsets_ref,
    w1_ref,
    w2_ref,
    gain1_ref,
    bias1_ref,
    gain2_ref,
    bias2_ref,
    head_ref,
    head_bias_ref,
    flat_ref,
    full_ref,
    wide_ref,
    pair_ref,
    params_ref,
    heads_ref,
    bias_ref,
    weights_ref,
    corner_ref,
    narrow_ref,
):
    channels = gain1_ref.shape[1]
    classes = head_ref.shape[0]
    rows = band_rows * spaces
    hidden_rows = band_rows + TAPS - 1
    step = 4 * channels
    band = lax.axis_index("space")
    patch = lax.axis_index("patch")

    repeat = repeat_matrix(channels, step, BF16)
    taps = [
        jnp.dot(w1_ref[t], repeat, preferred_element_type=F32) for t in range(TAPS * TAPS)
    ]
    mirror = iota((1, step), 1) // channels
    narrow_ref[...] = jnp.zeros_like(narrow_ref)
    for b in range(TAPS):
        for a in range(TAPS):
            one, two = taps[a * TAPS + b], taps[(TAPS - 1 - a) * TAPS + b]
            for c in range(TAPS):
                d = TAPS - 1 - c
                row = jnp.where(
                    mirror < 2,
                    jnp.where(mirror == 0, one[c : c + 1], two[c : c + 1]),
                    jnp.where(mirror == 2, one[d : d + 1], two[d : d + 1]),
                )
                at = SLOTS * b + a * TAPS + c
                narrow_ref[at : at + 1, :] = row
    lanes = flat_ref.shape[1]
    shape = (step, lanes)
    lane = iota(shape, 1)
    spread = iota(shape, 0) == lane // (hidden_rows * channels) * channels + lane % channels
    flat = jnp.dot(
        narrow_ref[...].astype(BF16), spread.astype(BF16), preferred_element_type=F32
    )
    flat_ref[...] = flat
    lane_row = iota((SLOTS, lanes), 1) // channels % hidden_rows
    for yi in range(hidden_rows + TAPS - 1):
        piece = jnp.zeros((SLOTS, lanes), F32)
        for b in range(TAPS):
            if 0 <= yi - b < hidden_rows:
                piece = jnp.where(lane_row == yi - b, flat[SLOTS * b : SLOTS * b + SLOTS], piece)
        full_ref[SLOTS * yi : SLOTS * yi + SLOTS, :] = piece.astype(BF16)

    lanes = ZG * band_rows * channels
    spread = repeat_matrix(channels, lanes, BF16)
    taps = [
        lax.dot_general(w2_ref[t], spread, CONTRACT_FIRST, preferred_element_type=F32)
        for t in range(TAPS * TAPS)
    ]
    half = lanes // 2
    group = iota((channels, lanes), 1) // channels
    outer = TAPS - 1
    for zi in range(ZI):
        for yi in range(hidden_rows):
            at = (zi * hidden_rows + yi) * channels
            piece = jnp.zeros((channels, lanes), F32)
            pair = jnp.zeros((channels, lanes), F32)
            for zo in range(ZG):
                for yo in range(band_rows):
                    a, b = zi - zo, yi - yo
                    if 0 <= a < TAPS and 0 <= b < TAPS:
                        to = zo * band_rows + yo
                        tap = taps[a * TAPS + b]
                        piece = jnp.where(group == to, tap[outer * channels :], piece)
                        if zo < ZG // 2:
                            pair = jnp.where(group == to, tap[:channels], pair)
                            to = to + half // channels
                            pair = jnp.where(
                                group == to, tap[channels : 2 * channels], pair
                            )
            wide_ref[at : at + channels, :] = piece.astype(BF16)
            if zi < ZI - ZG // 2:
                pair_ref[at : at + channels, :] = pair.astype(BF16)

    table = jnp.concatenate(
        [
            gain1_ref[...],
            bias1_ref[...],
            gain2_ref[...],
            bias2_ref[...],
            head_ref[...].astype(F32),
            jnp.zeros((8 - classes - 4, channels), F32),
        ],
        axis=0,
    )
    spread = repeat_matrix(channels, params_ref.shape[1], F32)
    table = jnp.dot(table, spread, precision=HI, preferred_element_type=F32)
    params_ref[...] = table
    table = table[:, :lanes]

    per_z = classes * band_rows
    shape = (ZG * per_z, lanes)
    row_z = iota(shape, 0) // per_z
    row_k = iota(shape, 0) // band_rows % classes
    row_y = iota(shape, 0) % band_rows
    full = jnp.zeros(shape, F32)
    for k in range(classes):
        full = jnp.where(row_k == k, table[4 + k : 5 + k], full)
    lane_z = iota(shape, 1) // (band_rows * channels)
    lane_y = iota(shape, 1) // channels % band_rows
    for f, z in enumerate((row_z, ZG - 1 - row_z)):
        heads_ref[f] = jnp.where((lane_z == z) & (lane_y == row_y), full, 0.0).astype(BF16)
    row_k = iota(bias_ref.shape, 0) // band_rows % classes
    bias = jnp.zeros(bias_ref.shape, F32)
    for k in range(classes):
        bias = jnp.where(row_k == k, head_bias_ref[k], bias)
    bias_ref[...] = bias

    items, count, width = weights_ref.shape
    shape = (count, width)
    slab = patch * slab_rows
    z = slab + iota(shape, 0) // per_z
    x = iota(shape, 1)
    y = (band * band_rows + iota(shape, 0) % band_rows).astype(F32) - (rows - 1) / 2.0
    across = y * y * (1.0 / (2.0 * (rows / 8.0) ** 2))
    shape = corner_ref.shape
    corner_row, corner_lane = iota(shape, 0), iota(shape, 1)
    own_z = jnp.where(corner_lane == 0, offsets_ref[0, patch], 0)
    corners = jnp.where(corner_row == items, own_z, 0)
    coverage = jnp.zeros((count, width), F32)
    weights = []
    for k in range(items):
        item = jnp.bitwise_xor(patch, k)
        start_z, start_x = offsets_ref[0, item], offsets_ref[1, item]
        first = jnp.clip(slab - start_z, -slab_rows, PZ) * per_z + count
        values = jnp.where(corner_lane == 0, first, start_x)
        corners = jnp.where((corner_row == k) & (corner_lane < 2), values, corners)
        rel_z, rel_x = z - start_z, x - start_x
        inside = (rel_z >= 0) & (rel_z < PZ) & (rel_x >= 0) & (rel_x < PX)
        far_z = rel_z.astype(F32) - (PZ - 1) / 2.0
        far_x = rel_x.astype(F32) - (PX - 1) / 2.0
        power = (
            across
            + far_z * far_z * (1.0 / (2.0 * (PZ / 8.0) ** 2))
            + far_x * far_x * (1.0 / (2.0 * (PX / 8.0) ** 2))
        )
        weight = jnp.where(inside, jnp.exp(-power), 0.0)
        weights.append(weight)
        coverage = coverage + weight
    share = 1.0 / jnp.maximum(coverage, 0.1)
    for k in range(items):
        weights_ref[k] = weights[k] * share
    corner_ref[...] = corners


def line_rows(start_z, gathered_ref, cells_ref, lines_ref, slab_rows, band_rows, spaces):
    block = slab_rows * band_rows
    pitch = block + 1
    slabs = gathered_ref.shape[0] // spaces
    for device in range(gathered_ref.shape[0]):
        at = (device % slabs * spaces + device // slabs) * pitch
        cells_ref[at : at + block, :] = gathered_ref[device].astype(F32)
    lane = iota((spaces, PX), 1)
    empty = jnp.zeros((spaces, PX), F32)
    edge = jnp.zeros((LINE, PX), F32)
    last = band_rows * (spaces + 2) * LINE
    lines_ref[last : last + SLOTS, :] = edge[:SLOTS]
    for y in range(band_rows):
        base = y * (spaces + 2) * LINE
        lines_ref[base : base + LINE, :] = edge
        lines_ref[base + (spaces + 1) * LINE : base + (spaces + 2) * LINE, :] = edge
        base = base + LINE
        for k in (0, 1, 2, LINE - 4, LINE - 3, LINE - 2, LINE - 1):
            lines_ref[pl.ds(base + k, spaces, stride=LINE), :] = empty
    for z in range(PZ):
        deep = start_z + z
        slab = lax.div(deep, slab_rows)
        first = slab * (spaces * pitch) + (deep - slab * slab_rows) * band_rows
        for y in range(band_rows):
            line = cells_ref[pl.ds(first + y, spaces, stride=pitch), :]
            before = jnp.where(lane == 0, 0.0, pltpu.roll(line, 1, 1))
            after = jnp.where(lane == PX - 1, 0.0, pltpu.roll(line, PX - 1, 1))
            base = (y * (spaces + 2) + 1) * LINE + TAPS * (z + 1)
            for c, value in enumerate((before, line, after)):
                lines_ref[pl.ds(base + c, spaces, stride=LINE), :] = value


def tree_sum(values):
    values = list(values)
    while len(values) > 1:
        values = [
            values[i] + values[i + 1] if i + 1 < len(values) else values[i]
            for i in range(0, len(values), 2)
        ]
    return values[0]


def first_moments(lines_ref, gram_ref, weights, band_rows, spaces):
    rows = band_rows * spaces
    chunks = gram_ref.shape[0]
    size = rows // chunks
    ahead = TAPS - 1
    cells = []
    sums = [None] * rows
    for y in range(rows + ahead):
        line = []
        for z in range(PZ):
            at = (y % band_rows * (spaces + 2) + y // band_rows + 1) * LINE + TAPS * z
            value = lines_ref[at : at + SLOTS, :]
            line.append(value.astype(BF16))
            if y < rows:
                sums[y] = value if sums[y] is None else sums[y] + value
        cells.append(jnp.concatenate(line, axis=1))
    for chunk in range(chunks):
        left = jnp.concatenate(cells[chunk * size : (chunk + 1) * size], axis=0)
        right = jnp.concatenate(cells[chunk * size : (chunk + 1) * size + ahead], axis=0)
        gram_ref[chunk] = lax.dot_general(
            left, right, CONTRACT_LAST, preferred_element_type=F32
        )

    def block(y, delta, chosen):
        lane = SLOTS * (y + delta)
        tile = lane // 128 * 128
        end = min(tile + 128, gram_ref.shape[2])
        value = tree_sum(
            [gram_ref[chunk, SLOTS * y : SLOTS * (y + 1), tile:end] for chunk in chosen]
        )
        if end < tile + 128:
            value = jnp.concatenate(
                [value, jnp.zeros((SLOTS, tile + 128 - end), F32)], axis=1
            )
        return pltpu.roll(value, (tile + 128 - lane) % 128, 1) if lane != tile else value

    def total(values):
        return jnp.where(iota((SLOTS, 128), 1) < SLOTS, tree_sum(values), 0.0)

    every = range(chunks)
    head, tail = total([block(0, 0, [0])]), total([block(size - 1, 0, [chunks - 1])])
    near = total([block(y, 0, every) for y in range(size)])
    next1 = 2.0 * total([block(y, 1, every) for y in range(size)])
    next2 = 2.0 * total([block(y, 2, every) for y in range(size)])
    move = lambda value, k: pltpu.roll(value, SLOTS * k, 1)
    form = jnp.concatenate(
        [
            near - tail + move(next1, 1) + move(next2, 2),
            move(near, 1) + move(next1, 2),
            move(near - head, 2),
        ],
        axis=0,
    )[:, : TAPS * SLOTS]
    high = form.astype(BF16)
    left = form - high.astype(F32)
    middle = left.astype(BF16)
    low = (left - middle.astype(F32)).astype(BF16)
    product = jnp.dot(
        jnp.concatenate([high, middle, low], axis=0),
        weights.astype(BF16),
        preferred_element_type=F32,
    )
    size = TAPS * SLOTS
    product = product[:size] + (product[size : 2 * size] + product[2 * size :])
    squares = jnp.sum(product * weights, axis=0, keepdims=True)
    every = tree_sum(sums)
    column = jnp.concatenate([every - sums[rows - 1], every, every - sums[0]], axis=0)
    column = jnp.sum(column, axis=1, keepdims=True)
    return jnp.sum(column * weights, axis=0, keepdims=True), squares


def spread_mirror(value, f, channels):
    value = jnp.where(iota(value.shape, 1) // channels == f, value, 0.0)
    reach = channels
    while reach < value.shape[1]:
        value = value + pltpu.roll(value, reach, 1)
        reach *= 2
    return value


def main_kernel(
    spaces,
    slab_rows,
    band_rows,
    channels,
    gathered_ref,
    corner_ref,
    flat_ref,
    full_ref,
    w2t_ref,
    w2p_ref,
    params_ref,
    conv_ref,
    stats_ref,
    cells_ref,
    lines_ref,
    gram_ref,
    wide_ref,
):
    rows = band_rows * spaces
    hidden_rows = band_rows + TAPS - 1
    step = hidden_rows * channels
    band = lax.axis_index("space")
    start_z = corner_ref[lax.axis_size("patch"), 0]
    line_rows(start_z, gathered_ref, cells_ref, lines_ref, slab_rows, band_rows, spaces)

    first, second = first_moments(lines_ref, gram_ref, flat_ref[...], band_rows, spaces)
    count = float(PZ * rows * PX)
    mean = first / count
    variance = second / count - mean * mean
    lane_row = iota(mean.shape, 1) // channels % hidden_rows
    y = band * band_rows - 1 + lane_row
    inside = (y >= 0) & (y < rows)
    scale = lax.rsqrt(variance + 1e-05) * params_ref[0:1]
    shift = jnp.where(inside, params_ref[1:2] - mean * scale, 0.0)
    scale = jnp.where(inside, scale, 0.0)

    out_lanes = conv_ref.shape[2]
    half = out_lanes // 2
    groups = PZ // ZG
    empty = jnp.zeros((PX, step), BF16)
    for f in range(4):
        for g, j in ((0, 0), (groups - 1, ZI - 1)):
            at = (ZI - 1 - j if f % 2 else j) * step
            wide_ref[g, f * PX : (f + 1) * PX, at : at + step] = empty
    weights = full_ref[...]

    def hidden(cells_z):
        cells = []
        for yi in range(hidden_rows + TAPS - 1):
            base = (yi % band_rows * (spaces + 2) + yi // band_rows + band) * LINE
            line = [
                lines_ref[pl.ds(base + TAPS * z, SLOTS), :].astype(BF16) for z in cells_z
            ]
            cells.append(jnp.concatenate(line, axis=1))
        cells = jnp.concatenate(cells, axis=0)
        values = lax.dot_general(cells, weights, CONTRACT_FIRST, preferred_element_type=F32)
        for k, z in enumerate(cells_z):
            value = values[k * PX : (k + 1) * PX] * scale + shift
            value = jnp.maximum(value, 0.01 * value).astype(BF16)
            for g in range(groups):
                j = z + 1 - ZG * g
                if 0 <= j < ZI:
                    for f in range(4):
                        at = (ZI - 1 - j if f % 2 else j) * step
                        wide_ref[g, f * PX : (f + 1) * PX, at : at + step] = value[
                            :, f * step : (f + 1) * step
                        ]

    x = iota((2 * PX, out_lanes), 0) % PX
    totals = [[None] * 4, [None] * 4]
    ends = [0] + [min(ZG * g + ZG + 1, PZ) for g in range(groups)]
    hidden(range(ends[0], ends[1]))
    for g in range(groups):
        if g + 1 < groups:
            hidden(range(ends[g + 1], ends[g + 2]))
        spans = ((0, 4),) if g + 1 < groups else ((0, 2), (2, 4))
        for low, high in spans:
            cells = wide_ref[g, low * PX : high * PX, :]
            last = jnp.dot(cells, w2t_ref[...], preferred_element_type=F32)
            pairs = [
                jnp.dot(
                    cells[:, at : at + w2p_ref.shape[0]],
                    w2p_ref[...],
                    preferred_element_type=F32,
                )
                for at in (0, ZG // 2 * step)
            ]
            first, middle = (
                jnp.concatenate([pair[:, at : at + half] for pair in pairs], axis=1)
                for at in (0, half)
            )
            for pair in range(low, high, 2):
                at = (pair - low) * PX
                before, after = (last, first) if pair >= 2 else (first, last)
                value = (
                    middle[at : at + 2 * PX]
                    + jnp.where(x == 0, 0.0, pltpu.roll(before[at : at + 2 * PX], 1, 0))
                    + jnp.where(
                        x == PX - 1, 0.0, pltpu.roll(after[at : at + 2 * PX], 2 * PX - 1, 0)
                    )
                )
                conv_ref[g, pair * PX : (pair + 2) * PX, :] = value
                for f in (pair, pair + 1):
                    part = value[(f - pair) * PX : (f - pair + 1) * PX]
                    for kind, item in enumerate((part, part * part)):
                        item = jnp.sum(item, axis=0, keepdims=True)
                        old = totals[kind][f]
                        totals[kind][f] = item if old is None else old + item
    sums = jnp.concatenate(totals[0] + totals[1], axis=0)
    lanes = 4 * channels
    sums = sum(sums[:, at : at + lanes] for at in range(0, out_lanes, lanes))
    reach = lanes // 2
    while reach >= channels:
        sums = sums + pltpu.roll(sums, reach, 1)
        reach //= 2
    mirror = iota((1, lanes), 1) // channels
    for kind in range(2):
        row = sums[4 * kind : 4 * kind + 1]
        for f in range(1, 4):
            row = jnp.where(mirror == f, sums[4 * kind + f : 4 * kind + f + 1], row)
        for space in range(spaces):
            stats_ref[space, kind : kind + 1, :] = row


def head_kernel(count, channels, conv_ref, stats_ref, params_ref, heads_ref, bias_ref, out_ref):
    lanes = conv_ref.shape[2]
    per_group = heads_ref.shape[1]
    sums = stats_ref[0]
    for space in range(1, stats_ref.shape[0]):
        sums = sums + stats_ref[space]
    mean = sums[0:1] / count
    variance = sums[1:2] / count - mean * mean
    scale = lax.rsqrt(variance + 1e-05) * params_ref[2:3, : 4 * channels]
    shift = params_ref[3:4, : 4 * channels] - mean * scale
    table = jnp.concatenate([scale, shift, jnp.zeros((6, 4 * channels), F32)], axis=0)
    groups = conv_ref.shape[0]
    totals = [None] * groups
    for f in range(4):
        own = spread_mirror(table, f, channels)
        own = jnp.concatenate([own] * (lanes // own.shape[1]), axis=1)
        for g in range(groups):
            value = conv_ref[g, f * PX : (f + 1) * PX, :] * own[0:1] + own[1:2]
            value = jnp.maximum(value, 0.01 * value).astype(BF16)
            logits = lax.dot_general(
                heads_ref[f % 2], value, CONTRACT_LAST, preferred_element_type=F32
            )
            totals[g] = logits if totals[g] is None else totals[g] + logits
    for g in range(groups):
        out_ref[g * per_group : (g + 1) * per_group, :] = (
            totals[g] * 0.25 + bias_ref[...]
        ).astype(out_ref.dtype)


def place_kernel(items, corner_ref, weights_ref, *refs):
    parts, (out_ref, pad_ref) = refs[:items], refs[items:]
    slab_rows, classes, band_rows, width = out_ref.shape
    per_z = classes * band_rows
    count = slab_rows * per_z
    blended = jnp.zeros((count, width), F32)
    for k in range(items):
        pad_ref[k, count : count + PZ * per_z, :] = parts[k][...].astype(F32)
        part = pad_ref[k, pl.ds(corner_ref[k, 0], count), :]
        part = jnp.concatenate([part, jnp.zeros((count, width - PX), F32)], axis=1)
        part = pltpu.roll(part, corner_ref[k, 1], 1)
        weight = weights_ref[k]
        blended = blended + jnp.where(weight > 0, part * weight, 0.0)
    for z in range(slab_rows):
        for k in range(classes):
            at = z * per_z + k * band_rows
            out_ref[z, k] = blended[at : at + band_rows]


def in_vmem(value):
    return pltpu.with_memory_space_constraint(value, pltpu.VMEM)


def in_hbm(value):
    return pltpu.with_memory_space_constraint(value, pltpu.HBM)


def local(
    image,
    offsets,
    conv1_weight,
    conv2_weight,
    norm1_gain,
    norm1_bias,
    norm2_gain,
    norm2_bias,
    head_weight,
    head_bias,
):
    groups = lax.axis_size("patch")
    spaces = lax.axis_size("space")
    slab_rows, band_rows, width = image.shape
    channels = norm1_gain.shape[0]
    classes = head_weight.shape[0]
    rows = band_rows * spaces
    hidden_rows = band_rows + TAPS - 1
    block = slab_rows * band_rows
    step = 4 * channels
    lanes1 = 4 * hidden_rows * channels
    lanes2 = ZG * band_rows * channels
    depth2 = ZI * hidden_rows * channels
    depth3 = (ZI - ZG // 2) * hidden_rows * channels
    per_z = classes * band_rows
    corners = in_hbm(offsets.T)

    windows = pl.pallas_call(
        cut_kernel,
        out_shape=pltpu.VMEM((groups * spaces, block, PX), BF16),
        in_specs=[SMEM, VMEM],
        out_specs=VMEM,
        scratch_shapes=[pltpu.VMEM((block, width), F32)],
        name="cut",
    )(corners, image)
    gathered = lax.all_to_all(windows, ("space", "patch"), 0, 0, tiled=True)

    flat, full, w2t, w2p, params, heads, bias, weights, corner = pl.pallas_call(
        functools.partial(prep_kernel, spaces, slab_rows, band_rows),
        out_shape=(
            pltpu.VMEM((TAPS * SLOTS, lanes1), F32),
            pltpu.VMEM(((hidden_rows + TAPS - 1) * SLOTS, lanes1), BF16),
            pltpu.VMEM((depth2, lanes2), BF16),
            pltpu.VMEM((depth3, lanes2), BF16),
            pltpu.VMEM((8, lanes1), F32),
            pltpu.VMEM((2, ZG * per_z, lanes2), BF16),
            pltpu.VMEM((ZG * per_z, PX), F32),
            pltpu.VMEM((groups, slab_rows * per_z, width), F32),
            pltpu.VMEM(((groups + 8) // 8 * 8, 128), jnp.int32),
        ),
        in_specs=[SMEM] + [VMEM] * 7 + [SMEM],
        out_specs=(VMEM,) * 9,
        scratch_shapes=[pltpu.VMEM((TAPS * SLOTS, step), F32)],
        compiler_params=pltpu.CompilerParams(vmem_limit_bytes=16 << 20),
        name="prep",
    )(
        corners,
        in_hbm(conv1_weight.transpose(0, 2, 1)),
        in_hbm(conv2_weight),
        in_hbm(norm1_gain.reshape(1, channels)),
        in_hbm(norm1_bias.reshape(1, channels)),
        in_hbm(norm2_gain.reshape(1, channels)),
        in_hbm(norm2_bias.reshape(1, channels)),
        in_hbm(head_weight),
        in_hbm(head_bias),
    )
    chunks = max(rows // 8, 1)
    scratch = (
        ((groups * spaces * (block + 1), PX), F32),
        ((band_rows * (spaces + 2) * LINE + SLOTS, PX), F32),
        ((chunks, rows // chunks * SLOTS, (rows // chunks + TAPS - 1) * SLOTS), F32),
        ((PZ // ZG, 4 * PX, depth2), BF16),
    )
    size = sum(math.prod(shape) * jnp.dtype(kind).itemsize for shape, kind in scratch)
    conv, stats = pl.pallas_call(
        functools.partial(main_kernel, spaces, slab_rows, band_rows, channels),
        out_shape=(
            pltpu.VMEM((PZ // ZG, 4 * PX, lanes2), F32),
            pltpu.VMEM((spaces, 2, step), F32),
        ),
        in_specs=[VMEM] * 7,
        out_specs=(VMEM, VMEM),
        scratch_shapes=[pltpu.VMEM(shape, kind) for shape, kind in scratch],
        compiler_params=pltpu.CompilerParams(vmem_limit_bytes=min(2 * size + (16 << 20), 40 << 20)),
        name="main",
    )(
        in_vmem(gathered),
        in_vmem(corner),
        in_vmem(flat),
        in_vmem(full),
        in_vmem(w2t),
        in_vmem(w2p),
        in_vmem(params),
    )
    stats = lax.all_to_all(stats, "space", 0, 0, tiled=True)
    averaged = pl.pallas_call(
        functools.partial(head_kernel, float(PZ * rows * PX), channels),
        out_shape=pltpu.VMEM((PZ * per_z, PX), BF16),
        in_specs=[VMEM] * 5,
        out_specs=VMEM,
        compiler_params=pltpu.CompilerParams(vmem_limit_bytes=8 << 20),
        name="head",
    )(in_vmem(conv), in_vmem(stats), in_vmem(params), in_vmem(heads), in_vmem(bias))
    parts = [averaged] + [
        lax.ppermute(averaged, "patch", [(i, i ^ k) for i in range(groups)])
        for k in range(1, groups)
    ]
    return pl.pallas_call(
        functools.partial(place_kernel, groups),
        out_shape=jax.ShapeDtypeStruct((slab_rows, classes, band_rows, width), F32),
        in_specs=[VMEM] * (2 + groups),
        out_specs=VMEM,
        scratch_shapes=[pltpu.VMEM((groups, (2 * slab_rows + PZ) * per_z, PX), F32)],
        compiler_params=pltpu.CompilerParams(vmem_limit_bytes=8 << 20),
        name="place",
    )(in_vmem(corner), in_vmem(weights), *[in_vmem(part) for part in parts])


def solution(mesh):
    return jax.shard_map(
        local,
        mesh=mesh,
        in_specs=(P("patch", "space", None), P(), P(), P(), P(), P(), P(), P(), P(), P()),
        out_specs=P("patch", None, "space", None),
        check_vma=False,
    )
```

```python
import functools
import math

import jax
import jax.numpy as jnp
from jax import lax
from jax.experimental import pallas as pl
from jax.experimental.pallas import tpu as pltpu
from jax.sharding import PartitionSpec as P

PX = 128
PZ = 16
TAPS = 3
ZG = 4
ZI = ZG + TAPS - 1
SLOTS = 16
LINE = TAPS * (PZ + 2) + 1
F32 = jnp.float32
BF16 = jnp.bfloat16
HI = lax.Precision.HIGHEST
CONTRACT_FIRST = (((0,), (0,)), ((), ()))
CONTRACT_LAST = (((1,), (1,)), ((), ()))
VMEM = pl.BlockSpec(memory_space=pltpu.VMEM)
SMEM = pl.BlockSpec(memory_space=pltpu.SMEM)


def iota(shape, dim):
    return lax.broadcasted_iota(jnp.int32, shape, dim)


def repeat_matrix(channels, lanes, dtype):
    shape = (channels, lanes)
    return (iota(shape, 0) == iota(shape, 1) % channels).astype(dtype)


def cut_kernel(offsets_ref, image_ref, out_ref, rows_ref):
    slab_rows, band_rows, width = image_ref.shape
    for z in range(slab_rows):
        rows_ref[z * band_rows : (z + 1) * band_rows, :] = image_ref[z].astype(F32)
    rows = rows_ref[...]
    items = offsets_ref.shape[1]
    spaces = out_ref.shape[0] // items
    for item in range(items):
        shift = lax.rem(width - offsets_ref[1, item], width)
        window = pltpu.roll(rows, shift, 1)[:, :PX].astype(BF16)
        for space in range(spaces):
            out_ref[space * items + item] = window


def prep_kernel(
    spaces,
    slab_rows,
    band_rows,
    offsets_ref,
    w1_ref,
    w2_ref,
    gain1_ref,
    bias1_ref,
    gain2_ref,
    bias2_ref,
    head_ref,
    head_bias_ref,
    flat_ref,
    full_ref,
    wide_ref,
    pair_ref,
    params_ref,
    heads_ref,
    bias_ref,
    weights_ref,
    corner_ref,
    narrow_ref,
):
    channels = gain1_ref.shape[1]
    classes = head_ref.shape[0]
    rows = band_rows * spaces
    hidden_rows = band_rows + TAPS - 1
    step = 4 * channels
    band = lax.axis_index("space")
    patch = lax.axis_index("patch")

    repeat = repeat_matrix(channels, step, BF16)
    taps = [
        jnp.dot(w1_ref[t], repeat, preferred_element_type=F32) for t in range(TAPS * TAPS)
    ]
    mirror = iota((1, step), 1) // channels
    narrow_ref[...] = jnp.zeros_like(narrow_ref)
    for b in range(TAPS):
        for a in range(TAPS):
            one, two = taps[a * TAPS + b], taps[(TAPS - 1 - a) * TAPS + b]
            for c in range(TAPS):
                d = TAPS - 1 - c
                row = jnp.where(
                    mirror < 2,
                    jnp.where(mirror == 0, one[c : c + 1], two[c : c + 1]),
                    jnp.where(mirror == 2, one[d : d + 1], two[d : d + 1]),
                )
                at = SLOTS * b + a * TAPS + c
                narrow_ref[at : at + 1, :] = row
    lanes = flat_ref.shape[1]
    shape = (step, lanes)
    lane = iota(shape, 1)
    spread = iota(shape, 0) == lane // (hidden_rows * channels) * channels + lane % channels
    flat = jnp.dot(
        narrow_ref[...].astype(BF16), spread.astype(BF16), preferred_element_type=F32
    )
    flat_ref[...] = flat
    lane_row = iota((SLOTS, lanes), 1) // channels % hidden_rows
    for yi in range(hidden_rows + TAPS - 1):
        piece = jnp.zeros((SLOTS, lanes), F32)
        for b in range(TAPS):
            if 0 <= yi - b < hidden_rows:
                piece = jnp.where(lane_row == yi - b, flat[SLOTS * b : SLOTS * b + SLOTS], piece)
        full_ref[SLOTS * yi : SLOTS * yi + SLOTS, :] = piece.astype(BF16)

    lanes = ZG * band_rows * channels
    spread = repeat_matrix(channels, lanes, BF16)
    taps = [
        lax.dot_general(w2_ref[t], spread, CONTRACT_FIRST, preferred_element_type=F32)
        for t in range(TAPS * TAPS)
    ]
    half = lanes // 2
    group = iota((channels, lanes), 1) // channels
    outer = TAPS - 1
    for zi in range(ZI):
        for yi in range(hidden_rows):
            at = (zi * hidden_rows + yi) * channels
            piece = jnp.zeros((channels, lanes), F32)
            pair = jnp.zeros((channels, lanes), F32)
            for zo in range(ZG):
                for yo in range(band_rows):
                    a, b = zi - zo, yi - yo
                    if 0 <= a < TAPS and 0 <= b < TAPS:
                        to = zo * band_rows + yo
                        tap = taps[a * TAPS + b]
                        piece = jnp.where(group == to, tap[outer * channels :], piece)
                        if zo < ZG // 2:
                            pair = jnp.where(group == to, tap[:channels], pair)
                            to = to + half // channels
                            pair = jnp.where(
                                group == to, tap[channels : 2 * channels], pair
                            )
            wide_ref[at : at + channels, :] = piece.astype(BF16)
            if zi < ZI - ZG // 2:
                pair_ref[at : at + channels, :] = pair.astype(BF16)

    table = jnp.concatenate(
        [
            gain1_ref[...],
            bias1_ref[...],
            gain2_ref[...],
            bias2_ref[...],
            head_ref[...].astype(F32),
            jnp.zeros((8 - classes - 4, channels), F32),
        ],
        axis=0,
    )
    spread = repeat_matrix(channels, params_ref.shape[1], F32)
    table = jnp.dot(table, spread, precision=HI, preferred_element_type=F32)
    params_ref[...] = table
    table = table[:, :lanes]

    per_z = classes * band_rows
    shape = (ZG * per_z, lanes)
    row_z = iota(shape, 0) // per_z
    row_k = iota(shape, 0) // band_rows % classes
    row_y = iota(shape, 0) % band_rows
    full = jnp.zeros(shape, F32)
    for k in range(classes):
        full = jnp.where(row_k == k, table[4 + k : 5 + k], full)
    lane_z = iota(shape, 1) // (band_rows * channels)
    lane_y = iota(shape, 1) // channels % band_rows
    for f, z in enumerate((row_z, ZG - 1 - row_z)):
        heads_ref[f] = jnp.where((lane_z == z) & (lane_y == row_y), full, 0.0).astype(BF16)
    row_k = iota(bias_ref.shape, 0) // band_rows % classes
    bias = jnp.zeros(bias_ref.shape, F32)
    for k in range(classes):
        bias = jnp.where(row_k == k, head_bias_ref[k], bias)
    bias_ref[...] = bias

    items, count, width = weights_ref.shape
    shape = (count, width)
    slab = patch * slab_rows
    z = slab + iota(shape, 0) // per_z
    x = iota(shape, 1)
    y = (band * band_rows + iota(shape, 0) % band_rows).astype(F32) - (rows - 1) / 2.0
    across = y * y * (1.0 / (2.0 * (rows / 8.0) ** 2))
    shape = corner_ref.shape
    corner_row, corner_lane = iota(shape, 0), iota(shape, 1)
    own_z = jnp.where(corner_lane == 0, offsets_ref[0, patch], 0)
    corners = jnp.where(corner_row == items, own_z, 0)
    coverage = jnp.zeros((count, width), F32)
    weights = []
    for k in range(items):
        item = jnp.bitwise_xor(patch, k)
        start_z, start_x = offsets_ref[0, item], offsets_ref[1, item]
        first = jnp.clip(slab - start_z, -slab_rows, PZ) * per_z + count
        values = jnp.where(corner_lane == 0, first, start_x)
        corners = jnp.where((corner_row == k) & (corner_lane < 2), values, corners)
        rel_z, rel_x = z - start_z, x - start_x
        inside = (rel_z >= 0) & (rel_z < PZ) & (rel_x >= 0) & (rel_x < PX)
        far_z = rel_z.astype(F32) - (PZ - 1) / 2.0
        far_x = rel_x.astype(F32) - (PX - 1) / 2.0
        power = (
            across
            + far_z * far_z * (1.0 / (2.0 * (PZ / 8.0) ** 2))
            + far_x * far_x * (1.0 / (2.0 * (PX / 8.0) ** 2))
        )
        weight = jnp.where(inside, jnp.exp(-power), 0.0)
        weights.append(weight)
        coverage = coverage + weight
    share = 1.0 / jnp.maximum(coverage, 0.1)
    for k in range(items):
        weights_ref[k] = weights[k] * share
    corner_ref[...] = corners


def line_rows(start_z, gathered_ref, cells_ref, lines_ref, slab_rows, band_rows, spaces):
    block = slab_rows * band_rows
    pitch = block + 1
    slabs = gathered_ref.shape[0] // spaces
    for device in range(gathered_ref.shape[0]):
        at = (device % slabs * spaces + device // slabs) * pitch
        cells_ref[at : at + block, :] = gathered_ref[device].astype(F32)
    lane = iota((spaces, PX), 1)
    empty = jnp.zeros((spaces, PX), F32)
    edge = jnp.zeros((LINE, PX), F32)
    last = band_rows * (spaces + 2) * LINE
    lines_ref[last : last + SLOTS, :] = edge[:SLOTS]
    for y in range(band_rows):
        base = y * (spaces + 2) * LINE
        lines_ref[base : base + LINE, :] = edge
        lines_ref[base + (spaces + 1) * LINE : base + (spaces + 2) * LINE, :] = edge
        base = base + LINE
        for k in (0, 1, 2, LINE - 4, LINE - 3, LINE - 2, LINE - 1):
            lines_ref[pl.ds(base + k, spaces, stride=LINE), :] = empty
    for z in range(PZ):
        deep = start_z + z
        slab = lax.div(deep, slab_rows)
        first = slab * (spaces * pitch) + (deep - slab * slab_rows) * band_rows
        for y in range(band_rows):
            line = cells_ref[pl.ds(first + y, spaces, stride=pitch), :]
            before = jnp.where(lane == 0, 0.0, pltpu.roll(line, 1, 1))
            after = jnp.where(lane == PX - 1, 0.0, pltpu.roll(line, PX - 1, 1))
            base = (y * (spaces + 2) + 1) * LINE + TAPS * (z + 1)
            for c, value in enumerate((before, line, after)):
                lines_ref[pl.ds(base + c, spaces, stride=LINE), :] = value


def tree_sum(values):
    values = list(values)
    while len(values) > 1:
        values = [
            values[i] + values[i + 1] if i + 1 < len(values) else values[i]
            for i in range(0, len(values), 2)
        ]
    return values[0]


def first_moments(lines_ref, gram_ref, weights, band_rows, spaces):
    rows = band_rows * spaces
    chunks = gram_ref.shape[0]
    size = rows // chunks
    ahead = TAPS - 1
    cells = []
    sums = [None] * rows
    for y in range(rows + ahead):
        line = []
        for z in range(PZ):
            at = (y % band_rows * (spaces + 2) + y // band_rows + 1) * LINE + TAPS * z
            value = lines_ref[at : at + SLOTS, :]
            line.append(value.astype(BF16))
            if y < rows:
                sums[y] = value if sums[y] is None else sums[y] + value
        cells.append(jnp.concatenate(line, axis=1))
    for chunk in range(chunks):
        left = jnp.concatenate(cells[chunk * size : (chunk + 1) * size], axis=0)
        right = jnp.concatenate(cells[chunk * size : (chunk + 1) * size + ahead], axis=0)
        gram_ref[chunk] = lax.dot_general(
            left, right, CONTRACT_LAST, preferred_element_type=F32
        )

    def block(y, delta, chosen):
        lane = SLOTS * (y + delta)
        tile = lane // 128 * 128
        end = min(tile + 128, gram_ref.shape[2])
        value = tree_sum(
            [gram_ref[chunk, SLOTS * y : SLOTS * (y + 1), tile:end] for chunk in chosen]
        )
        if end < tile + 128:
            value = jnp.concatenate(
                [value, jnp.zeros((SLOTS, tile + 128 - end), F32)], axis=1
            )
        return pltpu.roll(value, (tile + 128 - lane) % 128, 1) if lane != tile else value

    def total(values):
        return jnp.where(iota((SLOTS, 128), 1) < SLOTS, tree_sum(values), 0.0)

    every = range(chunks)
    head, tail = total([block(0, 0, [0])]), total([block(size - 1, 0, [chunks - 1])])
    near = total([block(y, 0, every) for y in range(size)])
    next1 = 2.0 * total([block(y, 1, every) for y in range(size)])
    next2 = 2.0 * total([block(y, 2, every) for y in range(size)])
    move = lambda value, k: pltpu.roll(value, SLOTS * k, 1)
    form = jnp.concatenate(
        [
            near - tail + move(next1, 1) + move(next2, 2),
            move(near, 1) + move(next1, 2),
            move(near - head, 2),
        ],
        axis=0,
    )[:, : TAPS * SLOTS]
    high = form.astype(BF16)
    left = form - high.astype(F32)
    middle = left.astype(BF16)
    low = (left - middle.astype(F32)).astype(BF16)
    product = jnp.dot(
        jnp.concatenate([high, middle, low], axis=0),
        weights.astype(BF16),
        preferred_element_type=F32,
    )
    size = TAPS * SLOTS
    product = product[:size] + (product[size : 2 * size] + product[2 * size :])
    squares = jnp.sum(product * weights, axis=0, keepdims=True)
    every = tree_sum(sums)
    column = jnp.concatenate([every - sums[rows - 1], every, every - sums[0]], axis=0)
    column = jnp.sum(column, axis=1, keepdims=True)
    return jnp.sum(column * weights, axis=0, keepdims=True), squares


def spread_mirror(value, f, channels):
    value = jnp.where(iota(value.shape, 1) // channels == f, value, 0.0)
    reach = channels
    while reach < value.shape[1]:
        value = value + pltpu.roll(value, reach, 1)
        reach *= 2
    return value


def main_kernel(
    spaces,
    slab_rows,
    band_rows,
    channels,
    gathered_ref,
    corner_ref,
    flat_ref,
    full_ref,
    w2t_ref,
    w2p_ref,
    params_ref,
    conv_ref,
    stats_ref,
    cells_ref,
    lines_ref,
    gram_ref,
    wide_ref,
):
    rows = band_rows * spaces
    hidden_rows = band_rows + TAPS - 1
    step = hidden_rows * channels
    band = lax.axis_index("space")
    start_z = corner_ref[lax.axis_size("patch"), 0]
    line_rows(start_z, gathered_ref, cells_ref, lines_ref, slab_rows, band_rows, spaces)

    first, second = first_moments(lines_ref, gram_ref, flat_ref[...], band_rows, spaces)
    count = float(PZ * rows * PX)
    mean = first / count
    variance = second / count - mean * mean
    lane_row = iota(mean.shape, 1) // channels % hidden_rows
    y = band * band_rows - 1 + lane_row
    inside = (y >= 0) & (y < rows)
    scale = lax.rsqrt(variance + 1e-05) * params_ref[0:1]
    shift = jnp.where(inside, params_ref[1:2] - mean * scale, 0.0)
    scale = jnp.where(inside, scale, 0.0)

    out_lanes = conv_ref.shape[2]
    half = out_lanes // 2
    groups = PZ // ZG
    empty = jnp.zeros((PX, step), BF16)
    for f in range(4):
        for g, j in ((0, 0), (groups - 1, ZI - 1)):
            at = (ZI - 1 - j if f % 2 else j) * step
            wide_ref[g, f * PX : (f + 1) * PX, at : at + step] = empty
    weights = full_ref[...]

    def hidden(cells_z):
        cells = []
        for yi in range(hidden_rows + TAPS - 1):
            base = (yi % band_rows * (spaces + 2) + yi // band_rows + band) * LINE
            line = [
                lines_ref[pl.ds(base + TAPS * z, SLOTS), :].astype(BF16) for z in cells_z
            ]
            cells.append(jnp.concatenate(line, axis=1))
        cells = jnp.concatenate(cells, axis=0)
        values = lax.dot_general(cells, weights, CONTRACT_FIRST, preferred_element_type=F32)
        for k, z in enumerate(cells_z):
            value = values[k * PX : (k + 1) * PX] * scale + shift
            value = jnp.maximum(value, 0.01 * value).astype(BF16)
            for g in range(groups):
                j = z + 1 - ZG * g
                if 0 <= j < ZI:
                    for f in range(4):
                        at = (ZI - 1 - j if f % 2 else j) * step
                        wide_ref[g, f * PX : (f + 1) * PX, at : at + step] = value[
                            :, f * step : (f + 1) * step
                        ]

    x = iota((2 * PX, out_lanes), 0) % PX
    totals = [[None] * 4, [None] * 4]
    ends = [0] + [min(ZG * g + ZG + 1, PZ) for g in range(groups)]
    hidden(range(ends[0], ends[1]))
    for g in range(groups):
        if g + 1 < groups:
            hidden(range(ends[g + 1], ends[g + 2]))
        spans = ((0, 4),) if g + 1 < groups else ((0, 2), (2, 4))
        for low, high in spans:
            cells = wide_ref[g, low * PX : high * PX, :]
            last = jnp.dot(cells, w2t_ref[...], preferred_element_type=F32)
            pairs = [
                jnp.dot(
                    cells[:, at : at + w2p_ref.shape[0]],
                    w2p_ref[...],
                    preferred_element_type=F32,
                )
                for at in (0, ZG // 2 * step)
            ]
            first, middle = (
                jnp.concatenate([pair[:, at : at + half] for pair in pairs], axis=1)
                for at in (0, half)
            )
            for pair in range(low, high, 2):
                at = (pair - low) * PX
                before, after = (last, first) if pair >= 2 else (first, last)
                value = (
                    middle[at : at + 2 * PX]
                    + jnp.where(x == 0, 0.0, pltpu.roll(before[at : at + 2 * PX], 1, 0))
                    + jnp.where(
                        x == PX - 1, 0.0, pltpu.roll(after[at : at + 2 * PX], 2 * PX - 1, 0)
                    )
                )
                conv_ref[g, pair * PX : (pair + 2) * PX, :] = value
                for f in (pair, pair + 1):
                    part = value[(f - pair) * PX : (f - pair + 1) * PX]
                    for kind, item in enumerate((part, part * part)):
                        item = jnp.sum(item, axis=0, keepdims=True)
                        old = totals[kind][f]
                        totals[kind][f] = item if old is None else old + item
    sums = jnp.concatenate(totals[0] + totals[1], axis=0)
    lanes = 4 * channels
    sums = sum(sums[:, at : at + lanes] for at in range(0, out_lanes, lanes))
    reach = lanes // 2
    while reach >= channels:
        sums = sums + pltpu.roll(sums, reach, 1)
        reach //= 2
    mirror = iota((1, lanes), 1) // channels
    for kind in range(2):
        row = sums[4 * kind : 4 * kind + 1]
        for f in range(1, 4):
            row = jnp.where(mirror == f, sums[4 * kind + f : 4 * kind + f + 1], row)
        for space in range(spaces):
            stats_ref[space, kind : kind + 1, :] = row


def head_kernel(count, channels, conv_ref, stats_ref, params_ref, heads_ref, bias_ref, out_ref):
    lanes = conv_ref.shape[2]
    per_group = heads_ref.shape[1]
    sums = stats_ref[0]
    for space in range(1, stats_ref.shape[0]):
        sums = sums + stats_ref[space]
    mean = sums[0:1] / count
    variance = sums[1:2] / count - mean * mean
    scale = lax.rsqrt(variance + 1e-05) * params_ref[2:3, : 4 * channels]
    shift = params_ref[3:4, : 4 * channels] - mean * scale
    table = jnp.concatenate([scale, shift, jnp.zeros((6, 4 * channels), F32)], axis=0)
    groups = conv_ref.shape[0]
    totals = [None] * groups
    for f in range(4):
        own = spread_mirror(table, f, channels)
        own = jnp.concatenate([own] * (lanes // own.shape[1]), axis=1)
        for g in range(groups):
            value = conv_ref[g, f * PX : (f + 1) * PX, :] * own[0:1] + own[1:2]
            value = jnp.maximum(value, 0.01 * value).astype(BF16)
            logits = lax.dot_general(
                heads_ref[f % 2], value, CONTRACT_LAST, preferred_element_type=F32
            )
            totals[g] = logits if totals[g] is None else totals[g] + logits
    for g in range(groups):
        out_ref[g * per_group : (g + 1) * per_group, :] = (
            totals[g] * 0.25 + bias_ref[...]
        ).astype(out_ref.dtype)


def place_kernel(items, corner_ref, weights_ref, *refs):
    parts, (out_ref, pad_ref) = refs[:items], refs[items:]
    slab_rows, classes, band_rows, width = out_ref.shape
    per_z = classes * band_rows
    count = slab_rows * per_z
    blended = jnp.zeros((count, width), F32)
    for k in range(items):
        pad_ref[k, count : count + PZ * per_z, :] = parts[k][...].astype(F32)
        part = pad_ref[k, pl.ds(corner_ref[k, 0], count), :]
        part = jnp.concatenate([part, jnp.zeros((count, width - PX), F32)], axis=1)
        part = pltpu.roll(part, corner_ref[k, 1], 1)
        weight = weights_ref[k]
        blended = blended + jnp.where(weight > 0, part * weight, 0.0)
    for z in range(slab_rows):
        for k in range(classes):
            at = z * per_z + k * band_rows
            out_ref[z, k] = blended[at : at + band_rows]


def in_vmem(value):
    return pltpu.with_memory_space_constraint(value, pltpu.VMEM)


def in_hbm(value):
    return pltpu.with_memory_space_constraint(value, pltpu.HBM)


def local(
    image,
    offsets,
    conv1_weight,
    conv2_weight,
    norm1_gain,
    norm1_bias,
    norm2_gain,
    norm2_bias,
    head_weight,
    head_bias,
):
    groups = lax.axis_size("patch")
    spaces = lax.axis_size("space")
    slab_rows, band_rows, width = image.shape
    channels = norm1_gain.shape[0]
    classes = head_weight.shape[0]
    rows = band_rows * spaces
    hidden_rows = band_rows + TAPS - 1
    block = slab_rows * band_rows
    step = 4 * channels
    lanes1 = 4 * hidden_rows * channels
    lanes2 = ZG * band_rows * channels
    depth2 = ZI * hidden_rows * channels
    depth3 = (ZI - ZG // 2) * hidden_rows * channels
    per_z = classes * band_rows
    corners = in_hbm(offsets.T)

    windows = pl.pallas_call(
        cut_kernel,
        out_shape=pltpu.VMEM((groups * spaces, block, PX), BF16),
        in_specs=[SMEM, VMEM],
        out_specs=VMEM,
        scratch_shapes=[pltpu.VMEM((block, width), F32)],
        name="cut",
    )(corners, image)
    gathered = lax.all_to_all(windows, ("space", "patch"), 0, 0, tiled=True)

    flat, full, w2t, w2p, params, heads, bias, weights, corner = pl.pallas_call(
        functools.partial(prep_kernel, spaces, slab_rows, band_rows),
        out_shape=(
            pltpu.VMEM((TAPS * SLOTS, lanes1), F32),
            pltpu.VMEM(((hidden_rows + TAPS - 1) * SLOTS, lanes1), BF16),
            pltpu.VMEM((depth2, lanes2), BF16),
            pltpu.VMEM((depth3, lanes2), BF16),
            pltpu.VMEM((8, lanes1), F32),
            pltpu.VMEM((2, ZG * per_z, lanes2), BF16),
            pltpu.VMEM((ZG * per_z, PX), F32),
            pltpu.VMEM((groups, slab_rows * per_z, width), F32),
            pltpu.VMEM(((groups + 8) // 8 * 8, 128), jnp.int32),
        ),
        in_specs=[SMEM] + [VMEM] * 7 + [SMEM],
        out_specs=(VMEM,) * 9,
        scratch_shapes=[pltpu.VMEM((TAPS * SLOTS, step), F32)],
        compiler_params=pltpu.CompilerParams(vmem_limit_bytes=16 << 20),
        name="prep",
    )(
        corners,
        in_hbm(conv1_weight.transpose(0, 2, 1)),
        in_hbm(conv2_weight),
        in_hbm(norm1_gain.reshape(1, channels)),
        in_hbm(norm1_bias.reshape(1, channels)),
        in_hbm(norm2_gain.reshape(1, channels)),
        in_hbm(norm2_bias.reshape(1, channels)),
        in_hbm(head_weight),
        in_hbm(head_bias),
    )
    chunks = max(rows // 8, 1)
    scratch = (
        ((groups * spaces * (block + 1), PX), F32),
        ((band_rows * (spaces + 2) * LINE + SLOTS, PX), F32),
        ((chunks, rows // chunks * SLOTS, (rows // chunks + TAPS - 1) * SLOTS), F32),
        ((PZ // ZG, 4 * PX, depth2), BF16),
    )
    size = sum(math.prod(shape) * jnp.dtype(kind).itemsize for shape, kind in scratch)
    conv, stats = pl.pallas_call(
        functools.partial(main_kernel, spaces, slab_rows, band_rows, channels),
        out_shape=(
            pltpu.VMEM((PZ // ZG, 4 * PX, lanes2), F32),
            pltpu.VMEM((spaces, 2, step), F32),
        ),
        in_specs=[VMEM] * 7,
        out_specs=(VMEM, VMEM),
        scratch_shapes=[pltpu.VMEM(shape, kind) for shape, kind in scratch],
        compiler_params=pltpu.CompilerParams(vmem_limit_bytes=min(2 * size + (16 << 20), 40 << 20)),
        name="main",
    )(
        in_vmem(gathered),
        in_vmem(corner),
        in_vmem(flat),
        in_vmem(full),
        in_vmem(w2t),
        in_vmem(w2p),
        in_vmem(params),
    )
    stats = lax.all_to_all(stats, "space", 0, 0, tiled=True)
    averaged = pl.pallas_call(
        functools.partial(head_kernel, float(PZ * rows * PX), channels),
        out_shape=pltpu.VMEM((PZ * per_z, PX), F32),
        in_specs=[VMEM] * 5,
        out_specs=VMEM,
        compiler_params=pltpu.CompilerParams(vmem_limit_bytes=8 << 20),
        name="head",
    )(in_vmem(conv), in_vmem(stats), in_vmem(params), in_vmem(heads), in_vmem(bias))
    parts = [averaged] + [
        lax.ppermute(averaged, "patch", [(i, i ^ k) for i in range(groups)])
        for k in range(1, groups)
    ]
    return pl.pallas_call(
        functools.partial(place_kernel, groups),
        out_shape=jax.ShapeDtypeStruct((slab_rows, classes, band_rows, width), F32),
        in_specs=[VMEM] * (2 + groups),
        out_specs=VMEM,
        scratch_shapes=[pltpu.VMEM((groups, (2 * slab_rows + PZ) * per_z, PX), F32)],
        compiler_params=pltpu.CompilerParams(vmem_limit_bytes=8 << 20),
        name="place",
    )(in_vmem(corner), in_vmem(weights), *[in_vmem(part) for part in parts])


def solution(mesh):
    return jax.shard_map(
        local,
        mesh=mesh,
        in_specs=(P("patch", "space", None), P(), P(), P(), P(), P(), P(), P(), P(), P()),
        out_specs=P("patch", None, "space", None),
        check_vma=False,
    )
```

```python
import functools
import math

import jax
import jax.numpy as jnp
from jax import lax
from jax.experimental import pallas as pl
from jax.experimental.pallas import tpu as pltpu
from jax.sharding import PartitionSpec as P

PX = 128
PZ = 16
TAPS = 3
ZG = 4
ZI = ZG + TAPS - 1
SLOTS = 16
LINE = TAPS * (PZ + 2) + 1
F32 = jnp.float32
BF16 = jnp.bfloat16
HI = lax.Precision.HIGHEST
CONTRACT_FIRST = (((0,), (0,)), ((), ()))
CONTRACT_LAST = (((1,), (1,)), ((), ()))
VMEM = pl.BlockSpec(memory_space=pltpu.VMEM)
SMEM = pl.BlockSpec(memory_space=pltpu.SMEM)


def iota(shape, dim):
    return lax.broadcasted_iota(jnp.int32, shape, dim)


def repeat_matrix(channels, lanes, dtype):
    shape = (channels, lanes)
    return (iota(shape, 0) == iota(shape, 1) % channels).astype(dtype)


def cut_kernel(offsets_ref, image_ref, out_ref, rows_ref):
    slab_rows, band_rows, width = image_ref.shape
    for z in range(slab_rows):
        rows_ref[z * band_rows : (z + 1) * band_rows, :] = image_ref[z].astype(F32)
    rows = rows_ref[...]
    items = offsets_ref.shape[1]
    spaces = out_ref.shape[0] // items
    for item in range(items):
        shift = lax.rem(width - offsets_ref[1, item], width)
        window = pltpu.roll(rows, shift, 1)[:, :PX].astype(BF16)
        for space in range(spaces):
            out_ref[space * items + item] = window


def prep_kernel(
    spaces,
    slab_rows,
    band_rows,
    offsets_ref,
    w1_ref,
    w2_ref,
    gain1_ref,
    bias1_ref,
    gain2_ref,
    bias2_ref,
    head_ref,
    head_bias_ref,
    flat_ref,
    full_ref,
    wide_ref,
    pair_ref,
    params_ref,
    heads_ref,
    bias_ref,
    weights_ref,
    corner_ref,
    narrow_ref,
):
    channels = gain1_ref.shape[1]
    classes = head_ref.shape[0]
    rows = band_rows * spaces
    hidden_rows = band_rows + TAPS - 1
    step = 4 * channels
    band = lax.axis_index("space")
    patch = lax.axis_index("patch")

    repeat = repeat_matrix(channels, step, BF16)
    taps = [
        jnp.dot(w1_ref[t], repeat, preferred_element_type=F32) for t in range(TAPS * TAPS)
    ]
    mirror = iota((1, step), 1) // channels
    narrow_ref[...] = jnp.zeros_like(narrow_ref)
    for b in range(TAPS):
        for a in range(TAPS):
            one, two = taps[a * TAPS + b], taps[(TAPS - 1 - a) * TAPS + b]
            for c in range(TAPS):
                d = TAPS - 1 - c
                row = jnp.where(
                    mirror < 2,
                    jnp.where(mirror == 0, one[c : c + 1], two[c : c + 1]),
                    jnp.where(mirror == 2, one[d : d + 1], two[d : d + 1]),
                )
                at = SLOTS * b + a * TAPS + c
                narrow_ref[at : at + 1, :] = row
    lanes = flat_ref.shape[1]
    shape = (step, lanes)
    lane = iota(shape, 1)
    spread = iota(shape, 0) == lane // (hidden_rows * channels) * channels + lane % channels
    flat = jnp.dot(
        narrow_ref[...].astype(BF16), spread.astype(BF16), preferred_element_type=F32
    )
    flat_ref[...] = flat
    lane_row = iota((SLOTS, lanes), 1) // channels % hidden_rows
    for yi in range(hidden_rows + TAPS - 1):
        piece = jnp.zeros((SLOTS, lanes), F32)
        for b in range(TAPS):
            if 0 <= yi - b < hidden_rows:
                piece = jnp.where(lane_row == yi - b, flat[SLOTS * b : SLOTS * b + SLOTS], piece)
        full_ref[SLOTS * yi : SLOTS * yi + SLOTS, :] = piece.astype(BF16)

    lanes = ZG * band_rows * channels
    spread = repeat_matrix(channels, lanes, BF16)
    taps = [
        lax.dot_general(w2_ref[t], spread, CONTRACT_FIRST, preferred_element_type=F32)
        for t in range(TAPS * TAPS)
    ]
    half = lanes // 2
    group = iota((channels, lanes), 1) // channels
    outer = TAPS - 1
    for zi in range(ZI):
        for yi in range(hidden_rows):
            at = (zi * hidden_rows + yi) * channels
            piece = jnp.zeros((channels, lanes), F32)
            pair = jnp.zeros((channels, lanes), F32)
            for zo in range(ZG):
                for yo in range(band_rows):
                    a, b = zi - zo, yi - yo
                    if 0 <= a < TAPS and 0 <= b < TAPS:
                        to = zo * band_rows + yo
                        tap = taps[a * TAPS + b]
                        piece = jnp.where(group == to, tap[outer * channels :], piece)
                        if zo < ZG // 2:
                            pair = jnp.where(group == to, tap[:channels], pair)
                            to = to + half // channels
                            pair = jnp.where(
                                group == to, tap[channels : 2 * channels], pair
                            )
            wide_ref[at : at + channels, :] = piece.astype(BF16)
            if zi < ZI - ZG // 2:
                pair_ref[at : at + channels, :] = pair.astype(BF16)

    table = jnp.concatenate(
        [
            gain1_ref[...],
            bias1_ref[...],
            gain2_ref[...],
            bias2_ref[...],
            head_ref[...].astype(F32),
            jnp.zeros((8 - classes - 4, channels), F32),
        ],
        axis=0,
    )
    spread = repeat_matrix(channels, params_ref.shape[1], F32)
    table = jnp.dot(table, spread, precision=HI, preferred_element_type=F32)
    params_ref[...] = table
    table = table[:, :lanes]

    per_z = classes * band_rows
    shape = (ZG * per_z, lanes)
    row_z = iota(shape, 0) // per_z
    row_k = iota(shape, 0) // band_rows % classes
    row_y = iota(shape, 0) % band_rows
    full = jnp.zeros(shape, F32)
    for k in range(classes):
        full = jnp.where(row_k == k, table[4 + k : 5 + k], full)
    lane_z = iota(shape, 1) // (band_rows * channels)
    lane_y = iota(shape, 1) // channels % band_rows
    for f, z in enumerate((row_z, ZG - 1 - row_z)):
        heads_ref[f] = jnp.where((lane_z == z) & (lane_y == row_y), full, 0.0).astype(BF16)
    row_k = iota(bias_ref.shape, 0) // band_rows % classes
    bias = jnp.zeros(bias_ref.shape, F32)
    for k in range(classes):
        bias = jnp.where(row_k == k, head_bias_ref[k], bias)
    bias_ref[...] = bias

    items, count, width = weights_ref.shape
    shape = (count, width)
    slab = patch * slab_rows
    z = slab + iota(shape, 0) // per_z
    x = iota(shape, 1)
    y = (band * band_rows + iota(shape, 0) % band_rows).astype(F32) - (rows - 1) / 2.0
    across = y * y * (1.0 / (2.0 * (rows / 8.0) ** 2))
    shape = corner_ref.shape
    corner_row, corner_lane = iota(shape, 0), iota(shape, 1)
    own_z = jnp.where(corner_lane == 0, offsets_ref[0, patch], 0)
    corners = jnp.where(corner_row == items, own_z, 0)
    coverage = jnp.zeros((count, width), F32)
    weights = []
    for k in range(items):
        item = jnp.bitwise_xor(patch, k)
        start_z, start_x = offsets_ref[0, item], offsets_ref[1, item]
        first = jnp.clip(slab - start_z, -slab_rows, PZ) * per_z + count
        values = jnp.where(corner_lane == 0, first, start_x)
        corners = jnp.where((corner_row == k) & (corner_lane < 2), values, corners)
        rel_z, rel_x = z - start_z, x - start_x
        inside = (rel_z >= 0) & (rel_z < PZ) & (rel_x >= 0) & (rel_x < PX)
        far_z = rel_z.astype(F32) - (PZ - 1) / 2.0
        far_x = rel_x.astype(F32) - (PX - 1) / 2.0
        power = (
            across
            + far_z * far_z * (1.0 / (2.0 * (PZ / 8.0) ** 2))
            + far_x * far_x * (1.0 / (2.0 * (PX / 8.0) ** 2))
        )
        weight = jnp.where(inside, jnp.exp(-power), 0.0)
        weights.append(weight)
        coverage = coverage + weight
    share = 1.0 / jnp.maximum(coverage, 0.1)
    for k in range(items):
        weights_ref[k] = weights[k] * share
    corner_ref[...] = corners


def line_rows(start_z, gathered_ref, cells_ref, lines_ref, slab_rows, band_rows, spaces):
    block = slab_rows * band_rows
    pitch = block + 1
    slabs = gathered_ref.shape[0] // spaces
    for device in range(gathered_ref.shape[0]):
        at = (device % slabs * spaces + device // slabs) * pitch
        cells_ref[at : at + block, :] = gathered_ref[device].astype(F32)
    lane = iota((spaces, PX), 1)
    empty = jnp.zeros((spaces, PX), F32)
    edge = jnp.zeros((LINE, PX), F32)
    last = band_rows * (spaces + 2) * LINE
    lines_ref[last : last + SLOTS, :] = edge[:SLOTS]
    for y in range(band_rows):
        base = y * (spaces + 2) * LINE
        lines_ref[base : base + LINE, :] = edge
        lines_ref[base + (spaces + 1) * LINE : base + (spaces + 2) * LINE, :] = edge
        base = base + LINE
        for k in (0, 1, 2, LINE - 4, LINE - 3, LINE - 2, LINE - 1):
            lines_ref[pl.ds(base + k, spaces, stride=LINE), :] = empty
    for z in range(PZ):
        deep = start_z + z
        slab = lax.div(deep, slab_rows)
        first = slab * (spaces * pitch) + (deep - slab * slab_rows) * band_rows
        for y in range(band_rows):
            line = cells_ref[pl.ds(first + y, spaces, stride=pitch), :]
            before = jnp.where(lane == 0, 0.0, pltpu.roll(line, 1, 1))
            after = jnp.where(lane == PX - 1, 0.0, pltpu.roll(line, PX - 1, 1))
            base = (y * (spaces + 2) + 1) * LINE + TAPS * (z + 1)
            for c, value in enumerate((before, line, after)):
                lines_ref[pl.ds(base + c, spaces, stride=LINE), :] = value


def tree_sum(values):
    values = list(values)
    while len(values) > 1:
        values = [
            values[i] + values[i + 1] if i + 1 < len(values) else values[i]
            for i in range(0, len(values), 2)
        ]
    return values[0]


def first_moments(lines_ref, gram_ref, weights, band_rows, spaces):
    rows = band_rows * spaces
    chunks = gram_ref.shape[0]
    size = rows // chunks
    ahead = TAPS - 1
    cells = []
    sums = [None] * rows
    for y in range(rows + ahead):
        line = []
        for z in range(PZ):
            at = (y % band_rows * (spaces + 2) + y // band_rows + 1) * LINE + TAPS * z
            value = lines_ref[at : at + SLOTS, :]
            line.append(value.astype(BF16))
            if y < rows:
                sums[y] = value if sums[y] is None else sums[y] + value
        cells.append(jnp.concatenate(line, axis=1))
    for chunk in range(chunks):
        left = jnp.concatenate(cells[chunk * size : (chunk + 1) * size], axis=0)
        right = jnp.concatenate(cells[chunk * size : (chunk + 1) * size + ahead], axis=0)
        gram_ref[chunk] = lax.dot_general(
            left, right, CONTRACT_LAST, preferred_element_type=F32
        )

    def block(y, delta, chosen):
        lane = SLOTS * (y + delta)
        tile = lane // 128 * 128
        end = min(tile + 128, gram_ref.shape[2])
        value = tree_sum(
            [gram_ref[chunk, SLOTS * y : SLOTS * (y + 1), tile:end] for chunk in chosen]
        )
        if end < tile + 128:
            value = jnp.concatenate(
                [value, jnp.zeros((SLOTS, tile + 128 - end), F32)], axis=1
            )
        return pltpu.roll(value, (tile + 128 - lane) % 128, 1) if lane != tile else value

    def total(values):
        return jnp.where(iota((SLOTS, 128), 1) < SLOTS, tree_sum(values), 0.0)

    every = range(chunks)
    head, tail = total([block(0, 0, [0])]), total([block(size - 1, 0, [chunks - 1])])
    near = total([block(y, 0, every) for y in range(size)])
    next1 = 2.0 * total([block(y, 1, every) for y in range(size)])
    next2 = 2.0 * total([block(y, 2, every) for y in range(size)])
    move = lambda value, k: pltpu.roll(value, SLOTS * k, 1)
    form = jnp.concatenate(
        [
            near - tail + move(next1, 1) + move(next2, 2),
            move(near, 1) + move(next1, 2),
            move(near - head, 2),
        ],
        axis=0,
    )[:, : TAPS * SLOTS]
    high = form.astype(BF16)
    left = form - high.astype(F32)
    middle = left.astype(BF16)
    low = (left - middle.astype(F32)).astype(BF16)
    product = jnp.dot(
        jnp.concatenate([high, middle, low], axis=0),
        weights.astype(BF16),
        preferred_element_type=F32,
    )
    size = TAPS * SLOTS
    product = product[:size] + (product[size : 2 * size] + product[2 * size :])
    squares = jnp.sum(product * weights, axis=0, keepdims=True)
    every = tree_sum(sums)
    column = jnp.concatenate([every - sums[rows - 1], every, every - sums[0]], axis=0)
    column = jnp.sum(column, axis=1, keepdims=True)
    return jnp.sum(column * weights, axis=0, keepdims=True), squares


def spread_mirror(value, f, channels):
    value = jnp.where(iota(value.shape, 1) // channels == f, value, 0.0)
    reach = channels
    while reach < value.shape[1]:
        value = value + pltpu.roll(value, reach, 1)
        reach *= 2
    return value


def main_kernel(
    spaces,
    slab_rows,
    band_rows,
    channels,
    gathered_ref,
    corner_ref,
    flat_ref,
    full_ref,
    w2t_ref,
    w2p_ref,
    params_ref,
    conv_ref,
    stats_ref,
    cells_ref,
    lines_ref,
    gram_ref,
    wide_ref,
):
    rows = band_rows * spaces
    hidden_rows = band_rows + TAPS - 1
    step = hidden_rows * channels
    band = lax.axis_index("space")
    start_z = corner_ref[lax.axis_size("patch"), 0]
    line_rows(start_z, gathered_ref, cells_ref, lines_ref, slab_rows, band_rows, spaces)

    first, second = first_moments(lines_ref, gram_ref, flat_ref[...], band_rows, spaces)
    count = float(PZ * rows * PX)
    mean = first / count
    variance = second / count - mean * mean
    lane_row = iota(mean.shape, 1) // channels % hidden_rows
    y = band * band_rows - 1 + lane_row
    inside = (y >= 0) & (y < rows)
    scale = lax.rsqrt(variance + 1e-05) * params_ref[0:1]
    shift = jnp.where(inside, params_ref[1:2] - mean * scale, 0.0)
    scale = jnp.where(inside, scale, 0.0)

    out_lanes = conv_ref.shape[2]
    half = out_lanes // 2
    groups = PZ // ZG
    empty = jnp.zeros((PX, step), BF16)
    for f in range(4):
        for g, j in ((0, 0), (groups - 1, ZI - 1)):
            at = (ZI - 1 - j if f % 2 else j) * step
            wide_ref[g, f * PX : (f + 1) * PX, at : at + step] = empty
    weights = full_ref[...]

    def hidden(cells_z):
        cells = []
        for yi in range(hidden_rows + TAPS - 1):
            base = (yi % band_rows * (spaces + 2) + yi // band_rows + band) * LINE
            line = [
                lines_ref[pl.ds(base + TAPS * z, SLOTS), :].astype(BF16) for z in cells_z
            ]
            cells.append(jnp.concatenate(line, axis=1))
        cells = jnp.concatenate(cells, axis=0)
        values = lax.dot_general(cells, weights, CONTRACT_FIRST, preferred_element_type=F32)
        for k, z in enumerate(cells_z):
            value = values[k * PX : (k + 1) * PX] * scale + shift
            value = jnp.maximum(value, 0.01 * value).astype(BF16)
            for g in range(groups):
                j = z + 1 - ZG * g
                if 0 <= j < ZI:
                    for f in range(4):
                        at = (ZI - 1 - j if f % 2 else j) * step
                        wide_ref[g, f * PX : (f + 1) * PX, at : at + step] = value[
                            :, f * step : (f + 1) * step
                        ]

    x = iota((2 * PX, out_lanes), 0) % PX
    totals = [[None] * 4, [None] * 4]
    blocks = ((0, 1), (1, 3), (3, groups))
    ends = [0] + [min(ZG * after, PZ - 1) + 1 for _, after in blocks]
    hidden(range(ends[0], ends[1]))
    for n, (start, after) in enumerate(blocks):
        if n + 1 < len(blocks):
            hidden(range(ends[n + 1], ends[n + 2]))
        cells = wide_ref[start:after].reshape((after - start) * 4 * PX, wide_ref.shape[2])
        last = jnp.dot(cells, w2t_ref[...], preferred_element_type=F32)
        pairs = [
            jnp.dot(
                cells[:, at : at + w2p_ref.shape[0]], w2p_ref[...], preferred_element_type=F32
            )
            for at in (0, ZG // 2 * step)
        ]
        first, middle = (
            jnp.concatenate([pair[:, at : at + half] for pair in pairs], axis=1)
            for at in (0, half)
        )
        for pair in range(2 * (after - start)):
            at = pair * 2 * PX
            g, low = start + pair // 2, pair % 2 * 2
            before, behind = (last, first) if low else (first, last)
            value = (
                middle[at : at + 2 * PX]
                + jnp.where(x == 0, 0.0, pltpu.roll(before[at : at + 2 * PX], 1, 0))
                + jnp.where(
                    x == PX - 1, 0.0, pltpu.roll(behind[at : at + 2 * PX], 2 * PX - 1, 0)
                )
            )
            conv_ref[g, low * PX : (low + 2) * PX, :] = value
            for f in (low, low + 1):
                part = value[(f - low) * PX : (f - low + 1) * PX]
                for kind, item in enumerate((part, part * part)):
                    item = jnp.sum(item, axis=0, keepdims=True)
                    old = totals[kind][f]
                    totals[kind][f] = item if old is None else old + item
    sums = jnp.concatenate(totals[0] + totals[1], axis=0)
    lanes = 4 * channels
    sums = sum(sums[:, at : at + lanes] for at in range(0, out_lanes, lanes))
    reach = lanes // 2
    while reach >= channels:
        sums = sums + pltpu.roll(sums, reach, 1)
        reach //= 2
    mirror = iota((1, lanes), 1) // channels
    for kind in range(2):
        row = sums[4 * kind : 4 * kind + 1]
        for f in range(1, 4):
            row = jnp.where(mirror == f, sums[4 * kind + f : 4 * kind + f + 1], row)
        for space in range(spaces):
            stats_ref[space, kind : kind + 1, :] = row


def head_kernel(count, channels, conv_ref, stats_ref, params_ref, heads_ref, bias_ref, out_ref):
    lanes = conv_ref.shape[2]
    per_group = heads_ref.shape[1]
    sums = stats_ref[0]
    for space in range(1, stats_ref.shape[0]):
        sums = sums + stats_ref[space]
    mean = sums[0:1] / count
    variance = sums[1:2] / count - mean * mean
    scale = lax.rsqrt(variance + 1e-05) * params_ref[2:3, : 4 * channels]
    shift = params_ref[3:4, : 4 * channels] - mean * scale
    table = jnp.concatenate([scale, shift, jnp.zeros((6, 4 * channels), F32)], axis=0)
    groups = conv_ref.shape[0]
    totals = [None] * groups
    for f in range(4):
        own = spread_mirror(table, f, channels)
        own = jnp.concatenate([own] * (lanes // own.shape[1]), axis=1)
        for g in range(groups):
            value = conv_ref[g, f * PX : (f + 1) * PX, :] * own[0:1] + own[1:2]
            value = jnp.maximum(value, 0.01 * value).astype(BF16)
            logits = lax.dot_general(
                heads_ref[f % 2], value, CONTRACT_LAST, preferred_element_type=F32
            )
            totals[g] = logits if totals[g] is None else totals[g] + logits
    for g in range(groups):
        out_ref[g * per_group : (g + 1) * per_group, :] = (
            totals[g] * 0.25 + bias_ref[...]
        ).astype(out_ref.dtype)


def place_kernel(items, corner_ref, weights_ref, *refs):
    parts, (out_ref, pad_ref) = refs[:items], refs[items:]
    slab_rows, classes, band_rows, width = out_ref.shape
    per_z = classes * band_rows
    count = slab_rows * per_z
    blended = jnp.zeros((count, width), F32)
    for k in range(items):
        pad_ref[k, count : count + PZ * per_z, :] = parts[k][...].astype(F32)
        part = pad_ref[k, pl.ds(corner_ref[k, 0], count), :]
        part = jnp.concatenate([part, jnp.zeros((count, width - PX), F32)], axis=1)
        part = pltpu.roll(part, corner_ref[k, 1], 1)
        weight = weights_ref[k]
        blended = blended + jnp.where(weight > 0, part * weight, 0.0)
    for z in range(slab_rows):
        for k in range(classes):
            at = z * per_z + k * band_rows
            out_ref[z, k] = blended[at : at + band_rows]


def in_vmem(value):
    return pltpu.with_memory_space_constraint(value, pltpu.VMEM)


def in_hbm(value):
    return pltpu.with_memory_space_constraint(value, pltpu.HBM)


def local(
    image,
    offsets,
    conv1_weight,
    conv2_weight,
    norm1_gain,
    norm1_bias,
    norm2_gain,
    norm2_bias,
    head_weight,
    head_bias,
):
    groups = lax.axis_size("patch")
    spaces = lax.axis_size("space")
    slab_rows, band_rows, width = image.shape
    channels = norm1_gain.shape[0]
    classes = head_weight.shape[0]
    rows = band_rows * spaces
    hidden_rows = band_rows + TAPS - 1
    block = slab_rows * band_rows
    step = 4 * channels
    lanes1 = 4 * hidden_rows * channels
    lanes2 = ZG * band_rows * channels
    depth2 = ZI * hidden_rows * channels
    depth3 = (ZI - ZG // 2) * hidden_rows * channels
    per_z = classes * band_rows
    corners = in_hbm(offsets.T)

    windows = pl.pallas_call(
        cut_kernel,
        out_shape=pltpu.VMEM((groups * spaces, block, PX), BF16),
        in_specs=[SMEM, VMEM],
        out_specs=VMEM,
        scratch_shapes=[pltpu.VMEM((block, width), F32)],
        name="cut",
    )(corners, image)
    gathered = lax.all_to_all(windows, ("space", "patch"), 0, 0, tiled=True)

    flat, full, w2t, w2p, params, heads, bias, weights, corner = pl.pallas_call(
        functools.partial(prep_kernel, spaces, slab_rows, band_rows),
        out_shape=(
            pltpu.VMEM((TAPS * SLOTS, lanes1), F32),
            pltpu.VMEM(((hidden_rows + TAPS - 1) * SLOTS, lanes1), BF16),
            pltpu.VMEM((depth2, lanes2), BF16),
            pltpu.VMEM((depth3, lanes2), BF16),
            pltpu.VMEM((8, lanes1), F32),
            pltpu.VMEM((2, ZG * per_z, lanes2), BF16),
            pltpu.VMEM((ZG * per_z, PX), F32),
            pltpu.VMEM((groups, slab_rows * per_z, width), F32),
            pltpu.VMEM(((groups + 8) // 8 * 8, 128), jnp.int32),
        ),
        in_specs=[SMEM] + [VMEM] * 7 + [SMEM],
        out_specs=(VMEM,) * 9,
        scratch_shapes=[pltpu.VMEM((TAPS * SLOTS, step), F32)],
        compiler_params=pltpu.CompilerParams(vmem_limit_bytes=16 << 20),
        name="prep",
    )(
        corners,
        in_hbm(conv1_weight.transpose(0, 2, 1)),
        in_hbm(conv2_weight),
        in_hbm(norm1_gain.reshape(1, channels)),
        in_hbm(norm1_bias.reshape(1, channels)),
        in_hbm(norm2_gain.reshape(1, channels)),
        in_hbm(norm2_bias.reshape(1, channels)),
        in_hbm(head_weight),
        in_hbm(head_bias),
    )
    chunks = max(rows // 8, 1)
    scratch = (
        ((groups * spaces * (block + 1), PX), F32),
        ((band_rows * (spaces + 2) * LINE + SLOTS, PX), F32),
        ((chunks, rows // chunks * SLOTS, (rows // chunks + TAPS - 1) * SLOTS), F32),
        ((PZ // ZG, 4 * PX, depth2), BF16),
    )
    size = sum(math.prod(shape) * jnp.dtype(kind).itemsize for shape, kind in scratch)
    conv, stats = pl.pallas_call(
        functools.partial(main_kernel, spaces, slab_rows, band_rows, channels),
        out_shape=(
            pltpu.VMEM((PZ // ZG, 4 * PX, lanes2), F32),
            pltpu.VMEM((spaces, 2, step), F32),
        ),
        in_specs=[VMEM] * 7,
        out_specs=(VMEM, VMEM),
        scratch_shapes=[pltpu.VMEM(shape, kind) for shape, kind in scratch],
        compiler_params=pltpu.CompilerParams(vmem_limit_bytes=min(2 * size + (16 << 20), 40 << 20)),
        name="main",
    )(
        in_vmem(gathered),
        in_vmem(corner),
        in_vmem(flat),
        in_vmem(full),
        in_vmem(w2t),
        in_vmem(w2p),
        in_vmem(params),
    )
    stats = lax.all_to_all(stats, "space", 0, 0, tiled=True)
    averaged = pl.pallas_call(
        functools.partial(head_kernel, float(PZ * rows * PX), channels),
        out_shape=pltpu.VMEM((PZ * per_z, PX), BF16),
        in_specs=[VMEM] * 5,
        out_specs=VMEM,
        compiler_params=pltpu.CompilerParams(vmem_limit_bytes=8 << 20),
        name="head",
    )(in_vmem(conv), in_vmem(stats), in_vmem(params), in_vmem(heads), in_vmem(bias))
    parts = [averaged] + [
        lax.ppermute(averaged, "patch", [(i, i ^ k) for i in range(groups)])
        for k in range(1, groups)
    ]
    return pl.pallas_call(
        functools.partial(place_kernel, groups),
        out_shape=jax.ShapeDtypeStruct((slab_rows, classes, band_rows, width), F32),
        in_specs=[VMEM] * (2 + groups),
        out_specs=VMEM,
        scratch_shapes=[pltpu.VMEM((groups, (2 * slab_rows + PZ) * per_z, PX), F32)],
        compiler_params=pltpu.CompilerParams(vmem_limit_bytes=8 << 20),
        name="place",
    )(in_vmem(corner), in_vmem(weights), *[in_vmem(part) for part in parts])


def solution(mesh):
    return jax.shard_map(
        local,
        mesh=mesh,
        in_specs=(P("patch", "space", None), P(), P(), P(), P(), P(), P(), P(), P(), P()),
        out_specs=P("patch", None, "space", None),
        check_vma=False,
    )
```
